32 devices in a mesh: expert: 16 (over z, y, x), shard: 2 (over core).
Axes of the slice: x: 2, y: 2, z: 4, core: 2. Of those that a mesh axis runs over, the one named last changes fastest.
Arguments:
- tokens: bfloat16 [4096, 2048], P(('expert', 'shard')), may hold values from -6 to 6
- lengths: int32 [32, 4], P(('expert', 'shard')), may hold values from 1 to 64, 128 in all within a row
- routes: int32 [4096, 8], P(('expert', 'shard')), may hold values from 0 to 31, all different within a row; in each aligned block of 128 rows (0 to 127, 128 to 255, ...) at most 48 rows name the same one
- cotangent: bfloat16 [4096, 2048], P(('expert', 'shard')), may hold values from -6 to 6
- query_weight: bfloat16 [2048, 4096], P(('expert', 'shard')), may hold values from -0.125 to 0.125
- key_weight: bfloat16 [2048, 512], P(('expert', 'shard')), may hold values from -0.125 to 0.125
- value_weight: bfloat16 [2048, 512], P(('expert', 'shard')), may hold values from -0.125 to 0.125
- output_weight: bfloat16 [4096, 2048], P(('expert', 'shard')), may hold values from -0.375 to 0.375
- router_weight: bfloat16 [2048, 32], P(('expert', 'shard')), may hold values from -0.125 to 0.125
- norm_gains: bfloat16 [4352], P(('expert', 'shard')), may hold values from 0.25 to 1.75
- gate_weight: bfloat16 [32, 2048, 768], P(('expert', 'shard')), may hold values from -0.125 to 0.125
- up_weight: bfloat16 [32, 2048, 768], P(('expert', 'shard')), may hold values from -0.125 to 0.125
- down_weight: bfloat16 [32, 768, 2048], P(('expert', 'shard')), may hold values from -0.875 to 0.875
Outputs:
- block_out: bfloat16 [4096, 2048], P(('expert', 'shard'))
- input_grad: float32 [4096, 2048], P(('expert', 'shard'))
- query_grad: float32 [2048, 4096], P(('expert', 'shard'))
- key_grad: float32 [2048, 512], P(('expert', 'shard'))
- value_grad: float32 [2048, 512], P(('expert', 'shard'))
- output_grad: float32 [4096, 2048], P(('expert', 'shard'))
- router_grad: float32 [2048, 32], P(('expert', 'shard'))
- gains_grad: float32 [4352], P(('expert', 'shard'))
- gate_grad: float32 [32, 2048, 768], P(('expert', 'shard'))
- up_grad: float32 [32, 2048, 768], P(('expert', 'shard'))
- down_grad: float32 [32, 768, 2048], P(('expert', 'shard'))
The draws below stay inside these ranges and needn't reach their ends.
Inputs may be any that keep to these rules, and one draw needn't show every extreme that they name: `lengths`: each row of a device sums with the others to 128; the longest is exactly 64. `routes`: each token names 8 different experts. Among the 128 rows of one device no expert is named more than 48 times; in every draw some expert is named exactly 48 times by some device's rows.
All inputs are finite; a program needn't handle non-finite values.
Results may differ from the reference program's by a relative error of at most 0.018.
Values may be sent and summed in bfloat16 or wider, within the bound.
A program may use at most 256 MiB of HBM per device.

```python
import math
from functools import partial
import jax
import jax.numpy as jnp
import numpy as np
from jax import lax

D = 2048
HEADS = 32
KV_HEADS = 4
HEAD_DIM = 128
FF = 768
TOP = 8
TOK_DEV = 128
SEQS = 4
SEQ_MAX = 64
EXPERTS = 32
CAP = 48
TOKENS = 4096
DEVICES = 32


def level_of(stream_key, shape, split, smallest, high):
    factor_of = 1.0
    for dim, parts in split:
        steps = jax.random.uniform(jax.random.fold_in(jax.random.fold_in(stream_key, 6), dim), (parts,), jnp.float32, smallest / len(split), high / len(split))
        factor_of = factor_of * jnp.repeat(jnp.exp(steps), shape[dim] // parts).reshape((-1,) + (1,) * (len(shape) - 1 - dim))
    return factor_of


def length_profile(number_of, total, reach, lean):
    loads = [(1 << 20) // math.isqrt(rank ** lean) + 1 for rank in range(2, number_of + 1)]
    surplus, given = total - reach - (number_of - 1), [1] * (number_of - 1)
    while surplus > 0:
        free = [i for i in range(number_of - 1) if given[i] < reach]
        pool, budget = sum([loads[i] for i in free]), surplus
        for i in free:
            addition = min(reach - given[i], max(1, budget * loads[i] // pool), surplus)
            given[i] = given[i] + addition
            surplus = surplus - addition
    return np.array([reach] + given)


def uneven_parts(rng, number_of, total, bound, skew):
    if number_of == 2:
        one = jax.random.randint(rng, (), max(1, total - bound), min(bound, total - 1) + 1)
        return jnp.stack([one, total - one])
    tallies = jnp.asarray(length_profile(number_of, total, bound, skew), jnp.int32)
    couples = (number_of - 1) // 2
    donor, taker = tallies[1:1 + 2 * couples:2], tallies[2:2 + 2 * couples:2]
    slack = jnp.minimum(donor - 1, bound - taker)
    passed = jax.random.randint(jax.random.fold_in(rng, 1), (couples,), 0, 1 << 20) % (slack + 1)
    tallies = tallies.at[1:1 + 2 * couples:2].set(donor - passed).at[2:2 + 2 * couples:2].set(taker + passed)
    return tallies[jax.random.permutation(jax.random.fold_in(rng, 2), number_of)]


def assign_block(key, own, number, rows, count, top, bound, slope):
    order = jax.random.permutation(key, count)
    heavy_load, usual = portions_of(count, rows * top, bound, slope, True), portions_of(count, rows * top, bound, slope, False)
    places = jnp.arange(count)

    def named(sizes, offset_by):
        used = int((sizes > 0).sum())
        fixed = max(1, used // 4)
        shifted = fixed + (places - fixed + offset_by * (used - fixed)) % max(1, count - fixed)
        return jnp.zeros((count,), jnp.int32).at[order[jnp.where(places < fixed, places, shifted)]].set(jnp.asarray(sizes, jnp.int32))

    sizes = jnp.where(number % 4 == 0, named(heavy_load, number // 4), named(usual, number - number // 4 - 1))
    mixed = jax.random.permutation(jax.random.fold_in(own, 3), count)
    source_of, receiver = mixed[0:count // 2 * 2:2], mixed[1:count // 2 * 2:2]
    slack = jnp.minimum(sizes[source_of] - 1, bound - sizes[receiver]) // 2
    slack = jnp.where((source_of == order[0]) | (receiver == order[0]) | (sizes[receiver] == 0), 0, jnp.maximum(slack, 0))
    shifted = jax.random.randint(jax.random.fold_in(own, 4), (count // 2,), 0, 1 << 20) % (slack + 1)
    sizes = sizes.at[source_of].add(-shifted).at[receiver].add(shifted)
    items = jnp.searchsorted(jnp.cumsum(sizes), jnp.arange(rows * top), side="right").astype(jnp.int32)
    grid = items.reshape(top, rows).T
    grid = grid[jax.random.permutation(jax.random.fold_in(own, 1), rows)]
    offset_by = jax.random.randint(jax.random.fold_in(own, 2), (rows, 1), 0, top)
    return jnp.take_along_axis(grid, (jnp.arange(top)[None, :] + offset_by) % top, axis=1)


def portions_of(count, total, bound, lean, full):
    weights = [(1 << 20) // math.isqrt(rank ** lean) + 1 for rank in range(1, count + 1)]
    largest = bound if full else min(bound, max(-(-total // count), total * weights[0] // sum(weights)))
    least = 1 if total - largest >= count - 1 else 0
    given, rest = [largest] + [least] * (count - 1), total - largest - least * (count - 1)
    while rest > 0:
        candidates = [i for i in range(1, count) if given[i] < largest] or [i for i in range(1, count) if given[i] < bound]
        whole, remaining = sum([weights[i] for i in candidates]), rest
        for i in candidates:
            extra = min(bound - given[i], max(1, remaining * weights[i] // whole), rest)
            given[i] = given[i] + extra
            rest = rest - extra
    return np.array(given)


def scatter_about(rng, extent, spread, most, pieces=(), kind=jnp.bfloat16):
    values = jax.random.normal(rng, extent, jnp.float32) * spread
    if len(pieces) > 0:
        values = level_of(rng, extent, pieces, -0.22, 0.18) * values
    return jnp.clip(values, min=-most, max=most).astype(kind)


def setup_inputs(seed: int = 0) -> dict:
    arg_keys = jax.random.split(jax.random.key(seed), 14)
    tokens = scatter_about(arg_keys[0], (TOKENS, D), 1.0, 6.0, ((0, 32),))
    lengths = jax.vmap(lambda own: uneven_parts(own, SEQS, TOK_DEV, SEQ_MAX, 1))(jax.random.split(arg_keys[1], DEVICES)).reshape((DEVICES, SEQS)).astype(jnp.int32)
    routes_keys = jax.random.split(jax.random.fold_in(arg_keys[2], 1), TOKENS // TOK_DEV)
    routes_turns = jax.random.permutation(jax.random.fold_in(arg_keys[2], 3), TOKENS // TOK_DEV)
    routes = jax.vmap(lambda own, number: assign_block(jax.random.fold_in(arg_keys[2], 2), own, number, TOK_DEV, EXPERTS, TOP, CAP, 1))(routes_keys, routes_turns).reshape((TOKENS, TOP))
    cotangent = scatter_about(arg_keys[3], (TOKENS, D), 1.0, 6.0, ((0, 32),))
    query_weight = scatter_about(arg_keys[4], (D, HEADS * HEAD_DIM), D ** -0.5, 0.125, ((0, 32),))
    key_weight = scatter_about(arg_keys[5], (D, KV_HEADS * HEAD_DIM), D ** -0.5, 0.125, ((0, 32),))
    value_weight = scatter_about(arg_keys[6], (D, KV_HEADS * HEAD_DIM), D ** -0.5, 0.125, ((0, 32),))
    output_weight = scatter_about(arg_keys[7], (HEADS * HEAD_DIM, D), (HEADS * HEAD_DIM // 16) ** -0.5, 0.375, ((0, 32),))
    router_weight = scatter_about(arg_keys[8], (D, EXPERTS), D ** -0.5, 0.125, ((0, 32),))
    norm_gains = jnp.clip(1.0 + 0.15 * jax.random.normal(arg_keys[9], (2 * D + 2 * HEAD_DIM,), jnp.float32), 0.25, 1.75).astype(jnp.bfloat16)
    gate_weight = scatter_about(arg_keys[10], (EXPERTS, D, FF), D ** -0.5, 0.125, ((0, 32),))
    up_weight = scatter_about(arg_keys[11], (EXPERTS, D, FF), D ** -0.5, 0.125, ((0, 32),))
    down_weight = scatter_about(arg_keys[12], (EXPERTS, FF, D), (FF // 16) ** -0.5, 0.875, ((0, 32),))
    return dict(tokens=tokens, lengths=lengths, routes=routes, cotangent=cotangent, query_weight=query_weight, key_weight=key_weight, value_weight=value_weight, output_weight=output_weight, router_weight=router_weight, norm_gains=norm_gains, gate_weight=gate_weight, up_weight=up_weight, down_weight=down_weight)


@jax.custom_vjp
def low(v):
    return lax.optimization_barrier(v.astype(jnp.bfloat16)).astype(jnp.float32)

@jax.custom_vjp
def low_back(v):
    return v

def low_keep(v):
    return (low(v), None)

def low_pass(kept, grad):
    return (grad,)

def back_keep(v):
    return (v, None)

def back_low(kept, grad):
    return (low(grad),)
low.defvjp(low_keep, low_pass)
low_back.defvjp(back_keep, back_low)
epsilon = 1e-06
rope_base = 1000000.0
masked_score = -1e+30
highest = lax.Precision.HIGHEST

def matmul(left, right):
    return jnp.dot(left, right, precision=highest, preferred_element_type=jnp.float32)

def rms_norm(values):
    return values * lax.rsqrt(lax.optimization_barrier(jnp.mean(values * values, axis=-1, keepdims=True)) + epsilon)

def sequence_layout(lengths_row, row_count):
    seq_ends = jnp.cumsum(lengths_row)
    places = jnp.arange(row_count, dtype=jnp.int32)
    segment = lax.optimization_barrier(jnp.sum((places[:, None] >= seq_ends[None, :]).astype(jnp.int32), axis=1))
    starts = seq_ends - lengths_row
    member = segment[:, None] == jnp.arange(lengths_row.shape[0], dtype=jnp.int32)[None, :]
    seg_start = lax.optimization_barrier(jnp.sum(jnp.where(member, starts[None, :], 0), axis=1))
    return (segment, (places - seg_start).astype(jnp.int32))

def rope_tables(positions, head_dim):
    half_dim = head_dim // 2
    inverse = rope_base ** (-2.0 * jnp.arange(half_dim, dtype=jnp.float32) / head_dim)
    angles = positions.astype(jnp.float32)[:, None] * inverse[None, :]
    return (jnp.cos(angles)[:, None, :], jnp.sin(angles)[:, None, :])

def rotate(values, cosine, sine_table):
    half_dim = values.shape[-1] // 2
    first_half = values[..., :half_dim]
    second_half = values[..., half_dim:]
    return jnp.concatenate([first_half * cosine - second_half * sine_table, second_half * cosine + first_half * sine_table], axis=-1)

def build_slots(routes):
    per_device = routes.reshape(DEVICES, TOK_DEV * TOP)
    onehot = (per_device[:, :, None] == jnp.arange(EXPERTS, dtype=jnp.int32)[None, None, :]).astype(jnp.int32)
    earlier = jnp.cumsum(onehot, axis=1) - onehot
    slot_index = lax.optimization_barrier(jnp.sum(earlier * onehot, axis=2))
    device_ids = jnp.arange(DEVICES, dtype=jnp.int32)[:, None]
    column = device_ids * CAP + slot_index
    flat_ids = device_ids * (TOK_DEV * TOP) + jnp.arange(TOK_DEV * TOP, dtype=jnp.int32)[None, :]
    token_ids = (flat_ids // TOP).astype(jnp.int32)
    row_table = jnp.full((EXPERTS, DEVICES * CAP), TOKENS, jnp.int32).at[per_device, column].set(token_ids)
    position = (per_device * (DEVICES * CAP) + column).reshape(-1).astype(jnp.int32)
    return (row_table, position)

def attention_block(block_args):
    query, keys, values_in, segment, positions = block_args
    scores = jnp.einsum('qkgd,skd->kgqs', query, keys, precision=highest) * HEAD_DIM ** (-0.5)
    scores = low_back(scores)
    allowed = (segment[:, None] == segment[None, :]) & (positions[None, :] <= positions[:, None])
    scores = jnp.where(allowed[None, None], scores, masked_score)
    attn_probs = low(jax.nn.softmax(scores, axis=-1))
    mixed_heads = jnp.einsum('kgqs,skd->qkgd', attn_probs, values_in, precision=highest)
    return mixed_heads.reshape(TOK_DEV, HEADS * HEAD_DIM)

def reference(tokens, lengths, routes, cotangent, query_weight, key_weight, value_weight, output_weight, router_weight, norm_gains, gate_weight, up_weight, down_weight):
    groups = HEADS // KV_HEADS
    segment, positions = jax.vmap(partial(sequence_layout, row_count=TOK_DEV))(lengths)
    segment = segment.reshape(-1)
    positions = positions.reshape(-1)
    row_table, position = build_slots(routes)
    cosine, sine_table = rope_tables(positions, HEAD_DIM)

    def forward(inputs, query_weight, key_weight, value_weight, output_weight, router_weight, norm_gains, gate_weight, up_weight, down_weight):
        gain_attn = norm_gains[:D]
        gain_ffn = norm_gains[D:2 * D]
        gain_query = norm_gains[2 * D:2 * D + HEAD_DIM]
        gain_key = norm_gains[2 * D + HEAD_DIM:]
        hidden_one = low(rms_norm(inputs) * gain_attn)
        query_proj = low_back(matmul(hidden_one, query_weight)).reshape(TOKENS, HEADS, HEAD_DIM)
        key_proj = low_back(matmul(hidden_one, key_weight)).reshape(TOKENS, KV_HEADS, HEAD_DIM)
        value_proj = low(low_back(matmul(hidden_one, value_weight))).reshape(TOKENS, KV_HEADS, HEAD_DIM)
        query_rot = low(rotate(rms_norm(query_proj) * gain_query, cosine, sine_table))
        key_rot = low(rotate(rms_norm(key_proj) * gain_key, cosine, sine_table))
        mixed_heads = lax.map(jax.checkpoint(attention_block), (query_rot.reshape(DEVICES, TOK_DEV, KV_HEADS, groups, HEAD_DIM), key_rot.reshape(DEVICES, TOK_DEV, KV_HEADS, HEAD_DIM), value_proj.reshape(DEVICES, TOK_DEV, KV_HEADS, HEAD_DIM), segment.reshape(DEVICES, TOK_DEV), positions.reshape(DEVICES, TOK_DEV)))
        mixed_heads = low(low_back(mixed_heads.reshape(TOKENS, HEADS * HEAD_DIM)))
        residual = inputs + low_back(matmul(mixed_heads, output_weight))
        hidden_two = low(rms_norm(residual) * gain_ffn)
        logits = low_back(matmul(hidden_two, router_weight))
        chosen = jnp.take_along_axis(logits, routes, axis=1)
        route_weight = jax.nn.softmax(chosen, axis=-1)
        padded = jnp.concatenate([hidden_two, jnp.zeros((1, D), jnp.float32)], axis=0)

        def expert_fn(block_args):
            rows_index, gate_mat, up_mat, down_mat = block_args
            gathered_rows = low_back(padded[rows_index])
            gate_act = low_back(matmul(gathered_rows, gate_mat))
            up_act = low_back(matmul(gathered_rows, up_mat))
            expert_hidden = low(jax.nn.silu(gate_act) * up_act)
            return low(low_back(matmul(expert_hidden, down_mat)))
        expert_outs = lax.map(jax.checkpoint(expert_fn), (row_table, gate_weight, up_weight, down_weight))
        route_out = expert_outs.reshape(EXPERTS * DEVICES * CAP, D)[position].reshape(TOKENS, TOP, D)
        return residual + lax.optimization_barrier(jnp.sum(route_weight[:, :, None] * route_out, axis=1))
    primal, pullback = jax.vjp(forward, tokens.astype(jnp.float32), query_weight.astype(jnp.float32), key_weight.astype(jnp.float32), value_weight.astype(jnp.float32), output_weight.astype(jnp.float32), router_weight.astype(jnp.float32), norm_gains.astype(jnp.float32), gate_weight.astype(jnp.float32), up_weight.astype(jnp.float32), down_weight.astype(jnp.float32))
    gradients = pullback(cotangent.astype(jnp.float32))
    return (primal.astype(jnp.bfloat16), gradients[0], gradients[1], gradients[2], gradients[3], gradients[4], gradients[5], gradients[6], gradients[7], gradients[8], gradients[9])
```

```python
import jax
import jax.numpy as jnp
from jax import lax
from jax.sharding import Mesh
from jax.sharding import PartitionSpec as P

D = 2048
HEADS = 32
KV_HEADS = 4
HEAD_DIM = 128
TOP = 8

epsilon = 1e-06
rope_base = 1000000.0
masked_score = -1e30

GROUPS = HEADS // KV_HEADS
Q_COLS = GROUPS * HEAD_DIM
LINE = "line"
PLANE = ("plane", "core")
ALL = ("line", "plane", "core")
F32 = jnp.float32
BF16 = jnp.bfloat16


def dot(left, right):
    return jnp.dot(left, right, preferred_element_type=F32)


def rms_scale(values):
    return lax.rsqrt(jnp.mean(values * values, axis=-1, keepdims=True) + epsilon)


def norm_back(upstream, normed, scale_rows):
    return scale_rows * (upstream - normed * jnp.mean(upstream * normed, axis=-1, keepdims=True))


def sequence_layout(lengths_row, row_count):
    seq_ends = jnp.cumsum(lengths_row)
    places = jnp.arange(row_count, dtype=jnp.int32)
    segment = jnp.sum((places[:, None] >= seq_ends[None, :]).astype(jnp.int32), axis=1)
    starts = seq_ends - lengths_row
    member = segment[:, None] == jnp.arange(lengths_row.shape[0], dtype=jnp.int32)[None, :]
    seg_start = jnp.sum(jnp.where(member, starts[None, :], 0), axis=1)
    return (segment, places - seg_start)


def rope_tables(positions, head_dim):
    half_dim = head_dim // 2
    inverse = rope_base ** (-2.0 * jnp.arange(half_dim, dtype=F32) / head_dim)
    angles = positions.astype(F32)[..., None] * inverse
    return (jnp.cos(angles), jnp.sin(angles))


def rotate(values, cosine, sine_table):
    half_dim = values.shape[-1] // 2
    first_half = values[..., :half_dim]
    second_half = values[..., half_dim:]
    return jnp.concatenate(
        [
            first_half * cosine - second_half * sine_table,
            second_half * cosine + first_half * sine_table,
        ],
        axis=-1,
    )


def masked_scores(query, keys, allowed, score_scale):
    scores = jnp.einsum("bqgd,bsd->bgqs", query, keys, preferred_element_type=F32) * score_scale
    return jnp.where(allowed[:, None], scores, masked_score)


def attend(query, keys, values_in, allowed, score_scale):
    scores = masked_scores(query, keys, allowed, score_scale)
    top_score = jnp.max(scores, axis=-1, keepdims=True)
    exponent = jnp.exp(scores - top_score)
    row_total = jnp.sum(exponent, axis=-1, keepdims=True)
    attn_probs = (exponent / row_total).astype(BF16)
    mixed_heads = jnp.einsum("bgqs,bsd->bqgd", attn_probs, values_in, preferred_element_type=F32)
    return (mixed_heads, top_score + jnp.log(row_total))


def attend_back(query, keys, values_in, allowed, score_scale, log_total, grad_mixed):
    scores = masked_scores(query, keys, allowed, score_scale)
    attn_probs = jnp.exp(scores - log_total)
    grad_probs = jnp.einsum("bqgd,bsd->bgqs", grad_mixed, values_in, preferred_element_type=F32)
    grad_scores = (
        attn_probs * (grad_probs - jnp.sum(attn_probs * grad_probs, axis=-1, keepdims=True))
    ).astype(BF16)
    grad_query = (
        jnp.einsum("bgqs,bsd->bqgd", grad_scores, keys, preferred_element_type=F32) * score_scale
    )
    grad_keys = (
        jnp.einsum("bgqs,bqgd->bsd", grad_scores, query, preferred_element_type=F32) * score_scale
    )
    grad_values = jnp.einsum(
        "bgqs,bqgd->bsd", attn_probs.astype(BF16), grad_mixed, preferred_element_type=F32
    )
    return (grad_query, grad_keys, grad_values)


def on_device(
    tokens,
    lengths,
    routes,
    cotangent,
    query_weight,
    key_weight,
    value_weight,
    output_weight,
    router_weight,
    norm_gains,
    gate_weight,
    up_weight,
    down_weight,
):
    rows = tokens.shape[0]
    lines = lax.axis_size("line")
    cells = lax.axis_size("plane") * lax.axis_size("core")
    experts = lines * cells
    capacity = (3 * rows * TOP + 2 * experts - 1) // (2 * experts)
    score_scale = HEAD_DIM ** (-0.5)
    large = experts > 32
    own_rows = query_weight.shape[0]
    line = lax.axis_index("line")
    me = (line * lax.axis_size("plane") + lax.axis_index("plane")) * lax.axis_size(
        "core"
    ) + lax.axis_index("core")

    packed = jnp.concatenate(
        [
            query_weight.reshape(own_rows, lines, Q_COLS),
            key_weight.reshape(own_rows, lines, HEAD_DIM),
            value_weight.reshape(own_rows, lines, HEAD_DIM),
        ],
        axis=2,
    ).transpose(1, 0, 2)
    width = packed.shape[2]
    packed = lax.all_to_all(packed, LINE, split_axis=0, concat_axis=0, tiled=True)
    packed = lax.all_gather(packed, PLANE, axis=1, tiled=False)
    weight_qkv = packed.reshape(lines * cells * own_rows, width)
    weight_o = lax.all_gather(output_weight, PLANE, axis=0, tiled=True)
    gains = lax.all_gather(norm_gains, ALL, axis=0, tiled=True).astype(F32)
    router = lax.all_gather(router_weight, ALL, axis=0, tiled=True)
    gain_attn = gains[:D]
    gain_ffn = gains[D : 2 * D]
    gain_query = gains[2 * D : 2 * D + HEAD_DIM]
    gain_key = gains[2 * D + HEAD_DIM :]

    routes_all = lax.all_gather(routes, ALL, axis=0, tiled=True)

    line_tokens = lax.all_gather(tokens, LINE, axis=0, tiled=True)
    line_lengths = lax.all_gather(lengths, LINE, axis=0, tiled=True)
    inputs = line_tokens.astype(F32)
    attn_scale = rms_scale(inputs)
    attn_normed = inputs * attn_scale
    hidden_one = (attn_normed * gain_attn).astype(BF16)
    proj = dot(hidden_one, weight_qkv)
    query_proj = proj[:, :Q_COLS].reshape(lines, rows, GROUPS, HEAD_DIM)
    key_proj = proj[:, Q_COLS : Q_COLS + HEAD_DIM].reshape(lines, rows, HEAD_DIM)
    value_proj = proj[:, Q_COLS + HEAD_DIM :].astype(BF16).reshape(lines, rows, HEAD_DIM)
    query_scale = rms_scale(query_proj)
    query_normed = query_proj * query_scale
    key_scale = rms_scale(key_proj)
    key_normed = key_proj * key_scale
    segment, positions = jax.vmap(lambda row: sequence_layout(row, rows))(line_lengths)
    cosine, sine_table = rope_tables(positions, HEAD_DIM)
    query_rot = rotate(
        query_normed * gain_query, cosine[:, :, None], sine_table[:, :, None]
    ).astype(BF16)
    key_rot = rotate(key_normed * gain_key, cosine, sine_table).astype(BF16)
    allowed = (segment[:, :, None] == segment[:, None, :]) & (
        positions[:, None, :] <= positions[:, :, None]
    )
    mixed_heads, log_total = attend(query_rot, key_rot, value_proj, allowed, score_scale)
    mixed_low = mixed_heads.reshape(lines * rows, Q_COLS).astype(BF16)
    projected = lax.psum_scatter(dot(mixed_low, weight_o), LINE, scatter_dimension=0, tiled=True)
    own_inputs = tokens.astype(F32)
    residual = own_inputs + projected
    ffn_scale = rms_scale(residual)
    ffn_normed = residual * ffn_scale
    hidden_two = (ffn_normed * gain_ffn).astype(BF16)

    hidden_all = lax.all_gather(hidden_two, ALL, axis=0, tiled=True)
    logits = dot(hidden_all, router)
    expert_ids = jnp.arange(experts, dtype=jnp.int32)
    picked = jnp.any(routes_all[:, :, None] == expert_ids, axis=1)
    masked = jnp.where(picked, logits, masked_score)
    exponent = jnp.where(picked, jnp.exp(masked - jnp.max(masked, axis=1, keepdims=True)), 0.0)
    weights_all = exponent / jnp.sum(exponent, axis=1, keepdims=True)
    mine = jnp.any(routes_all == me, axis=1).reshape(experts, rows)
    weight_mine = jnp.sum(jnp.where(expert_ids == me, weights_all, 0.0), axis=1).reshape(
        experts, rows
    )
    rank = jnp.cumsum(mine.astype(jnp.int32), axis=1) - 1
    slots = jnp.arange(capacity, dtype=jnp.int32)
    select = (rank[:, None, :] == slots[None, :, None]) & mine[:, None, :]
    select_low = select.astype(BF16)
    slot_weight = jnp.sum(jnp.where(select, weight_mine[:, None, :], 0.0), axis=2).reshape(-1, 1)

    def pick(values):
        return jnp.einsum(
            "sjt,std->sjd",
            select_low,
            values.reshape(experts, rows, D),
            preferred_element_type=F32,
        ).reshape(experts * capacity, D)

    def place(values):
        return (
            jnp.einsum(
                "sjt,sjd->std",
                select_low,
                values.reshape(experts, capacity, D),
                preferred_element_type=F32,
            )
            .astype(BF16)
            .reshape(experts * rows, D)
        )

    expert_rows = pick(hidden_all).astype(BF16)
    own_columns = lax.dynamic_slice_in_dim(hidden_all, me * own_rows, own_rows, axis=1)
    if large:
        expert_rows, own_columns, cotangent = lax.optimization_barrier(
            (expert_rows, own_columns, cotangent)
        )
    cotangent_all = lax.all_gather(cotangent, ALL, axis=0, tiled=True)
    grad_rows_out = pick(cotangent_all)
    grad_slots = (slot_weight * grad_rows_out).astype(BF16)
    gate_act = dot(expert_rows, gate_weight[0])
    up_act = dot(expert_rows, up_weight[0])
    gate_sig = jax.nn.sigmoid(gate_act)
    gate_silu = gate_act * gate_sig
    expert_hidden = (gate_silu * up_act).astype(BF16)
    grad_expert_hidden = dot(grad_slots, down_weight[0].T)
    grad_gate_act = (
        grad_expert_hidden * up_act * gate_sig * (1.0 + gate_act * (1.0 - gate_sig))
    ).astype(BF16)
    grad_up_act = (grad_expert_hidden * gate_silu).astype(BF16)
    grad_rows_in = (
        dot(grad_gate_act, gate_weight[0].T) + dot(grad_up_act, up_weight[0].T)
    ).astype(BF16)
    expert_out = dot(expert_hidden, down_weight[0]).astype(BF16).astype(F32)
    grad_weight_slot = jnp.sum(grad_rows_out * expert_out, axis=1).reshape(experts, capacity)
    grad_weight_mine = jnp.sum(jnp.where(select, grad_weight_slot[:, :, None], 0.0), axis=1)
    grad_weight = lax.all_gather(grad_weight_mine.reshape(-1), ALL, axis=0, tiled=False).T
    grad_rows_sum = lax.psum_scatter(place(grad_rows_in), ALL, scatter_dimension=0, tiled=True)
    if large:
        expert_out, grad_rows_sum = lax.optimization_barrier((expert_out, grad_rows_sum))
    out_sum = lax.psum_scatter(
        place((slot_weight * expert_out).astype(BF16)), ALL, scatter_dimension=0, tiled=True
    )
    block_out = (residual + out_sum.astype(F32)).astype(BF16)
    grad_down = dot(expert_hidden.T, grad_slots)
    grad_gate = dot(expert_rows.T, grad_gate_act)
    grad_up = dot(expert_rows.T, grad_up_act)

    grad_logits = weights_all * (
        grad_weight - jnp.sum(weights_all * grad_weight, axis=1, keepdims=True)
    )
    grad_logits = grad_logits.astype(BF16)
    router_grad = dot(own_columns.T, grad_logits)
    own_grad_logits = lax.dynamic_slice_in_dim(grad_logits, me * rows, rows, axis=0)

    grad_out = cotangent.astype(F32)
    grad_hidden_two = dot(own_grad_logits, router.T) + grad_rows_sum.astype(F32)
    grad_gain_ffn = jnp.sum(grad_hidden_two * ffn_normed, axis=0)
    grad_residual = grad_out + norm_back(grad_hidden_two * gain_ffn, ffn_normed, ffn_scale)
    grad_attn = lax.all_gather(grad_residual.astype(BF16), LINE, axis=0, tiled=True)
    output_part = dot(mixed_low.T, grad_attn).astype(BF16)
    output_grad = lax.psum_scatter(output_part, PLANE, scatter_dimension=0, tiled=True)
    grad_mixed = dot(grad_attn, weight_o.T).astype(BF16).reshape(lines, rows, GROUPS, HEAD_DIM)
    grad_query_rot, grad_key_rot, grad_value_rot = attend_back(
        query_rot, key_rot, value_proj, allowed, score_scale, log_total, grad_mixed
    )
    grad_value_proj = grad_value_rot.astype(BF16)
    grad_query_gained = rotate(grad_query_rot, cosine[:, :, None], -sine_table[:, :, None])
    grad_gain_query = jnp.sum(grad_query_gained * query_normed, axis=(0, 1, 2))
    grad_query_proj = norm_back(grad_query_gained * gain_query, query_normed, query_scale).astype(
        BF16
    )
    grad_key_gained = rotate(grad_key_rot, cosine, -sine_table)
    grad_gain_key = jnp.sum(grad_key_gained * key_normed, axis=(0, 1))
    grad_key_proj = norm_back(grad_key_gained * gain_key, key_normed, key_scale).astype(BF16)
    grad_proj = jnp.concatenate(
        [
            grad_query_proj.reshape(lines * rows, Q_COLS),
            grad_key_proj.reshape(lines * rows, HEAD_DIM),
            grad_value_proj.reshape(lines * rows, HEAD_DIM),
        ],
        axis=1,
    )
    grad_hidden_one = lax.psum_scatter(
        dot(grad_proj, weight_qkv.T), LINE, scatter_dimension=0, tiled=True
    )
    own_scale = rms_scale(own_inputs)
    own_normed = own_inputs * own_scale
    grad_gain_attn = jnp.sum(grad_hidden_one * own_normed, axis=0)
    input_grad = grad_residual + norm_back(grad_hidden_one * gain_attn, own_normed, own_scale)
    qkv_part = dot(hidden_one.T, grad_proj).astype(BF16).reshape(lines, cells, own_rows, width)
    qkv_part = qkv_part.transpose(1, 0, 2, 3).reshape(cells * lines * own_rows, width)
    qkv_part = lax.psum_scatter(qkv_part, PLANE, scatter_dimension=0, tiled=True)
    qkv_part = qkv_part.reshape(lines, own_rows, width)
    qkv_part = lax.all_to_all(qkv_part, LINE, split_axis=0, concat_axis=0, tiled=True)
    qkv_part = qkv_part.transpose(1, 0, 2).astype(F32)
    query_grad = qkv_part[:, :, :Q_COLS].reshape(own_rows, lines * Q_COLS)
    key_grad = qkv_part[:, :, Q_COLS : Q_COLS + HEAD_DIM].reshape(own_rows, lines * HEAD_DIM)
    value_grad = qkv_part[:, :, Q_COLS + HEAD_DIM :].reshape(own_rows, lines * HEAD_DIM)
    gains_local = jnp.concatenate([grad_gain_attn, grad_gain_ffn, grad_gain_query, grad_gain_key])
    gains_grad = lax.psum_scatter(gains_local, ALL, scatter_dimension=0, tiled=True)
    return (
        block_out,
        input_grad,
        query_grad,
        key_grad,
        value_grad,
        output_grad.astype(F32),
        router_grad,
        gains_grad,
        grad_gate[None],
        grad_up[None],
        grad_down[None],
    )


def solution(mesh):
    chips = mesh.shape["expert"]
    cores = mesh.shape["shard"]
    inner = Mesh(
        mesh.devices.reshape(KV_HEADS, chips // KV_HEADS, cores), ("line", "plane", "core")
    )
    return jax.shard_map(
        on_device,
        mesh=inner,
        in_specs=(
            P(ALL, None),
            P(ALL, None),
            P(ALL, None),
            P(ALL, None),
            P(ALL, None),
            P(ALL, None),
            P(ALL, None),
            P(ALL, None),
            P(ALL, None),
            P(ALL),
            P(ALL, None, None),
            P(ALL, None, None),
            P(ALL, None, None),
        ),
        out_specs=(
            P(ALL, None),
            P(ALL, None),
            P(ALL, None),
            P(ALL, None),
            P(ALL, None),
            P(ALL, None),
            P(ALL, None),
            P(ALL),
            P(ALL, None, None),
            P(ALL, None, None),
            P(ALL, None, None),
        ),
        check_vma=False,
    )
```

```python
import jax
import jax.numpy as jnp
from jax import lax
from jax.experimental import pallas as pl
from jax.experimental.pallas import tpu as pltpu
from jax.sharding import Mesh
from jax.sharding import PartitionSpec as P

D = 2048
HEADS = 32
KV_HEADS = 4
HEAD_DIM = 128
TOP = 8

epsilon = 1e-06
rope_base = 1000000.0
masked_score = -1e30

GROUPS = HEADS // KV_HEADS
Q_COLS = GROUPS * HEAD_DIM
LINE = "line"
PLANE = ("plane", "core")
ALL = ("line", "plane", "core")
F32 = jnp.float32
BF16 = jnp.bfloat16
MESH = pl.DeviceIdType.MESH
DMA = pltpu.SemaphoreType.DMA


def dot(left, right):
    return jnp.dot(left, right, preferred_element_type=F32)


def rms_scale(values):
    return lax.rsqrt(jnp.mean(values * values, axis=-1, keepdims=True) + epsilon)


def norm_back(upstream, normed, scale_rows):
    return scale_rows * (upstream - normed * jnp.mean(upstream * normed, axis=-1, keepdims=True))


def sequence_layout(lengths_row, row_count):
    seq_ends = jnp.cumsum(lengths_row)
    places = jnp.arange(row_count, dtype=jnp.int32)
    segment = jnp.sum((places[:, None] >= seq_ends[None, :]).astype(jnp.int32), axis=1)
    starts = seq_ends - lengths_row
    member = segment[:, None] == jnp.arange(lengths_row.shape[0], dtype=jnp.int32)[None, :]
    seg_start = jnp.sum(jnp.where(member, starts[None, :], 0), axis=1)
    return (segment, places - seg_start)


def rope_tables(positions, head_dim):
    half_dim = head_dim // 2
    inverse = rope_base ** (-2.0 * jnp.arange(half_dim, dtype=F32) / head_dim)
    angles = positions.astype(F32)[..., None] * inverse
    return (jnp.cos(angles), jnp.sin(angles))


def rotate(values, cosine, sine_table):
    half_dim = values.shape[-1] // 2
    first_half = values[..., :half_dim]
    second_half = values[..., half_dim:]
    return jnp.concatenate(
        [
            first_half * cosine - second_half * sine_table,
            second_half * cosine + first_half * sine_table,
        ],
        axis=-1,
    )


def masked_scores(query, keys, allowed, score_scale):
    scores = jnp.einsum("bqgd,bsd->bgqs", query, keys, preferred_element_type=F32) * score_scale
    return jnp.where(allowed[:, None], scores, masked_score)


def attend(query, keys, values_in, allowed, score_scale):
    scores = masked_scores(query, keys, allowed, score_scale)
    top_score = jnp.max(scores, axis=-1, keepdims=True)
    exponent = jnp.exp(scores - top_score)
    row_total = jnp.sum(exponent, axis=-1, keepdims=True)
    attn_probs = (exponent / row_total).astype(BF16)
    mixed_heads = jnp.einsum("bgqs,bsd->bqgd", attn_probs, values_in, preferred_element_type=F32)
    return (mixed_heads, top_score + jnp.log(row_total))


def attend_back(query, keys, values_in, allowed, score_scale, log_total, grad_mixed):
    scores = masked_scores(query, keys, allowed, score_scale)
    attn_probs = jnp.exp(scores - log_total)
    grad_probs = jnp.einsum("bqgd,bsd->bgqs", grad_mixed, values_in, preferred_element_type=F32)
    grad_scores = (
        attn_probs * (grad_probs - jnp.sum(attn_probs * grad_probs, axis=-1, keepdims=True))
    ).astype(BF16)
    grad_query = (
        jnp.einsum("bgqs,bsd->bqgd", grad_scores, keys, preferred_element_type=F32) * score_scale
    )
    grad_keys = (
        jnp.einsum("bgqs,bqgd->bsd", grad_scores, query, preferred_element_type=F32) * score_scale
    )
    grad_values = jnp.einsum(
        "bgqs,bqgd->bsd", attn_probs.astype(BF16), grad_mixed, preferred_element_type=F32
    )
    return (grad_query, grad_keys, grad_values)


class Spot:
    def __init__(self, lines):
        self.lines = lines
        self.z = lax.axis_index("line")
        self.b = lax.axis_index("plane")
        self.c = lax.axis_index("core")
        self.xn = self.b + 1 - 2 * (self.b % 2)
        self.yn = (self.b + 2) % 4
        self.dg = 3 - self.b

    def each(self, d, fn):
        if d == 0:
            fn(self.z, 0)
            return

        @pl.when(self.z - d >= 0)
        def _():
            fn(self.z - d, 1)

        @pl.when(self.z + d < self.lines)
        def _():
            fn(self.z + d, -1)

    def greet(self):
        sem = pltpu.get_barrier_semaphore()

        def tell(dev):
            pl.semaphore_signal(sem, inc=1, device_id=dev, device_id_type=MESH)

        tell((self.z, self.xn, self.c))
        tell((self.z, self.yn, self.c))
        tell((self.z, self.b, 1 - self.c))
        for d in range(1, self.lines):
            self.each(d, lambda zz, way: tell((zz, self.b, self.c)))
        pl.semaphore_wait(sem, self.lines + 2)


def send(src, dst, ssem, rsem, dev):
    return pltpu.make_async_remote_copy(
        src_ref=src, dst_ref=dst, send_sem=ssem, recv_sem=rsem, device_id=dev, device_id_type=MESH
    )


def gather_sems(mode, lines):
    n = 1 if mode == "plane" else lines
    return [DMA, DMA((2, n)), DMA((n,)), DMA((n, 8)), DMA((n, 8))]


def gather(spot, mode, x_ref, out_ref, sems):
    own_sem, zs, zr, ps, pr = sems
    z, b, c, xn, yn, dg, lines = spot.z, spot.b, spot.c, spot.xn, spot.yn, spot.dg, spot.lines
    here = (z, b, c)
    rows = out_ref.shape[-2]
    lo, hi = pl.ds(0, rows // 2), pl.ds(rows // 2, rows // 2)
    flat = mode == "plane"
    planar = mode != "line"
    steps = 1 if flat else lines

    def blk(zz, bb, cc=c):
        if flat:
            return out_ref.at[bb, cc]
        return out_ref.at[zz, bb, cc] if planar else out_ref.at[zz]

    mine = 0 if flat else z

    def each(d, fn):
        if flat:
            fn(0, 0)
        else:
            spot.each(d, fn)

    def own():
        return x_ref.at[z] if mode == "swap" else x_ref

    def source(zz, d):
        return own() if d == 0 else blk(zz, b)

    def hop(zz, way, d):
        return send(source(zz, d), blk(zz, b), zs.at[way, zz], zr.at[zz], (z + 1 - 2 * way, b, c))

    def plane_copies(zz, d):
        s = source(zz, d)
        return [
            send(s, blk(zz, b), ps.at[zz, 0], pr.at[zz, 0], (z, xn, c)),
            send(s, blk(zz, b), ps.at[zz, 1], pr.at[zz, 1], (z, yn, c)),
            send(s, blk(zz, b), ps.at[zz, 4], pr.at[zz, 4], (z, b, 1 - c)),
        ]

    def cross(zz, k):
        if k == 0:
            piece = blk(zz, yn).at[lo]
            return send(piece, piece, ps.at[zz, 2], pr.at[zz, 2], (z, xn, c))
        piece = blk(zz, xn).at[hi]
        return send(piece, piece, ps.at[zz, 3], pr.at[zz, 3], (z, yn, c))

    def share(zz, k):
        bb = (b, xn, yn, dg)[k]
        piece = blk(zz, bb)
        return send(piece, piece, ps.at[zz, 4 + k], pr.at[zz, 4 + k], (z, b, 1 - c))

    def received(piece, sem):
        send(piece, piece, own_sem, sem, here).wait_recv()

    def start():
        pltpu.make_async_copy(own(), blk(mine, b), own_sem).start()
        if mode in ("all", "line"):

            @pl.when(z < lines - 1)
            def _():
                hop(z, 0, 0).start()

            @pl.when(z > 0)
            def _():
                hop(z, 1, 0).start()

        if mode == "swap":
            for d in range(lines - 1, 0, -1):
                spot.each(
                    d,
                    lambda zz, way: send(
                        x_ref.at[zz], blk(z, b), zs.at[0, zz], zr.at[z], (zz, b, c)
                    ).start(),
                )
        if planar:
            for copy in plane_copies(mine, 0):
                copy.start()

    def line_arrive(zz, way):
        received(blk(zz, b), zr.at[zz])
        if mode in ("all", "line"):
            if way > 0:

                @pl.when(z < lines - 1)
                def _():
                    hop(zz, 0, 1).start()
            else:

                @pl.when(z > 0)
                def _():
                    hop(zz, 1, 1).start()

        if planar:
            for copy in plane_copies(zz, 1):
                copy.start()

    def plane_arrive(zz, way):
        received(blk(zz, xn), pr.at[zz, 0])
        cross(zz, 1).start()
        received(blk(zz, yn), pr.at[zz, 1])
        cross(zz, 0).start()
        share(zz, 1).start()
        share(zz, 2).start()

    def cross_arrive(zz, way):
        received(blk(zz, dg).at[lo], pr.at[zz, 2])
        received(blk(zz, dg).at[hi], pr.at[zz, 3])
        share(zz, 3).start()

    def drain(zz, way):
        if planar:
            for k, bb in enumerate((b, xn, yn, dg)):
                received(blk(zz, bb, 1 - c), pr.at[zz, 4 + k])
                share(zz, k).wait_send()
            for copy in plane_copies(zz, 1)[:2]:
                copy.wait_send()
            cross(zz, 0).wait_send()
            cross(zz, 1).wait_send()
        if mode in ("all", "line"):
            if way >= 0:

                @pl.when(z < lines - 1)
                def _():
                    hop(zz, 0, 1).wait_send()

            if way <= 0:

                @pl.when(z > 0)
                def _():
                    hop(zz, 1, 1).wait_send()

        if mode == "swap" and way != 0:
            send(x_ref.at[zz], blk(z, b), zs.at[0, zz], zr.at[z], (zz, b, c)).wait_send()

    start()
    yield
    for s in range(1, steps + 2):
        if s < steps:
            each(s, line_arrive)
        if planar and 0 <= s - 1 < steps:
            each(s - 1, plane_arrive)
        if planar and 0 <= s - 2 < steps:
            each(s - 2, cross_arrive)
        yield
    for d in range(steps):
        each(d, drain)
    pltpu.make_async_copy(own(), blk(mine, b), own_sem).wait()
    yield


def reduce_scratch(mode, lines, rows, cols, dtype=BF16):
    n = 1 if mode == "plane" else lines
    out = []
    if mode != "line":
        out += [
            pltpu.VMEM((n, 4, rows, cols), dtype),
            pltpu.VMEM((n, 2, rows // 2, cols), dtype),
            pltpu.VMEM((n, 2, rows, cols), dtype),
            DMA((n, 8)),
            DMA((n, 8)),
        ]
    if mode in ("all", "line"):
        out += [pltpu.VMEM((2, lines, rows, cols), dtype)]
    if mode != "plane":
        out += [DMA((2, lines)), DMA((2, lines))]
    if mode == "line":
        out += [pltpu.VMEM((lines, rows, cols), dtype)]
    return out


def add_into(dst, *parts, chunk=16):
    rows = dst.shape[0]

    @pl.loop(0, rows // chunk)
    def _(i):
        at = pl.ds(pl.multiple_of(i * chunk, chunk), chunk)
        total = parts[0][at].astype(F32)
        for part in parts[1:]:
            total = total + part[at].astype(F32)
        dst[at] = total.astype(dst.dtype)


def reduce(spot, mode, p_ref, out_ref, scratch):
    z, b, c, xn, yn, dg, lines = spot.z, spot.b, spot.c, spot.xn, spot.yn, spot.dg, spot.lines
    here = (z, b, c)
    flat = mode == "plane"
    planar = mode != "line"
    steps = 1 if flat else lines
    scratch = list(scratch)
    if planar:
        pair, crossed, met, ps, pr = scratch[:5]
        scratch = scratch[5:]
        rows = pair.shape[-2]
        lo, hi = pl.ds(0, rows // 2), pl.ds(rows // 2, rows // 2)
    if mode in ("all", "line"):
        passed = scratch.pop(0)
    if mode != "plane":
        zs, zr = scratch[:2]
        scratch = scratch[2:]
    if mode == "line":
        total_ref = scratch[0]

    def total(zz):
        return met.at[zz, 0] if planar else total_ref.at[zz]

    def term(zz, bb, cc):
        return p_ref.at[bb, cc] if flat else p_ref.at[zz, bb, cc]

    def each(d, fn):
        if flat:
            fn(0, 0)
        else:
            spot.each(d, fn)

    bbs = (dg, xn, yn, b)

    def share(zz, k):
        return send(
            term(zz, bbs[k], 1 - c), pair.at[zz, k], ps.at[zz, k], pr.at[zz, k], (z, b, 1 - c)
        )

    def cross(zz, k):
        piece = pair.at[zz, 0, (lo, hi)[k]]
        dev = (z, (yn, xn)[k], c)
        return send(piece, crossed.at[zz, k], ps.at[zz, 4 + k], pr.at[zz, 4 + k], dev)

    def meet(zz, k):
        dev = (z, (xn, yn)[k], c)
        return send(pair.at[zz, 1 + k], met.at[zz, k], ps.at[zz, 6 + k], pr.at[zz, 6 + k], dev)

    def hop(zz, way):
        return send(
            total(zz),
            passed.at[way, zz],
            zs.at[way, zz],
            zr.at[way, zz],
            (z + 1 - 2 * way, b, c),
        )

    def received(piece, sem):
        send(piece, piece, ps.at[0, 0] if planar else zs.at[0, 0], sem, here).wait_recv()

    def start(zz, way):
        for k in range(4):
            share(zz, k).start()

    def first(zz, way):
        for k in range(3):
            received(pair.at[zz, k], pr.at[zz, k])
            add_into(pair.at[zz, k], pair.at[zz, k], term(zz, bbs[k], c))
            if k == 0:
                cross(zz, 0).start()
                cross(zz, 1).start()

    def second(zz, way):
        received(crossed.at[zz, 0], pr.at[zz, 4])
        add_into(pair.at[zz, 1, lo], pair.at[zz, 1, lo], crossed.at[zz, 0])
        meet(zz, 0).start()
        received(crossed.at[zz, 1], pr.at[zz, 5])
        add_into(pair.at[zz, 2, hi], pair.at[zz, 2, hi], crossed.at[zz, 1])
        meet(zz, 1).start()

    def third(zz, way):
        received(pair.at[zz, 3], pr.at[zz, 3])
        received(met.at[zz, 0], pr.at[zz, 6])
        received(met.at[zz, 1], pr.at[zz, 7])
        dst = out_ref if flat else total(zz)
        add_into(dst, met.at[zz, 0], met.at[zz, 1], pair.at[zz, 3], term(zz, b, c))
        if mode == "swap" and way != 0:
            send(total(zz), out_ref.at[z], zs.at[0, zz], zr.at[0, z], (zz, b, c)).start()

    def line(zz, way):
        if way == 0:
            base = total(zz) if planar else p_ref.at[zz]
            both = (passed.at[0, zz], passed.at[1, zz])

            @pl.when(z > 0)
            def _():
                received(passed.at[0, zz], zr.at[0, zz])

            @pl.when(z < lines - 1)
            def _():
                received(passed.at[1, zz], zr.at[1, zz])

            @pl.when(z == 0)
            def _():
                add_into(out_ref, base, both[1])

            @pl.when(z == lines - 1)
            def _():
                add_into(out_ref, base, both[0])

            @pl.when((z > 0) & (z < lines - 1))
            def _():
                add_into(out_ref, base, both[0], both[1])

            return
        down = 1 if way > 0 else 0
        first_one = (z == lines - 1) if down else (z == 0)
        base = total(zz) if planar else p_ref.at[zz]

        @pl.when(jnp.logical_not(first_one))
        def _():
            received(passed.at[down, zz], zr.at[down, zz])
            add_into(total(zz), base, passed.at[down, zz])
            hop(zz, down).start()

        @pl.when(first_one)
        def _():
            if planar:
                hop(zz, down).start()
            else:
                send(
                    p_ref.at[zz],
                    passed.at[down, zz],
                    zs.at[down, zz],
                    zr.at[down, zz],
                    (z + 1 - 2 * down, b, c),
                ).start()

    order = list(range(steps - 1, -1, -1))
    if planar:
        for d in order:
            each(d, start)
    lag = (1, 2, 3, 4) if planar else (9, 9, 9, 1)
    yield
    for s in range(1, steps + 4):
        for fn, behind in zip((first, second, third, line), lag):
            i = s - behind
            if not 0 <= i < steps or behind > 8:
                continue
            if fn is line and mode not in ("all", "line"):
                continue
            each(order[i], fn)
        yield

    def drain(zz, way):
        if planar:
            for k in range(4):
                share(zz, k).wait_send()
            for k in range(2):
                cross(zz, k).wait_send()
                meet(zz, k).wait_send()
        if mode in ("all", "line") and way != 0:
            hop(zz, 1 if way > 0 else 0).wait_send()
        if mode == "swap" and way != 0:
            send(total(zz), out_ref.at[z], zs.at[0, zz], zr.at[0, z], (zz, b, c)).wait_send()
            received(out_ref.at[zz], zr.at[0, zz])

    for d in range(steps):
        each(d, drain)
    if mode == "swap":
        add_into(out_ref.at[z], total(z))
    yield


def run_steps(makers):
    live = list(makers)
    while live:
        for g in list(live):
            try:
                next(g)
            except StopIteration:
                live.remove(g)

def exchange(name, cid, jobs):
    lines = lax.axis_size("line")
    cells = lax.axis_size("plane") * lax.axis_size("core")
    if cells != 8 or lines != 4:
        return [exchange_by_xla(kind, mode, x, lines, cells) for kind, mode, x in jobs]
    in_specs, out_shapes, out_specs, scratch, counts = [], [], [], [], []
    for kind, mode, x in jobs:
        rows, cols = x.shape[-2:]
        space = pltpu.VMEM if kind == "reduce" else pl.ANY
        in_specs.append(pl.BlockSpec(memory_space=space))
        if kind == "gather":
            lead = {"line": (lines,), "plane": (4, 2)}.get(mode, (lines, 4, 2))
            out_shapes.append(jax.ShapeDtypeStruct((*lead, rows, cols), x.dtype))
            own = gather_sems(mode, lines)
        else:
            if mode == "swap":
                out_shapes.append(jax.ShapeDtypeStruct((lines, rows, cols), x.dtype))
            else:
                out_shapes.append(jax.ShapeDtypeStruct((rows, cols), F32))
            own = reduce_scratch(mode, lines, rows, cols, x.dtype)
        out_specs.append(pl.BlockSpec(memory_space=space))
        scratch += own
        counts.append(len(own))
    n = len(jobs)

    def body(*refs):
        spot = Spot(lines)
        spot.greet()
        at = 2 * n
        makers = []
        for i, (kind, mode, _) in enumerate(jobs):
            mine = refs[at : at + counts[i]]
            at += counts[i]
            fn = gather if kind == "gather" else reduce
            makers.append(fn(spot, mode, refs[i], refs[n + i], mine))
        run_steps(makers)

    return pl.pallas_call(
        body,
        out_shape=tuple(out_shapes),
        in_specs=in_specs,
        out_specs=tuple(out_specs),
        scratch_shapes=scratch,
        compiler_params=pltpu.CompilerParams(
            collective_id=cid, has_side_effects=True, vmem_limit_bytes=60 << 20
        ),
        name=name,
    )(*[x for _, _, x in jobs])


def exchange_by_xla(kind, mode, x, lines, cells):
    rows, cols = x.shape[-2:]
    if kind == "gather":
        if mode == "swap":
            x = lax.all_to_all(x, LINE, split_axis=0, concat_axis=0, tiled=True)
            return lax.all_gather(x, PLANE, axis=1)
        return lax.all_gather(x, {"line": LINE, "plane": PLANE, "all": ALL}[mode])
    if mode == "swap":
        x = x.reshape(lines, cells, rows, cols).transpose(1, 0, 2, 3)
        x = lax.psum_scatter(x, PLANE, scatter_dimension=0, tiled=True)
        x = x.reshape(lines, rows, cols)
        return lax.all_to_all(x, LINE, split_axis=0, concat_axis=0, tiled=True)
    x = x.reshape(-1, cols)
    axes = {"line": LINE, "plane": PLANE, "all": ALL}[mode]
    return lax.psum_scatter(x, axes, scatter_dimension=0, tiled=True).astype(F32)


def padded(flat, unit):
    size = -(-flat.shape[0] // unit) * unit
    return jnp.pad(flat, (0, size - flat.shape[0])).reshape(-1, 128)


def on_device(
    tokens,
    lengths,
    routes,
    cotangent,
    query_weight,
    key_weight,
    value_weight,
    output_weight,
    router_weight,
    norm_gains,
    gate_weight,
    up_weight,
    down_weight,
):
    rows = tokens.shape[0]
    lines = lax.axis_size("line")
    cells = lax.axis_size("plane") * lax.axis_size("core")
    experts = lines * cells
    capacity = (3 * rows * TOP + 2 * experts - 1) // (2 * experts)
    score_scale = HEAD_DIM ** (-0.5)
    large = experts > 32
    own_rows = query_weight.shape[0]
    line = lax.axis_index("line")
    me = (line * lax.axis_size("plane") + lax.axis_index("plane")) * lax.axis_size(
        "core"
    ) + lax.axis_index("core")

    packed = jnp.concatenate(
        [
            query_weight.reshape(own_rows, lines, Q_COLS),
            key_weight.reshape(own_rows, lines, HEAD_DIM),
            value_weight.reshape(own_rows, lines, HEAD_DIM),
        ],
        axis=2,
    ).transpose(1, 0, 2)
    width = packed.shape[2]
    floats = padded(jnp.concatenate([router_weight.reshape(-1), norm_gains]), 32 * 128)
    whole_numbers = padded(jnp.concatenate([routes.reshape(-1), lengths.reshape(-1)]), 16 * 128)
    floats_all, numbers_all, weight_qkv, line_tokens, weight_o = exchange(
        "gather_inputs",
        0,
        [
            ("gather", "all", floats),
            ("gather", "all", whole_numbers),
            ("gather", "swap", packed),
            ("gather", "line", tokens),
            ("gather", "plane", output_weight),
        ],
    )
    weight_qkv = weight_qkv.reshape(lines * cells * own_rows, width)
    weight_o = weight_o.reshape(cells * output_weight.shape[0], D)
    floats_all = floats_all.reshape(experts, -1)
    router_size = own_rows * experts
    router = floats_all[:, :router_size].reshape(D, experts)
    gains = floats_all[:, router_size : router_size + norm_gains.shape[0]].reshape(-1).astype(F32)
    numbers_all = numbers_all.reshape(experts, -1)
    routes_all = numbers_all[:, : rows * TOP].reshape(experts * rows, TOP)
    lengths_all = numbers_all[:, rows * TOP : rows * TOP + lengths.shape[1]]
    line_lengths = lax.dynamic_slice_in_dim(
        lengths_all.reshape(lines, cells, -1), me % cells, 1, axis=1
    )[:, 0]
    gain_attn = gains[:D]
    gain_ffn = gains[D : 2 * D]
    gain_query = gains[2 * D : 2 * D + HEAD_DIM]
    gain_key = gains[2 * D + HEAD_DIM :]

    inputs = line_tokens.reshape(lines * rows, D).astype(F32)
    attn_scale = rms_scale(inputs)
    attn_normed = inputs * attn_scale
    hidden_one = (attn_normed * gain_attn).astype(BF16)
    proj = dot(hidden_one, weight_qkv)
    query_proj = proj[:, :Q_COLS].reshape(lines, rows, GROUPS, HEAD_DIM)
    key_proj = proj[:, Q_COLS : Q_COLS + HEAD_DIM].reshape(lines, rows, HEAD_DIM)
    value_proj = proj[:, Q_COLS + HEAD_DIM :].astype(BF16).reshape(lines, rows, HEAD_DIM)
    query_scale = rms_scale(query_proj)
    query_normed = query_proj * query_scale
    key_scale = rms_scale(key_proj)
    key_normed = key_proj * key_scale
    segment, positions = jax.vmap(lambda row: sequence_layout(row, rows))(line_lengths)
    cosine, sine_table = rope_tables(positions, HEAD_DIM)
    query_rot = rotate(
        query_normed * gain_query, cosine[:, :, None], sine_table[:, :, None]
    ).astype(BF16)
    key_rot = rotate(key_normed * gain_key, cosine, sine_table).astype(BF16)
    allowed = (segment[:, :, None] == segment[:, None, :]) & (
        positions[:, None, :] <= positions[:, :, None]
    )
    mixed_heads, log_total = attend(query_rot, key_rot, value_proj, allowed, score_scale)
    mixed_low = mixed_heads.reshape(lines * rows, Q_COLS).astype(BF16)
    projected = dot(mixed_low, weight_o).astype(BF16).reshape(lines, rows, D)
    (projected,) = exchange("sum_residual", 1, [("reduce", "line", projected)])
    own_inputs = tokens.astype(F32)
    residual = own_inputs + projected
    ffn_scale = rms_scale(residual)
    ffn_normed = residual * ffn_scale
    hidden_two = (ffn_normed * gain_ffn).astype(BF16)

    (hidden_all,) = exchange("gather_hidden", 2, [("gather", "all", hidden_two)])
    hidden_all = hidden_all.reshape(experts * rows, D)
    logits = dot(hidden_all, router)
    expert_ids = jnp.arange(experts, dtype=jnp.int32)
    picked = jnp.any(routes_all[:, :, None] == expert_ids, axis=1)
    masked = jnp.where(picked, logits, masked_score)
    exponent = jnp.where(picked, jnp.exp(masked - jnp.max(masked, axis=1, keepdims=True)), 0.0)
    weights_all = exponent / jnp.sum(exponent, axis=1, keepdims=True)
    mine = jnp.any(routes_all == me, axis=1).reshape(experts, rows)
    weight_mine = jnp.sum(jnp.where(expert_ids == me, weights_all, 0.0), axis=1).reshape(
        experts, rows
    )
    rank = jnp.cumsum(mine.astype(jnp.int32), axis=1) - 1
    slots = jnp.arange(capacity, dtype=jnp.int32)
    select = (rank[:, None, :] == slots[None, :, None]) & mine[:, None, :]
    select_low = select.astype(BF16)
    slot_weight = jnp.sum(jnp.where(select, weight_mine[:, None, :], 0.0), axis=2).reshape(-1, 1)

    def pick(values):
        return jnp.einsum(
            "sjt,std->sjd",
            select_low,
            values.reshape(experts, rows, D),
            preferred_element_type=F32,
        ).reshape(experts * capacity, D)

    def place(values):
        return (
            jnp.einsum(
                "sjt,sjd->std",
                select_low,
                values.reshape(experts, capacity, D),
                preferred_element_type=F32,
            )
            .astype(BF16)
            .reshape(experts * rows, D)
        )

    expert_rows = pick(hidden_all).astype(BF16)
    own_columns = lax.dynamic_slice_in_dim(hidden_all, me * own_rows, own_rows, axis=1)
    if large:
        expert_rows, own_columns, cotangent = lax.optimization_barrier(
            (expert_rows, own_columns, cotangent)
        )
    cotangent_all = lax.all_gather(cotangent, ALL, axis=0, tiled=True)
    grad_rows_out = pick(cotangent_all)
    grad_slots = (slot_weight * grad_rows_out).astype(BF16)
    gate_act = dot(expert_rows, gate_weight[0])
    up_act = dot(expert_rows, up_weight[0])
    gate_sig = jax.nn.sigmoid(gate_act)
    gate_silu = gate_act * gate_sig
    expert_hidden = (gate_silu * up_act).astype(BF16)
    grad_expert_hidden = dot(grad_slots, down_weight[0].T)
    grad_gate_act = (
        grad_expert_hidden * up_act * gate_sig * (1.0 + gate_act * (1.0 - gate_sig))
    ).astype(BF16)
    grad_up_act = (grad_expert_hidden * gate_silu).astype(BF16)
    grad_rows_in = (
        dot(grad_gate_act, gate_weight[0].T) + dot(grad_up_act, up_weight[0].T)
    ).astype(BF16)
    expert_out = dot(expert_hidden, down_weight[0]).astype(BF16).astype(F32)
    grad_weight_slot = jnp.sum(grad_rows_out * expert_out, axis=1).reshape(experts, capacity)
    grad_weight_mine = jnp.sum(jnp.where(select, grad_weight_slot[:, :, None], 0.0), axis=1)
    placed = place(grad_rows_in).reshape(lines, -1, 2, rows, D)
    grad_weight, grad_rows_sum = exchange(
        "sum_rows",
        3,
        [
            ("gather", "all", grad_weight_mine.reshape(experts, rows)),
            ("reduce", "all", placed),
        ],
    )
    grad_weight = grad_weight.reshape(experts, experts * rows).T
    if large:
        expert_out, grad_rows_sum = lax.optimization_barrier((expert_out, grad_rows_sum))
    out_sum = lax.psum_scatter(
        place((slot_weight * expert_out).astype(BF16)), ALL, scatter_dimension=0, tiled=True
    )
    block_out = (residual + out_sum.astype(F32)).astype(BF16)
    grad_down = dot(expert_hidden.T, grad_slots)
    grad_gate = dot(expert_rows.T, grad_gate_act)
    grad_up = dot(expert_rows.T, grad_up_act)

    grad_logits = weights_all * (
        grad_weight - jnp.sum(weights_all * grad_weight, axis=1, keepdims=True)
    )
    grad_logits = grad_logits.astype(BF16)
    router_grad = dot(own_columns.T, grad_logits)
    own_grad_logits = lax.dynamic_slice_in_dim(grad_logits, me * rows, rows, axis=0)

    grad_out = cotangent.astype(F32)
    grad_hidden_two = dot(own_grad_logits, router.T) + grad_rows_sum.astype(F32)
    grad_gain_ffn = jnp.sum(grad_hidden_two * ffn_normed, axis=0)
    grad_residual = grad_out + norm_back(grad_hidden_two * gain_ffn, ffn_normed, ffn_scale)
    (grad_attn,) = exchange(
        "gather_grad", 4, [("gather", "line", grad_residual.astype(BF16))]
    )
    grad_attn = grad_attn.reshape(lines * rows, D)
    output_part = dot(mixed_low.T, grad_attn).astype(BF16)
    grad_mixed = dot(grad_attn, weight_o.T).astype(BF16).reshape(lines, rows, GROUPS, HEAD_DIM)
    grad_query_rot, grad_key_rot, grad_value_rot = attend_back(
        query_rot, key_rot, value_proj, allowed, score_scale, log_total, grad_mixed
    )
    grad_value_proj = grad_value_rot.astype(BF16)
    grad_query_gained = rotate(grad_query_rot, cosine[:, :, None], -sine_table[:, :, None])
    grad_gain_query = jnp.sum(grad_query_gained * query_normed, axis=(0, 1, 2))
    grad_query_proj = norm_back(grad_query_gained * gain_query, query_normed, query_scale).astype(
        BF16
    )
    grad_key_gained = rotate(grad_key_rot, cosine, -sine_table)
    grad_gain_key = jnp.sum(grad_key_gained * key_normed, axis=(0, 1))
    grad_key_proj = norm_back(grad_key_gained * gain_key, key_normed, key_scale).astype(BF16)
    grad_proj = jnp.concatenate(
        [
            grad_query_proj.reshape(lines * rows, Q_COLS),
            grad_key_proj.reshape(lines * rows, HEAD_DIM),
            grad_value_proj.reshape(lines * rows, HEAD_DIM),
        ],
        axis=1,
    )
    hidden_one_part = dot(grad_proj, weight_qkv.T)
    grad_gain_attn = jnp.sum(hidden_one_part * attn_normed, axis=0)
    qkv_part = dot(hidden_one.T, grad_proj).astype(BF16)
    gains_local = jnp.concatenate([grad_gain_attn, grad_gain_ffn, grad_gain_query, grad_gain_key])
    gains_all, grad_hidden_one, qkv_part, output_grad = exchange(
        "sum_gradients",
        5,
        [
            ("gather", "all", padded(gains_local, 16 * 128)),
            ("reduce", "line", hidden_one_part.astype(BF16).reshape(lines, rows, D)),
            ("reduce", "swap", qkv_part.reshape(lines, -1, 2, own_rows, width)),
            ("reduce", "plane", output_part.reshape(-1, 2, output_weight.shape[0], D)),
        ],
    )
    own_scale = rms_scale(own_inputs)
    own_normed = own_inputs * own_scale
    input_grad = grad_residual + norm_back(grad_hidden_one * gain_attn, own_normed, own_scale)
    qkv_part = qkv_part.transpose(1, 0, 2).astype(F32)
    query_grad = qkv_part[:, :, :Q_COLS].reshape(own_rows, lines * Q_COLS)
    key_grad = qkv_part[:, :, Q_COLS : Q_COLS + HEAD_DIM].reshape(own_rows, lines * HEAD_DIM)
    value_grad = qkv_part[:, :, Q_COLS + HEAD_DIM :].reshape(own_rows, lines * HEAD_DIM)
    share = norm_gains.shape[0]
    gains_all = gains_all.reshape(experts, -1)
    gains_all = lax.dynamic_slice_in_dim(gains_all, me * share, share, axis=1)
    gains_grad = jnp.sum(gains_all, axis=0)
    return (
        block_out,
        input_grad,
        query_grad,
        key_grad,
        value_grad,
        output_grad,
        router_grad,
        gains_grad,
        grad_gate[None],
        grad_up[None],
        grad_down[None],
    )


def solution(mesh):
    chips = mesh.shape["expert"]
    cores = mesh.shape["shard"]
    inner = Mesh(
        mesh.devices.reshape(KV_HEADS, chips // KV_HEADS, cores), ("line", "plane", "core")
    )
    return jax.shard_map(
        on_device,
        mesh=inner,
        in_specs=(
            P(ALL, None),
            P(ALL, None),
            P(ALL, None),
            P(ALL, None),
            P(ALL, None),
            P(ALL, None),
            P(ALL, None),
            P(ALL, None),
            P(ALL, None),
            P(ALL),
            P(ALL, None, None),
            P(ALL, None, None),
            P(ALL, None, None),
        ),
        out_specs=(
            P(ALL, None),
            P(ALL, None),
            P(ALL, None),
            P(ALL, None),
            P(ALL, None),
            P(ALL, None),
            P(ALL, None),
            P(ALL),
            P(ALL, None, None),
            P(ALL, None, None),
            P(ALL, None, None),
        ),
        check_vma=False,
    )
```

```python
import functools

import jax
import jax.numpy as jnp
from jax import lax
from jax.experimental import pallas as pl
from jax.experimental.pallas import tpu as pltpu
from jax.sharding import Mesh
from jax.sharding import PartitionSpec as P

D = 2048
HEADS = 32
KV_HEADS = 4
HEAD_DIM = 128
TOP = 8

epsilon = 1e-06
rope_base = 1000000.0
masked_score = -1e30

GROUPS = HEADS // KV_HEADS
Q_COLS = GROUPS * HEAD_DIM
LINE = "line"
PLANE = ("plane", "core")
ALL = ("line", "plane", "core")
F32 = jnp.float32
BF16 = jnp.bfloat16
MESH = pl.DeviceIdType.MESH
DMA = pltpu.SemaphoreType.DMA


def dot(left, right):
    return jnp.dot(left, right, preferred_element_type=F32)


def rms_scale(values):
    return lax.rsqrt(jnp.mean(values * values, axis=-1, keepdims=True) + epsilon)


def norm_back(upstream, normed, scale_rows):
    return scale_rows * (upstream - normed * jnp.mean(upstream * normed, axis=-1, keepdims=True))


def sequence_layout(lengths_row, row_count):
    seq_ends = jnp.cumsum(lengths_row)
    places = jnp.arange(row_count, dtype=jnp.int32)
    segment = jnp.sum((places[:, None] >= seq_ends[None, :]).astype(jnp.int32), axis=1)
    starts = seq_ends - lengths_row
    member = segment[:, None] == jnp.arange(lengths_row.shape[0], dtype=jnp.int32)[None, :]
    seg_start = jnp.sum(jnp.where(member, starts[None, :], 0), axis=1)
    return (segment, places - seg_start)


def rope_tables(positions, head_dim):
    half_dim = head_dim // 2
    inverse = rope_base ** (-2.0 * jnp.arange(half_dim, dtype=F32) / head_dim)
    angles = positions.astype(F32)[..., None] * inverse
    return (jnp.cos(angles), jnp.sin(angles))


def rotate(values, cosine, sine_table):
    half_dim = values.shape[-1] // 2
    first_half = values[..., :half_dim]
    second_half = values[..., half_dim:]
    return jnp.concatenate(
        [
            first_half * cosine - second_half * sine_table,
            second_half * cosine + first_half * sine_table,
        ],
        axis=-1,
    )


def masked_scores(query, keys, allowed, score_scale):
    scores = jnp.einsum("bqgd,bsd->bgqs", query, keys, preferred_element_type=F32) * score_scale
    return jnp.where(allowed[:, None], scores, masked_score)


def attend(query, keys, values_in, allowed, score_scale):
    scores = masked_scores(query, keys, allowed, score_scale)
    top_score = jnp.max(scores, axis=-1, keepdims=True)
    exponent = jnp.exp(scores - top_score)
    row_total = jnp.sum(exponent, axis=-1, keepdims=True)
    attn_probs = (exponent / row_total).astype(BF16)
    mixed_heads = jnp.einsum("bgqs,bsd->bqgd", attn_probs, values_in, preferred_element_type=F32)
    return (mixed_heads, top_score + jnp.log(row_total))


def attend_back(query, keys, values_in, allowed, score_scale, log_total, grad_mixed):
    scores = masked_scores(query, keys, allowed, score_scale)
    attn_probs = jnp.exp(scores - log_total)
    grad_probs = jnp.einsum("bqgd,bsd->bgqs", grad_mixed, values_in, preferred_element_type=F32)
    grad_scores = (
        attn_probs * (grad_probs - jnp.sum(attn_probs * grad_probs, axis=-1, keepdims=True))
    ).astype(BF16)
    grad_query = (
        jnp.einsum("bgqs,bsd->bqgd", grad_scores, keys, preferred_element_type=F32) * score_scale
    )
    grad_keys = (
        jnp.einsum("bgqs,bqgd->bsd", grad_scores, query, preferred_element_type=F32) * score_scale
    )
    grad_values = jnp.einsum(
        "bgqs,bqgd->bsd", attn_probs.astype(BF16), grad_mixed, preferred_element_type=F32
    )
    return (grad_query, grad_keys, grad_values)


class Spot:
    def __init__(self, lines):
        self.lines = lines
        self.z = lax.axis_index("line")
        self.b = lax.axis_index("plane")
        self.c = lax.axis_index("core")
        self.xn = self.b + 1 - 2 * (self.b % 2)
        self.yn = (self.b + 2) % 4
        self.dg = 3 - self.b

    def each(self, d, fn):
        if d == 0:
            fn(self.z, 0)
            return

        @pl.when(self.z - d >= 0)
        def _():
            fn(self.z - d, 1)

        @pl.when(self.z + d < self.lines)
        def _():
            fn(self.z + d, -1)

    def greet(self):
        sem = pltpu.get_barrier_semaphore()

        def tell(dev):
            pl.semaphore_signal(sem, inc=1, device_id=dev, device_id_type=MESH)

        tell((self.z, self.xn, self.c))
        tell((self.z, self.yn, self.c))
        tell((self.z, self.b, 1 - self.c))
        for d in range(1, self.lines):
            self.each(d, lambda zz, way: tell((zz, self.b, self.c)))
        pl.semaphore_wait(sem, self.lines + 2)


def send(src, dst, ssem, rsem, dev):
    return pltpu.make_async_remote_copy(
        src_ref=src, dst_ref=dst, send_sem=ssem, recv_sem=rsem, device_id=dev, device_id_type=MESH
    )


def gather_sems(mode, lines):
    n = 1 if mode == "plane" else lines
    return [DMA, DMA((2, n)), DMA((n,)), DMA((n, 8)), DMA((n, 8))]


def gather_parts(spot, x_ref, out_ref, sems, mode="all"):
    own_sem, zs, zr, ps, pr = sems
    z, b, c, xn, yn, dg, lines = spot.z, spot.b, spot.c, spot.xn, spot.yn, spot.dg, spot.lines
    here = (z, b, c)
    rows = out_ref.shape[-2]
    lo, hi = pl.ds(0, rows // 2), pl.ds(rows // 2, rows // 2)
    flat = mode == "plane"
    planar = mode != "line"
    steps = 1 if flat else lines

    def blk(zz, bb, cc=c):
        if flat:
            return out_ref.at[bb, cc]
        return out_ref.at[zz, bb, cc] if planar else out_ref.at[zz]

    mine = 0 if flat else z

    def each(d, fn):
        if flat:
            fn(0, 0)
        else:
            spot.each(d, fn)

    def own():
        return x_ref.at[z] if mode == "swap" else x_ref

    def source(zz, d):
        return own() if d == 0 else blk(zz, b)

    def hop(zz, way, d):
        return send(source(zz, d), blk(zz, b), zs.at[way, zz], zr.at[zz], (z + 1 - 2 * way, b, c))

    def plane_copies(zz, d):
        s = source(zz, d)
        return [
            send(s, blk(zz, b), ps.at[zz, 0], pr.at[zz, 0], (z, xn, c)),
            send(s, blk(zz, b), ps.at[zz, 1], pr.at[zz, 1], (z, yn, c)),
            send(s, blk(zz, b), ps.at[zz, 4], pr.at[zz, 4], (z, b, 1 - c)),
        ]

    def cross(zz, k):
        if k == 0:
            piece = blk(zz, yn).at[lo]
            return send(piece, piece, ps.at[zz, 2], pr.at[zz, 2], (z, xn, c))
        piece = blk(zz, xn).at[hi]
        return send(piece, piece, ps.at[zz, 3], pr.at[zz, 3], (z, yn, c))

    def share(zz, k):
        bb = (b, xn, yn, dg)[k]
        piece = blk(zz, bb)
        return send(piece, piece, ps.at[zz, 4 + k], pr.at[zz, 4 + k], (z, b, 1 - c))

    def received(piece, sem):
        send(piece, piece, own_sem, sem, here).wait_recv()

    def start():
        pltpu.make_async_copy(own(), blk(mine, b), own_sem).start()
        if mode in ("all", "line"):

            @pl.when(z < lines - 1)
            def _():
                hop(z, 0, 0).start()

            @pl.when(z > 0)
            def _():
                hop(z, 1, 0).start()

        if mode == "swap":
            for d in range(lines - 1, 0, -1):
                spot.each(
                    d,
                    lambda zz, way: send(
                        x_ref.at[zz], blk(z, b), zs.at[0, zz], zr.at[z], (zz, b, c)
                    ).start(),
                )
        if planar:
            for copy in plane_copies(mine, 0):
                copy.start()

    def line_arrive(zz, way):
        received(blk(zz, b), zr.at[zz])
        if mode in ("all", "line"):
            if way > 0:

                @pl.when(z < lines - 1)
                def _():
                    hop(zz, 0, 1).start()
            else:

                @pl.when(z > 0)
                def _():
                    hop(zz, 1, 1).start()

        if planar:
            for copy in plane_copies(zz, 1):
                copy.start()

    def plane_arrive(zz, way):
        received(blk(zz, xn), pr.at[zz, 0])
        cross(zz, 1).start()
        received(blk(zz, yn), pr.at[zz, 1])
        cross(zz, 0).start()
        share(zz, 1).start()
        share(zz, 2).start()

    def cross_arrive(zz, way):
        received(blk(zz, dg).at[lo], pr.at[zz, 2])
        received(blk(zz, dg).at[hi], pr.at[zz, 3])
        share(zz, 3).start()

    def drain(zz, way):
        if planar:
            for k in range(4):
                share(zz, k).wait_send()
            for copy in plane_copies(zz, 1)[:2]:
                copy.wait_send()
            cross(zz, 0).wait_send()
            cross(zz, 1).wait_send()
        if mode in ("all", "line"):
            if way >= 0:

                @pl.when(z < lines - 1)
                def _():
                    hop(zz, 0, 1).wait_send()

            if way <= 0:

                @pl.when(z > 0)
                def _():
                    hop(zz, 1, 1).wait_send()

        if mode == "swap" and way != 0:
            send(x_ref.at[zz], blk(z, b), zs.at[0, zz], zr.at[z], (zz, b, c)).wait_send()

    def shared(zz, k):
        received(blk(zz, (b, xn, yn, dg)[k], 1 - c), pr.at[zz, 4 + k])

    def end():
        pltpu.make_async_copy(own(), blk(mine, b), own_sem).wait()

    return {
        "start": start,
        "line": line_arrive,
        "plane": plane_arrive,
        "cross": cross_arrive,
        "shared": shared,
        "drain": drain,
        "end": end,
    }


def gather(spot, mode, x_ref, out_ref, sems):
    parts = gather_parts(spot, x_ref, out_ref, sems, mode)
    flat = mode == "plane"
    planar = mode != "line"
    steps = 1 if flat else spot.lines

    def each(d, fn):
        if flat:
            fn(0, 0)
        else:
            spot.each(d, fn)

    def drain(zz, way):
        if planar:
            for k in range(4):
                parts["shared"](zz, k)
        parts["drain"](zz, way)

    parts["start"]()
    yield
    for s in range(1, steps + 2):
        if s < steps:
            each(s, parts["line"])
        if planar and 0 <= s - 1 < steps:
            each(s - 1, parts["plane"])
        if planar and 0 <= s - 2 < steps:
            each(s - 2, parts["cross"])
        yield
    for d in range(steps):
        each(d, drain)
    parts["end"]()
    yield


def reduce_scratch(mode, lines, rows, cols, dtype=BF16):
    n = 1 if mode == "plane" else lines
    out = []
    if mode != "line":
        out += [
            pltpu.VMEM((n, 4, rows, cols), dtype),
            pltpu.VMEM((n, 2, rows // 2, cols), dtype),
            pltpu.VMEM((n, 2, rows, cols), dtype),
            DMA((n, 8)),
            DMA((n, 8)),
        ]
    if mode in ("all", "line"):
        out += [pltpu.VMEM((2, lines, rows, cols), dtype)]
    if mode != "plane":
        out += [DMA((2, lines)), DMA((2, lines))]
    if mode == "line":
        out += [pltpu.VMEM((lines, rows, cols), dtype)]
    if mode == "all":
        out += [pltpu.VMEM((n, 4, rows, cols), dtype), DMA]
    return out


def add_into(dst, *parts, chunk=16):
    rows = dst.shape[0]

    @pl.loop(0, rows // chunk)
    def _(i):
        at = pl.ds(pl.multiple_of(i * chunk, chunk), chunk)
        total = parts[0][at].astype(F32)
        for part in parts[1:]:
            total = total + part[at].astype(F32)
        dst[at] = total.astype(dst.dtype)


def reduce(spot, mode, p_ref, out_ref, scratch):
    z, b, c, xn, yn, dg, lines = spot.z, spot.b, spot.c, spot.xn, spot.yn, spot.dg, spot.lines
    here = (z, b, c)
    flat = mode == "plane"
    planar = mode != "line"
    steps = 1 if flat else lines
    scratch = list(scratch)
    if planar:
        pair, crossed, met, ps, pr = scratch[:5]
        scratch = scratch[5:]
        rows = pair.shape[-2]
        lo, hi = pl.ds(0, rows // 2), pl.ds(rows // 2, rows // 2)
    if mode in ("all", "line"):
        passed = scratch.pop(0)
    if mode != "plane":
        zs, zr = scratch[:2]
        scratch = scratch[2:]
    if mode == "line":
        total_ref = scratch[0]
    if mode == "all":
        kept, kept_sem = scratch

    def total(zz):
        return met.at[zz, 0] if planar else total_ref.at[zz]

    def term(zz, bb, cc):
        return p_ref.at[bb, cc] if flat else p_ref.at[zz, bb, cc]

    def each(d, fn):
        if flat:
            fn(0, 0)
        else:
            spot.each(d, fn)

    def kept_term(zz, bb):
        return kept.at[zz, bb] if mode == "all" else term(zz, bb, c)

    bbs = (dg, xn, yn, b)

    def share(zz, k):
        return send(
            term(zz, bbs[k], 1 - c), pair.at[zz, k], ps.at[zz, k], pr.at[zz, k], (z, b, 1 - c)
        )

    def cross(zz, k):
        piece = pair.at[zz, 0, (lo, hi)[k]]
        dev = (z, (yn, xn)[k], c)
        return send(piece, crossed.at[zz, k], ps.at[zz, 4 + k], pr.at[zz, 4 + k], dev)

    def meet(zz, k):
        dev = (z, (xn, yn)[k], c)
        return send(pair.at[zz, 1 + k], met.at[zz, k], ps.at[zz, 6 + k], pr.at[zz, 6 + k], dev)

    def hop(zz, way):
        return send(
            total(zz),
            passed.at[way, zz],
            zs.at[way, zz],
            zr.at[way, zz],
            (z + 1 - 2 * way, b, c),
        )

    def received(piece, sem):
        send(piece, piece, ps.at[0, 0] if planar else zs.at[0, 0], sem, here).wait_recv()

    def start(zz, way):
        for k in range(4):
            share(zz, k).start()

    def first(zz, way):
        for k in range(3):
            received(pair.at[zz, k], pr.at[zz, k])
            add_into(pair.at[zz, k], pair.at[zz, k], kept_term(zz, bbs[k]))
            if k == 0:
                cross(zz, 0).start()
                cross(zz, 1).start()

    def second(zz, way):
        received(crossed.at[zz, 0], pr.at[zz, 4])
        add_into(pair.at[zz, 1, lo], pair.at[zz, 1, lo], crossed.at[zz, 0])
        meet(zz, 0).start()
        received(crossed.at[zz, 1], pr.at[zz, 5])
        add_into(pair.at[zz, 2, hi], pair.at[zz, 2, hi], crossed.at[zz, 1])
        meet(zz, 1).start()

    def third(zz, way):
        received(pair.at[zz, 3], pr.at[zz, 3])
        received(met.at[zz, 0], pr.at[zz, 6])
        received(met.at[zz, 1], pr.at[zz, 7])
        dst = out_ref if flat else total(zz)
        add_into(dst, met.at[zz, 0], met.at[zz, 1], pair.at[zz, 3], kept_term(zz, b))
        if mode == "swap" and way != 0:
            send(total(zz), out_ref.at[z], zs.at[0, zz], zr.at[0, z], (zz, b, c)).start()

    def line(zz, way):
        if way == 0:
            base = total(zz) if planar else p_ref.at[zz]
            both = (passed.at[0, zz], passed.at[1, zz])

            @pl.when(z > 0)
            def _():
                received(passed.at[0, zz], zr.at[0, zz])

            @pl.when(z < lines - 1)
            def _():
                received(passed.at[1, zz], zr.at[1, zz])

            @pl.when(z == 0)
            def _():
                add_into(out_ref, base, both[1])

            @pl.when(z == lines - 1)
            def _():
                add_into(out_ref, base, both[0])

            @pl.when((z > 0) & (z < lines - 1))
            def _():
                add_into(out_ref, base, both[0], both[1])

            return
        down = 1 if way > 0 else 0
        first_one = (z == lines - 1) if down else (z == 0)
        base = total(zz) if planar else p_ref.at[zz]

        @pl.when(jnp.logical_not(first_one))
        def _():
            received(passed.at[down, zz], zr.at[down, zz])
            add_into(total(zz), base, passed.at[down, zz])
            hop(zz, down).start()

        @pl.when(first_one)
        def _():
            if planar:
                hop(zz, down).start()
            else:
                send(
                    p_ref.at[zz],
                    passed.at[down, zz],
                    zs.at[down, zz],
                    zr.at[down, zz],
                    (z + 1 - 2 * down, b, c),
                ).start()

    order = list(range(steps - 1, -1, -1))
    if planar:
        for d in order:
            each(d, start)
    if mode == "all":
        bring = pltpu.make_async_copy(p_ref.at[:, :, c], kept, kept_sem)
        bring.start()
        bring.wait()
    lag = (1, 2, 3, 4) if planar else (9, 9, 9, 1)
    yield
    for s in range(1, steps + 4):
        for fn, behind in zip((first, second, third, line), lag):
            i = s - behind
            if not 0 <= i < steps or behind > 8:
                continue
            if fn is line and mode not in ("all", "line"):
                continue
            each(order[i], fn)
        yield

    def drain(zz, way):
        if planar:
            for k in range(4):
                share(zz, k).wait_send()
            for k in range(2):
                cross(zz, k).wait_send()
                meet(zz, k).wait_send()
        if mode in ("all", "line") and way != 0:
            hop(zz, 1 if way > 0 else 0).wait_send()
        if mode == "swap" and way != 0:
            send(total(zz), out_ref.at[z], zs.at[0, zz], zr.at[0, z], (zz, b, c)).wait_send()
            received(out_ref.at[zz], zr.at[0, zz])

    for d in range(steps):
        each(d, drain)
    if mode == "swap":
        add_into(out_ref.at[z], total(z))
    yield


def run_steps(makers):
    live = list(makers)
    while live:
        for g in list(live):
            try:
                next(g)
            except StopIteration:
                live.remove(g)

def exchange(name, cid, jobs):
    lines = lax.axis_size("line")
    cells = lax.axis_size("plane") * lax.axis_size("core")
    if cells != 8 or lines != 4:
        return [exchange_by_xla(kind, mode, x, lines, cells) for kind, mode, x in jobs]
    in_specs, out_shapes, out_specs, scratch, counts = [], [], [], [], []
    for kind, mode, x in jobs:
        rows, cols = x.shape[-2:]
        space = pltpu.VMEM if kind == "reduce" else pl.ANY
        far = kind == "gather" or mode == "all"
        in_specs.append(pl.BlockSpec(memory_space=pl.ANY if far else pltpu.VMEM))
        if kind == "gather":
            lead = {"line": (lines,), "plane": (4, 2)}.get(mode, (lines, 4, 2))
            out_shapes.append(jax.ShapeDtypeStruct((*lead, rows, cols), x.dtype))
            own = gather_sems(mode, lines)
        else:
            if mode == "swap":
                out_shapes.append(jax.ShapeDtypeStruct((lines, rows, cols), x.dtype))
            else:
                out_shapes.append(jax.ShapeDtypeStruct((rows, cols), F32))
            own = reduce_scratch(mode, lines, rows, cols, x.dtype)
        out_specs.append(pl.BlockSpec(memory_space=space))
        scratch += own
        counts.append(len(own))
    n = len(jobs)

    def body(*refs):
        spot = Spot(lines)
        spot.greet()
        at = 2 * n
        makers = []
        for i, (kind, mode, _) in enumerate(jobs):
            mine = refs[at : at + counts[i]]
            at += counts[i]
            fn = gather if kind == "gather" else reduce
            makers.append(fn(spot, mode, refs[i], refs[n + i], mine))
        run_steps(makers)

    return pl.pallas_call(
        body,
        out_shape=tuple(out_shapes),
        in_specs=in_specs,
        out_specs=tuple(out_specs),
        scratch_shapes=scratch,
        compiler_params=pltpu.CompilerParams(
            collective_id=cid, has_side_effects=True, vmem_limit_bytes=60 << 20
        ),
        name=name,
    )(*[x for _, _, x in jobs])


def exchange_by_xla(kind, mode, x, lines, cells):
    rows, cols = x.shape[-2:]
    if kind == "gather":
        if mode == "swap":
            x = lax.all_to_all(x, LINE, split_axis=0, concat_axis=0, tiled=True)
            return lax.all_gather(x, PLANE, axis=1)
        return lax.all_gather(x, {"line": LINE, "plane": PLANE, "all": ALL}[mode])
    if mode == "swap":
        x = x.reshape(lines, cells, rows, cols).transpose(1, 0, 2, 3)
        x = lax.psum_scatter(x, PLANE, scatter_dimension=0, tiled=True)
        x = x.reshape(lines, rows, cols)
        return lax.all_to_all(x, LINE, split_axis=0, concat_axis=0, tiled=True)
    x = x.reshape(-1, cols)
    axes = {"line": LINE, "plane": PLANE, "all": ALL}[mode]
    return lax.psum_scatter(x, axes, scatter_dimension=0, tiled=True).astype(F32)


def padded(flat, unit):
    size = -(-flat.shape[0] // unit) * unit
    return jnp.pad(flat, (0, size - flat.shape[0])).reshape(-1, 128)


def pick_order(z, i):
    far = z // 2
    near = z * (1 - far) + (3 - z) * far
    place = (near + i) % 2 if i < 2 else i
    return place * (1 - far) + (3 - place) * far


def dot_nt(left, right):
    return lax.dot_general(left, right, (((1,), (1,)), ((), ())), preferred_element_type=F32)


def experts_body(capacity, experts, *refs):
    lines = 4
    (h_ref, t_ref, sel_ref, spread_ref, named_ref, router_ref, gate_ref, up_ref, down_ref) = refs[:9]
    (hall, tall, px, py, w_ref, dw_ref, x_out, dy_out, a_out, dg_out, du_out) = refs[9:20]
    rest = list(refs[20:])
    h_sems, t_sems = rest[:5], rest[5:10]
    (wg, wu, wd, hb, tb, xs, zs, dys, acts, dgs, dus, rs, ys, stage, slot_w, acc) = rest[10:26]
    (w_sem, l_sem, o_sem, p_sem) = rest[26:]
    spot = Spot(lines)
    z, b, c, xn, yn, dg_spot = spot.z, spot.b, spot.c, spot.xn, spot.yn, spot.dg
    me = (z * 4 + b) * 2 + c
    pair = 2 * capacity
    spot.greet()
    steps_h = gather_parts(spot, h_ref, hall, h_sems)
    steps_t = gather_parts(spot, t_ref, tall, t_sems)
    both = (steps_h, steps_t)
    columns = (b, xn, yn, dg_spot)
    loads = [
        pltpu.make_async_copy(gate_ref, wg, w_sem.at[0]),
        pltpu.make_async_copy(up_ref, wu, w_sem.at[1]),
        pltpu.make_async_copy(down_ref, wd, w_sem.at[2]),
    ]

    def comm(name, d):
        for s in both:
            spot.each(d, s[name])

    def load(i, k, n):
        zz, bb = pick_order(z, i), columns[k]
        return [
            pltpu.make_async_copy(hall.at[zz, bb], hb.at[n % 2], l_sem.at[0, n % 2]),
            pltpu.make_async_copy(tall.at[zz, bb], tb.at[n % 2], l_sem.at[1, n % 2]),
        ]

    def fetch(i, k, n):
        zz = pick_order(z, i)
        for s in both:
            s["shared"](zz, k)
        for copy in load(i, k, n):
            copy.start()

    def pick(i, k, n):
        zz, bb = pick_order(z, i), columns[k]
        at = pl.ds(pl.multiple_of(bb * pair, 16), pair)
        which = zz * 4 + bb
        for copy in load(i, k, n):
            copy.wait()
        rows = hb.shape[2]
        width = hb.shape[3]
        hidden = hb.at[n % 2]
        token = tb.at[n % 2]
        cols = pl.ds(pl.multiple_of(which * 2 * rows, 2 * rows), 2 * rows)
        logits = dot_nt(router_ref[...], hidden[...].reshape(2 * rows, width))
        named = named_ref[:, cols] > 0.5
        masked = jnp.where(named, logits, masked_score)
        top = jnp.max(masked, axis=0, keepdims=True)
        exponent = jnp.where(named, jnp.exp(masked - top), 0.0)
        weights = exponent / jnp.sum(exponent, axis=0, keepdims=True)
        w_ref[:, cols] = weights
        expert_row = lax.broadcasted_iota(jnp.int32, weights.shape, 0)
        mine = jnp.sum(jnp.where(expert_row == me, weights, 0.0), axis=0, keepdims=True)
        select = sel_ref[which]
        per_slot = jnp.sum(select.astype(F32) * mine, axis=1, keepdims=True)
        slot_w[i % 2, at, :] = jnp.broadcast_to(per_slot, (pair, 128))

        @pl.loop(0, width // 512)
        def _(j):
            part = pl.ds(pl.multiple_of(j * 512, 512), 512)
            h = hb[n % 2, :, :, part].reshape(2 * rows, 512)
            t = tb[n % 2, :, :, part].reshape(2 * rows, 512)
            xs[i % 2, at, part] = jnp.dot(select, h, preferred_element_type=F32).astype(BF16)
            t = jnp.dot(select, t, preferred_element_type=F32)
            zs[i % 2, at, part] = t.astype(BF16)
            dys[i % 2, at, part] = (per_slot * t).astype(BF16)

    def keep(i):
        zz = pick_order(z, i)
        q = i % 2
        return [
            pltpu.make_async_copy(xs.at[q], x_out.at[zz], o_sem.at[q, 0]),
            pltpu.make_async_copy(dys.at[q], dy_out.at[zz], o_sem.at[q, 1]),
            pltpu.make_async_copy(acts.at[q], a_out.at[zz], o_sem.at[q, 2]),
            pltpu.make_async_copy(dgs.at[q], dg_out.at[zz], o_sem.at[q, 3]),
            pltpu.make_async_copy(dus.at[q], du_out.at[zz], o_sem.at[q, 4]),
        ]

    def inner(i):
        q = i % 2

        @pl.loop(0, wg.shape[1] // 256)
        def _(j):
            part = pl.ds(pl.multiple_of(j * 256, 256), 256)
            g = jnp.dot(xs[q], wg[:, part], preferred_element_type=F32)
            u = jnp.dot(xs[q], wu[:, part], preferred_element_type=F32)
            da = dot_nt(dys[q], wd[part, :])
            sig = jax.nn.sigmoid(g)
            silu = g * sig
            acts[q, :, part] = (silu * u).astype(BF16)
            dgs[q, :, part] = (da * u * sig * (1.0 + g * (1.0 - sig))).astype(BF16)
            dus[q, :, part] = (da * silu).astype(BF16)

        for copy in keep(i):
            copy.start()

    def outer(i):
        q = i % 2
        acc[...] = jnp.zeros_like(acc)

        @pl.loop(0, wg.shape[0] // 256)
        def _(j):
            part = pl.ds(pl.multiple_of(j * 256, 256), 256)
            r = dot_nt(dgs[q], wg[part, :]) + dot_nt(dus[q], wu[part, :])
            rs[:, part] = r.astype(BF16)
            y = jnp.dot(acts[q], wd[:, part], preferred_element_type=F32)
            y = y.astype(BF16).astype(F32)
            met = y * zs[q, :, part].astype(F32)
            acc[...] += met[:, :128] + met[:, 128:]
            ys[:, part] = (slot_w[q, :, 0:1] * y).astype(BF16)

    def put(zz, bb, m):
        return [
            pltpu.make_async_copy(stage.at[m % 2, 0], px.at[zz, bb], p_sem.at[m % 2, 0]),
            pltpu.make_async_copy(stage.at[m % 2, 1], py.at[zz, bb], p_sem.at[m % 2, 1]),
        ]

    def place(i, k, m):
        zz, bb = pick_order(z, i), columns[k]
        at = pl.ds(pl.multiple_of(bb * pair, 16), pair)
        which = zz * 4 + bb
        if m >= 2:
            for copy in put(zz, bb, m):
                copy.wait()
        dw_slot = jnp.sum(acc[at, :], axis=1, keepdims=True)
        dw_ref[pl.ds(which, 1), :] = jnp.sum(
            sel_ref[which].astype(F32) * dw_slot, axis=0, keepdims=True
        )
        spread = spread_ref[which]
        rows = stage.shape[3]

        @pl.loop(0, rs.shape[1] // 512)
        def _(j):
            part = pl.ds(pl.multiple_of(j * 512, 512), 512)
            for n, src in enumerate((rs, ys)):
                full = jnp.dot(spread, src[at, part], preferred_element_type=F32)
                stage[m % 2, n, :, :, part] = full.astype(BF16).reshape(2, rows, 512)

        for copy in put(zz, bb, m):
            copy.start()

    for s in both:
        s["start"]()
    for copy in loads:
        copy.start()
    for s in both:
        s["end"]()
    fetch(0, 0, 0)
    comm("line", 1)
    comm("plane", 0)
    fetch(0, 1, 1)
    pick(0, 0, 0)
    fetch(0, 2, 2)
    pick(0, 1, 1)
    comm("line", 2)
    fetch(1, 0, 3)
    pick(0, 2, 2)
    comm("plane", 1)
    comm("cross", 0)
    fetch(0, 3, 4)
    pick(1, 0, 3)
    for copy in loads:
        copy.wait()
    fetch(1, 1, 5)
    pick(0, 3, 4)
    comm("line", 3)
    inner(0)
    comm("plane", 2)
    fetch(1, 2, 6)
    pick(1, 1, 5)
    outer(0)
    comm("cross", 1)
    fetch(1, 3, 7)
    pick(1, 2, 6)
    place(0, 0, 0)
    place(0, 1, 1)
    comm("plane", 3)
    place(0, 2, 2)
    place(0, 3, 3)
    pick(1, 3, 7)
    inner(1)
    for copy in keep(0):
        copy.wait()
    fetch(2, 0, 8)
    comm("cross", 2)
    fetch(2, 1, 9)
    pick(2, 0, 8)
    outer(1)
    fetch(2, 2, 10)
    pick(2, 1, 9)
    for k in range(4):
        place(1, k, 4 + k)
    comm("cross", 3)
    fetch(2, 3, 11)
    pick(2, 2, 10)
    fetch(3, 0, 12)
    pick(2, 3, 11)
    inner(2)
    for copy in keep(1):
        copy.wait()
    fetch(3, 1, 13)
    pick(3, 0, 12)
    outer(2)
    fetch(3, 2, 14)
    pick(3, 1, 13)
    for k in range(4):
        place(2, k, 8 + k)
    fetch(3, 3, 15)
    pick(3, 2, 14)
    pick(3, 3, 15)
    inner(3)
    outer(3)
    for k in range(4):
        place(3, k, 12 + k)
    for m in (0, 1):
        for copy in put(z, b, m):
            copy.wait()
    for i in (2, 3):
        for copy in keep(i):
            copy.wait()
    for d in range(lines):
        comm("drain", d)


def experts_call(hidden_two, cotangent, routes_all, router, gate, up, down, capacity):
    lines, experts = 4, 32
    rows, width = hidden_two.shape
    ff = gate.shape[1]
    pair = 2 * capacity
    group = 4 * pair
    me = (lax.axis_index("line") * 4 + lax.axis_index("plane")) * 2 + lax.axis_index("core")
    named = jnp.any(
        routes_all.T[:, None, :] == jnp.arange(experts, dtype=jnp.int32)[None, :, None], axis=0
    )
    mine = jnp.any(routes_all == me, axis=1).reshape(experts, rows)
    rank = jnp.cumsum(mine.astype(jnp.int32), axis=1) - 1
    slot = rank + (jnp.arange(experts, dtype=jnp.int32) % 2 * capacity)[:, None]
    slot = jnp.where(mine, slot, -1).reshape(experts // 2, 2 * rows)
    places = jnp.arange(pair, dtype=jnp.int32)
    select = (slot[:, None, :] == places[None, :, None]).astype(BF16)
    spread = (slot[:, :, None] == places[None, None, :]).astype(BF16)
    anywhere = pl.BlockSpec(memory_space=pl.ANY)
    near = pl.BlockSpec(memory_space=pltpu.VMEM)
    all_rows = jax.ShapeDtypeStruct((lines, 4, 2, rows, width), BF16)
    wide = jax.ShapeDtypeStruct((lines, group, width), BF16)
    thin = jax.ShapeDtypeStruct((lines, group, ff), BF16)
    return pl.pallas_call(
        functools.partial(experts_body, capacity, experts),
        out_shape=(
            all_rows,
            all_rows,
            all_rows,
            all_rows,
            jax.ShapeDtypeStruct((experts, experts * rows), F32),
            jax.ShapeDtypeStruct((experts // 2, 2 * rows), F32),
            wide,
            wide,
            thin,
            thin,
            thin,
        ),
        in_specs=[anywhere, anywhere, near, near, near, near, anywhere, anywhere, anywhere],
        out_specs=(*[anywhere] * 4, near, near, *[anywhere] * 5),
        scratch_shapes=[
            *gather_sems("all", lines),
            *gather_sems("all", lines),
            pltpu.VMEM((width, ff), BF16),
            pltpu.VMEM((width, ff), BF16),
            pltpu.VMEM((ff, width), BF16),
            pltpu.VMEM((2, 2, rows, width), BF16),
            pltpu.VMEM((2, 2, rows, width), BF16),
            pltpu.VMEM((2, group, width), BF16),
            pltpu.VMEM((2, group, width), BF16),
            pltpu.VMEM((2, group, width), BF16),
            pltpu.VMEM((2, group, ff), BF16),
            pltpu.VMEM((2, group, ff), BF16),
            pltpu.VMEM((2, group, ff), BF16),
            pltpu.VMEM((group, width), BF16),
            pltpu.VMEM((group, width), BF16),
            pltpu.VMEM((2, 2, 2, rows, width), BF16),
            pltpu.VMEM((2, group, 128), F32),
            pltpu.VMEM((group, 128), F32),
            DMA((3,)),
            DMA((2, 2)),
            DMA((2, 5)),
            DMA((2, 2)),
        ],
        compiler_params=pltpu.CompilerParams(
            collective_id=2, has_side_effects=True, vmem_limit_bytes=60 << 20
        ),
        name="experts",
    )(hidden_two, cotangent, select, spread, named.astype(F32), router.T, gate, up, down)


def experts_by_xla(hidden_two, cotangent, routes_all, router, gate, up, down, capacity, me, experts):
    rows = hidden_two.shape[0]
    hidden_all = lax.all_gather(hidden_two, ALL, axis=0, tiled=True)
    logits = dot(hidden_all, router)
    expert_ids = jnp.arange(experts, dtype=jnp.int32)
    picked = jnp.any(routes_all[:, :, None] == expert_ids, axis=1)
    masked = jnp.where(picked, logits, masked_score)
    exponent = jnp.where(picked, jnp.exp(masked - jnp.max(masked, axis=1, keepdims=True)), 0.0)
    weights_all = exponent / jnp.sum(exponent, axis=1, keepdims=True)
    mine = jnp.any(routes_all == me, axis=1).reshape(experts, rows)
    weight_mine = jnp.sum(jnp.where(expert_ids == me, weights_all, 0.0), axis=1).reshape(
        experts, rows
    )
    rank = jnp.cumsum(mine.astype(jnp.int32), axis=1) - 1
    slots = jnp.arange(capacity, dtype=jnp.int32)
    select = (rank[:, None, :] == slots[None, :, None]) & mine[:, None, :]
    select_low = select.astype(BF16)
    slot_weight = jnp.sum(jnp.where(select, weight_mine[:, None, :], 0.0), axis=2).reshape(-1, 1)

    def pick(values):
        return jnp.einsum(
            "sjt,std->sjd",
            select_low,
            values.reshape(experts, rows, D),
            preferred_element_type=F32,
        ).reshape(experts * capacity, D)

    def place(values):
        return (
            jnp.einsum(
                "sjt,sjd->std",
                select_low,
                values.reshape(experts, capacity, D),
                preferred_element_type=F32,
            )
            .astype(BF16)
            .reshape(experts * rows, D)
        )

    expert_rows = pick(hidden_all).astype(BF16)
    own_width = D // experts
    own_columns = lax.dynamic_slice_in_dim(hidden_all, me * own_width, own_width, axis=1)
    expert_rows, own_columns, cotangent = lax.optimization_barrier(
        (expert_rows, own_columns, cotangent)
    )
    cotangent_all = lax.all_gather(cotangent, ALL, axis=0, tiled=True)
    grad_rows_out = pick(cotangent_all)
    grad_slots = (slot_weight * grad_rows_out).astype(BF16)
    gate_act = dot(expert_rows, gate)
    up_act = dot(expert_rows, up)
    gate_sig = jax.nn.sigmoid(gate_act)
    gate_silu = gate_act * gate_sig
    expert_hidden = (gate_silu * up_act).astype(BF16)
    grad_expert_hidden = dot(grad_slots, down.T)
    grad_gate_act = (
        grad_expert_hidden * up_act * gate_sig * (1.0 + gate_act * (1.0 - gate_sig))
    ).astype(BF16)
    grad_up_act = (grad_expert_hidden * gate_silu).astype(BF16)
    grad_rows_in = (dot(grad_gate_act, gate.T) + dot(grad_up_act, up.T)).astype(BF16)
    expert_out = dot(expert_hidden, down).astype(BF16).astype(F32)
    grad_weight_slot = jnp.sum(grad_rows_out * expert_out, axis=1).reshape(experts, capacity)
    grad_weight_mine = jnp.sum(jnp.where(select, grad_weight_slot[:, :, None], 0.0), axis=1)
    out_rows = (slot_weight * expert_out).astype(BF16)

    def placed_out(after):
        return place(lax.optimization_barrier((out_rows, after))[0])

    return (
        own_columns,
        cotangent_all,
        place(grad_rows_in),
        placed_out,
        weights_all.T,
        grad_weight_mine,
        expert_rows,
        grad_slots,
        expert_hidden,
        grad_gate_act,
        grad_up_act,
    )


def on_device(
    tokens,
    lengths,
    routes,
    cotangent,
    query_weight,
    key_weight,
    value_weight,
    output_weight,
    router_weight,
    norm_gains,
    gate_weight,
    up_weight,
    down_weight,
):
    rows = tokens.shape[0]
    lines = lax.axis_size("line")
    cells = lax.axis_size("plane") * lax.axis_size("core")
    experts = lines * cells
    capacity = (3 * rows * TOP + 2 * experts - 1) // (2 * experts)
    score_scale = HEAD_DIM ** (-0.5)
    large = experts > 32
    own_rows = query_weight.shape[0]
    line = lax.axis_index("line")
    me = (line * lax.axis_size("plane") + lax.axis_index("plane")) * lax.axis_size(
        "core"
    ) + lax.axis_index("core")

    packed = jnp.concatenate(
        [
            query_weight.reshape(own_rows, lines, Q_COLS),
            key_weight.reshape(own_rows, lines, HEAD_DIM),
            value_weight.reshape(own_rows, lines, HEAD_DIM),
        ],
        axis=2,
    ).transpose(1, 0, 2)
    width = packed.shape[2]
    floats = padded(jnp.concatenate([router_weight.reshape(-1), norm_gains]), 32 * 128)
    whole_numbers = padded(jnp.concatenate([routes.reshape(-1), lengths.reshape(-1)]), 16 * 128)
    floats_all, numbers_all, weight_qkv, line_tokens, weight_o = exchange(
        "gather_inputs",
        0,
        [
            ("gather", "all", floats),
            ("gather", "all", whole_numbers),
            ("gather", "swap", packed),
            ("gather", "line", tokens),
            ("gather", "plane", output_weight),
        ],
    )
    weight_qkv = weight_qkv.reshape(lines * cells * own_rows, width)
    weight_o = weight_o.reshape(cells * output_weight.shape[0], D)
    floats_all = floats_all.reshape(experts, -1)
    router_size = own_rows * experts
    router = floats_all[:, :router_size].reshape(D, experts)
    gains = floats_all[:, router_size : router_size + norm_gains.shape[0]].reshape(-1).astype(F32)
    numbers_all = numbers_all.reshape(experts, -1)
    routes_all = numbers_all[:, : rows * TOP].reshape(experts * rows, TOP)
    lengths_all = numbers_all[:, rows * TOP : rows * TOP + lengths.shape[1]]
    line_lengths = lax.dynamic_slice_in_dim(
        lengths_all.reshape(lines, cells, -1), me % cells, 1, axis=1
    )[:, 0]
    gain_attn = gains[:D]
    gain_ffn = gains[D : 2 * D]
    gain_query = gains[2 * D : 2 * D + HEAD_DIM]
    gain_key = gains[2 * D + HEAD_DIM :]

    inputs = line_tokens.reshape(lines * rows, D).astype(F32)
    attn_scale = rms_scale(inputs)
    attn_normed = inputs * attn_scale
    hidden_one = (attn_normed * gain_attn).astype(BF16)
    proj = dot(hidden_one, weight_qkv)
    query_proj = proj[:, :Q_COLS].reshape(lines, rows, GROUPS, HEAD_DIM)
    key_proj = proj[:, Q_COLS : Q_COLS + HEAD_DIM].reshape(lines, rows, HEAD_DIM)
    value_proj = proj[:, Q_COLS + HEAD_DIM :].astype(BF16).reshape(lines, rows, HEAD_DIM)
    query_scale = rms_scale(query_proj)
    query_normed = query_proj * query_scale
    key_scale = rms_scale(key_proj)
    key_normed = key_proj * key_scale
    segment, positions = jax.vmap(lambda row: sequence_layout(row, rows))(line_lengths)
    cosine, sine_table = rope_tables(positions, HEAD_DIM)
    query_rot = rotate(
        query_normed * gain_query, cosine[:, :, None], sine_table[:, :, None]
    ).astype(BF16)
    key_rot = rotate(key_normed * gain_key, cosine, sine_table).astype(BF16)
    allowed = (segment[:, :, None] == segment[:, None, :]) & (
        positions[:, None, :] <= positions[:, :, None]
    )
    mixed_heads, log_total = attend(query_rot, key_rot, value_proj, allowed, score_scale)
    mixed_low = mixed_heads.reshape(lines * rows, Q_COLS).astype(BF16)
    projected = dot(mixed_low, weight_o).astype(BF16).reshape(lines, rows, D)
    (projected,) = exchange("sum_residual", 1, [("reduce", "line", projected)])
    own_inputs = tokens.astype(F32)
    residual = own_inputs + projected
    ffn_scale = rms_scale(residual)
    ffn_normed = residual * ffn_scale
    hidden_two = (ffn_normed * gain_ffn).astype(BF16)

    given = (hidden_two, cotangent, routes_all, router, gate_weight[0], up_weight[0], down_weight[0])
    if large:
        done = experts_by_xla(*given, capacity, me, experts)
    else:
        done = experts_call(*given, capacity)
    hidden_all, _, placed, placed_out, weights_all, grad_weight_mine = done[:6]
    expert_rows, grad_slots, expert_hidden, grad_gate_act, grad_up_act = [
        v.reshape(-1, v.shape[-1]) for v in done[6:]
    ]
    if large:
        own_columns = hidden_all
    else:
        hidden_all = hidden_all.reshape(experts * rows, D)
        own_columns = lax.dynamic_slice_in_dim(hidden_all, me * own_rows, own_rows, axis=1)
    grad_weight, grad_rows_sum = exchange(
        "sum_rows",
        3,
        [
            ("gather", "all", grad_weight_mine.reshape(experts, rows)),
            ("reduce", "all", placed.reshape(lines, -1, 2, rows, D)),
        ],
    )
    grad_weight = grad_weight.reshape(experts, experts * rows)
    if large:
        placed_out = placed_out(grad_rows_sum)
    else:
        placed_out, grad_rows_sum = lax.optimization_barrier((placed_out, grad_rows_sum))
    out_sum = lax.psum_scatter(
        placed_out.reshape(experts * rows, D), ALL, scatter_dimension=0, tiled=True
    )
    block_out = (residual + out_sum.astype(F32)).astype(BF16)
    grad_down = dot(expert_hidden.T, grad_slots)
    grad_gate = dot(expert_rows.T, grad_gate_act)
    grad_up = dot(expert_rows.T, grad_up_act)

    grad_logits = weights_all * (
        grad_weight - jnp.sum(weights_all * grad_weight, axis=0, keepdims=True)
    )
    grad_logits = grad_logits.astype(BF16)
    router_grad = lax.dot_general(
        own_columns, grad_logits, (((0,), (1,)), ((), ())), preferred_element_type=F32
    )
    own_grad_logits = lax.dynamic_slice_in_dim(grad_logits, me * rows, rows, axis=1).T

    grad_out = cotangent.astype(F32)
    grad_hidden_two = dot(own_grad_logits, router.T) + grad_rows_sum.astype(F32)
    grad_gain_ffn = jnp.sum(grad_hidden_two * ffn_normed, axis=0)
    grad_residual = grad_out + norm_back(grad_hidden_two * gain_ffn, ffn_normed, ffn_scale)
    (grad_attn,) = exchange(
        "gather_grad", 4, [("gather", "line", grad_residual.astype(BF16))]
    )
    grad_attn = grad_attn.reshape(lines * rows, D)
    output_part = dot(mixed_low.T, grad_attn).astype(BF16)
    grad_mixed = dot(grad_attn, weight_o.T).astype(BF16).reshape(lines, rows, GROUPS, HEAD_DIM)
    grad_query_rot, grad_key_rot, grad_value_rot = attend_back(
        query_rot, key_rot, value_proj, allowed, score_scale, log_total, grad_mixed
    )
    grad_value_proj = grad_value_rot.astype(BF16)
    grad_query_gained = rotate(grad_query_rot, cosine[:, :, None], -sine_table[:, :, None])
    grad_gain_query = jnp.sum(grad_query_gained * query_normed, axis=(0, 1, 2))
    grad_query_proj = norm_back(grad_query_gained * gain_query, query_normed, query_scale).astype(
        BF16
    )
    grad_key_gained = rotate(grad_key_rot, cosine, -sine_table)
    grad_gain_key = jnp.sum(grad_key_gained * key_normed, axis=(0, 1))
    grad_key_proj = norm_back(grad_key_gained * gain_key, key_normed, key_scale).astype(BF16)
    grad_proj = jnp.concatenate(
        [
            grad_query_proj.reshape(lines * rows, Q_COLS),
            grad_key_proj.reshape(lines * rows, HEAD_DIM),
            grad_value_proj.reshape(lines * rows, HEAD_DIM),
        ],
        axis=1,
    )
    hidden_one_part = dot(grad_proj, weight_qkv.T)
    grad_gain_attn = jnp.sum(hidden_one_part * attn_normed, axis=0)
    qkv_part = dot(hidden_one.T, grad_proj).astype(BF16)
    gains_local = jnp.concatenate([grad_gain_attn, grad_gain_ffn, grad_gain_query, grad_gain_key])
    gains_all, grad_hidden_one, qkv_part, output_grad = exchange(
        "sum_gradients",
        5,
        [
            ("gather", "all", padded(gains_local, 16 * 128)),
            ("reduce", "line", hidden_one_part.astype(BF16).reshape(lines, rows, D)),
            ("reduce", "swap", qkv_part.reshape(lines, -1, 2, own_rows, width)),
            ("reduce", "plane", output_part.reshape(-1, 2, output_weight.shape[0], D)),
        ],
    )
    own_scale = rms_scale(own_inputs)
    own_normed = own_inputs * own_scale
    input_grad = grad_residual + norm_back(grad_hidden_one * gain_attn, own_normed, own_scale)
    qkv_part = qkv_part.transpose(1, 0, 2).astype(F32)
    query_grad = qkv_part[:, :, :Q_COLS].reshape(own_rows, lines * Q_COLS)
    key_grad = qkv_part[:, :, Q_COLS : Q_COLS + HEAD_DIM].reshape(own_rows, lines * HEAD_DIM)
    value_grad = qkv_part[:, :, Q_COLS + HEAD_DIM :].reshape(own_rows, lines * HEAD_DIM)
    share = norm_gains.shape[0]
    gains_all = gains_all.reshape(experts, -1)
    gains_all = lax.dynamic_slice_in_dim(gains_all, me * share, share, axis=1)
    gains_grad = jnp.sum(gains_all, axis=0)
    return (
        block_out,
        input_grad,
        query_grad,
        key_grad,
        value_grad,
        output_grad,
        router_grad,
        gains_grad,
        grad_gate[None],
        grad_up[None],
        grad_down[None],
    )


def solution(mesh):
    chips = mesh.shape["expert"]
    cores = mesh.shape["shard"]
    inner = Mesh(
        mesh.devices.reshape(KV_HEADS, chips // KV_HEADS, cores), ("line", "plane", "core")
    )
    return jax.shard_map(
        on_device,
        mesh=inner,
        in_specs=(
            P(ALL, None),
            P(ALL, None),
            P(ALL, None),
            P(ALL, None),
            P(ALL, None),
            P(ALL, None),
            P(ALL, None),
            P(ALL, None),
            P(ALL, None),
            P(ALL),
            P(ALL, None, None),
            P(ALL, None, None),
            P(ALL, None, None),
        ),
        out_specs=(
            P(ALL, None),
            P(ALL, None),
            P(ALL, None),
            P(ALL, None),
            P(ALL, None),
            P(ALL, None),
            P(ALL, None),
            P(ALL),
            P(ALL, None, None),
            P(ALL, None, None),
            P(ALL, None, None),
        ),
        check_vma=False,
    )
```

```python
import functools

import jax
import jax.numpy as jnp
from jax import lax
from jax.experimental import pallas as pl
from jax.experimental.pallas import tpu as pltpu
from jax.sharding import Mesh
from jax.sharding import PartitionSpec as P

D = 2048
HEADS = 32
KV_HEADS = 4
HEAD_DIM = 128
TOP = 8

epsilon = 1e-06
rope_base = 1000000.0
masked_score = -1e30

GROUPS = HEADS // KV_HEADS
Q_COLS = GROUPS * HEAD_DIM
LINE = "line"
PLANE = ("plane", "core")
ALL = ("line", "plane", "core")
F32 = jnp.float32
BF16 = jnp.bfloat16
MESH = pl.DeviceIdType.MESH
DMA = pltpu.SemaphoreType.DMA


def dot(left, right):
    return jnp.dot(left, right, preferred_element_type=F32)


def rms_scale(values):
    return lax.rsqrt(jnp.mean(values * values, axis=-1, keepdims=True) + epsilon)


def norm_back(upstream, normed, scale_rows):
    return scale_rows * (upstream - normed * jnp.mean(upstream * normed, axis=-1, keepdims=True))


def sequence_layout(lengths_row, row_count):
    seq_ends = jnp.cumsum(lengths_row)
    places = jnp.arange(row_count, dtype=jnp.int32)
    segment = jnp.sum((places[:, None] >= seq_ends[None, :]).astype(jnp.int32), axis=1)
    starts = seq_ends - lengths_row
    member = segment[:, None] == jnp.arange(lengths_row.shape[0], dtype=jnp.int32)[None, :]
    seg_start = jnp.sum(jnp.where(member, starts[None, :], 0), axis=1)
    return (segment, places - seg_start)


def rope_tables(positions, head_dim):
    half_dim = head_dim // 2
    inverse = rope_base ** (-2.0 * jnp.arange(half_dim, dtype=F32) / head_dim)
    angles = positions.astype(F32)[..., None] * inverse
    return (jnp.cos(angles), jnp.sin(angles))


def rotate(values, cosine, sine_table):
    half_dim = values.shape[-1] // 2
    first_half = values[..., :half_dim]
    second_half = values[..., half_dim:]
    return jnp.concatenate(
        [
            first_half * cosine - second_half * sine_table,
            second_half * cosine + first_half * sine_table,
        ],
        axis=-1,
    )


def masked_scores(query, keys, allowed, score_scale):
    scores = jnp.einsum("bqgd,bsd->bgqs", query, keys, preferred_element_type=F32) * score_scale
    return jnp.where(allowed[:, None], scores, masked_score)


def attend(query, keys, values_in, allowed, score_scale):
    scores = masked_scores(query, keys, allowed, score_scale)
    top_score = jnp.max(scores, axis=-1, keepdims=True)
    exponent = jnp.exp(scores - top_score)
    row_total = jnp.sum(exponent, axis=-1, keepdims=True)
    attn_probs = (exponent / row_total).astype(BF16)
    mixed_heads = jnp.einsum("bgqs,bsd->bqgd", attn_probs, values_in, preferred_element_type=F32)
    return (mixed_heads, top_score + jnp.log(row_total))


def attend_back(query, keys, values_in, allowed, score_scale, log_total, grad_mixed):
    scores = masked_scores(query, keys, allowed, score_scale)
    attn_probs = jnp.exp(scores - log_total)
    grad_probs = jnp.einsum("bqgd,bsd->bgqs", grad_mixed, values_in, preferred_element_type=F32)
    grad_scores = (
        attn_probs * (grad_probs - jnp.sum(attn_probs * grad_probs, axis=-1, keepdims=True))
    ).astype(BF16)
    grad_query = (
        jnp.einsum("bgqs,bsd->bqgd", grad_scores, keys, preferred_element_type=F32) * score_scale
    )
    grad_keys = (
        jnp.einsum("bgqs,bqgd->bsd", grad_scores, query, preferred_element_type=F32) * score_scale
    )
    grad_values = jnp.einsum(
        "bgqs,bqgd->bsd", attn_probs.astype(BF16), grad_mixed, preferred_element_type=F32
    )
    return (grad_query, grad_keys, grad_values)


class Spot:
    def __init__(self, lines):
        self.lines = lines
        self.z = lax.axis_index("line")
        self.b = lax.axis_index("plane")
        self.c = lax.axis_index("core")
        self.xn = self.b + 1 - 2 * (self.b % 2)
        self.yn = (self.b + 2) % 4
        self.dg = 3 - self.b

    def each(self, d, fn):
        if d == 0:
            fn(self.z, 0)
            return

        @pl.when(self.z - d >= 0)
        def _():
            fn(self.z - d, 1)

        @pl.when(self.z + d < self.lines)
        def _():
            fn(self.z + d, -1)

    def greet(self):
        sem = pltpu.get_barrier_semaphore()

        def tell(dev):
            pl.semaphore_signal(sem, inc=1, device_id=dev, device_id_type=MESH)

        tell((self.z, self.xn, self.c))
        tell((self.z, self.yn, self.c))
        tell((self.z, self.b, 1 - self.c))
        for d in range(1, self.lines):
            self.each(d, lambda zz, way: tell((zz, self.b, self.c)))
        pl.semaphore_wait(sem, self.lines + 2)


def send(src, dst, ssem, rsem, dev):
    return pltpu.make_async_remote_copy(
        src_ref=src, dst_ref=dst, send_sem=ssem, recv_sem=rsem, device_id=dev, device_id_type=MESH
    )


def gather_sems(mode, lines):
    n = 1 if mode == "plane" else lines
    return [DMA, DMA((2, n)), DMA((n,)), DMA((n, 8)), DMA((n, 8)), DMA((2, n, 3)), DMA((n, 3))]


def gather_parts(spot, x_ref, out_ref, sems, mode="all", even=False):
    own_sem, zs, zr, ps, pr, vs, vr = sems
    z, b, c, xn, yn, dg, lines = spot.z, spot.b, spot.c, spot.xn, spot.yn, spot.dg, spot.lines
    here = (z, b, c)
    rows = out_ref.shape[-2]
    flat = mode == "plane"
    planar = mode != "line"
    relayed = mode in ("all", "line")
    via = rows // 4 if even else 0
    last = pl.ds(rows - via, via)
    columns = (b, xn, yn, dg)

    def span(way):
        return rows if way == 0 else rows - via

    def lo(way):
        return pl.ds(0, span(way) // 2)

    def hi(way):
        return pl.ds(span(way) // 2, span(way) // 2)

    def blk(zz, bb, cc=c):
        if flat:
            return out_ref.at[bb, cc]
        return out_ref.at[zz, bb, cc] if planar else out_ref.at[zz]

    mine = 0 if flat else z

    def own():
        return x_ref.at[z] if mode == "swap" else x_ref

    def source(zz, way):
        return own() if way == 0 else blk(zz, b)

    def onward(way, fn):
        if way >= 0:

            @pl.when(z < lines - 1)
            def _():
                fn(0)

        if way <= 0:

            @pl.when(z > 0)
            def _():
                fn(1)

    def hop(zz, down, way):
        return send(source(zz, way), blk(zz, b), zs.at[down, zz], zr.at[zz], (z + 1 - 2 * down, b, c))

    def hop_via(zz, k, down):
        piece = blk(zz, columns[k]).at[last]
        return send(
            piece, piece, vs.at[down, zz, k - 1], vr.at[zz, k - 1], (z + 1 - 2 * down, b, c)
        )

    def plane_copies(zz, way):
        s, d = source(zz, way), blk(zz, b)
        whole = (s, d)
        if via and way != 0:
            s, d = s.at[pl.ds(0, span(way))], d.at[pl.ds(0, span(way))]
        return [
            send(s, d, ps.at[zz, 0], pr.at[zz, 0], (z, xn, c)),
            send(s, d, ps.at[zz, 1], pr.at[zz, 1], (z, yn, c)),
            send(*whole, ps.at[zz, 4], pr.at[zz, 4], (z, b, 1 - c)),
        ]

    def cross(zz, k, way):
        if k == 0:
            piece = blk(zz, yn).at[lo(way)]
            return send(piece, piece, ps.at[zz, 2], pr.at[zz, 2], (z, xn, c))
        piece = blk(zz, xn).at[hi(way)]
        return send(piece, piece, ps.at[zz, 3], pr.at[zz, 3], (z, yn, c))

    def share(zz, k):
        piece = blk(zz, columns[k])
        return send(piece, piece, ps.at[zz, 4 + k], pr.at[zz, 4 + k], (z, b, 1 - c))

    def received(piece, sem):
        send(piece, piece, own_sem, sem, here).wait_recv()

    def over_line(zz, k, way):
        if not via:
            return
        if way != 0:
            received(blk(zz, columns[k]).at[last], vr.at[zz, k - 1])
        onward(way, lambda down: hop_via(zz, k, down).start())

    def start():
        pltpu.make_async_copy(own(), blk(mine, b), own_sem).start()
        if relayed:
            onward(0, lambda down: hop(z, down, 0).start())
        if mode == "swap":
            for d in range(lines - 1, 0, -1):
                spot.each(
                    d,
                    lambda zz, way: send(
                        x_ref.at[zz], blk(z, b), zs.at[0, zz], zr.at[z], (zz, b, c)
                    ).start(),
                )
        if planar:
            for copy in plane_copies(mine, 0):
                copy.start()

    def line_arrive(zz, way):
        received(blk(zz, b), zr.at[zz])
        if relayed:
            onward(way, lambda down: hop(zz, down, way).start())
        if planar:
            for copy in plane_copies(zz, way):
                copy.start()

    def plane_arrive(zz, way):
        part = pl.ds(0, span(way))
        received(blk(zz, xn).at[part], pr.at[zz, 0])
        cross(zz, 1, way).start()
        received(blk(zz, yn).at[part], pr.at[zz, 1])
        cross(zz, 0, way).start()
        over_line(zz, 1, way)
        over_line(zz, 2, way)
        share(zz, 1).start()
        share(zz, 2).start()

    def cross_arrive(zz, way):
        received(blk(zz, dg).at[lo(way)], pr.at[zz, 2])
        received(blk(zz, dg).at[hi(way)], pr.at[zz, 3])
        over_line(zz, 3, way)
        share(zz, 3).start()

    def drain(zz, way):
        if planar:
            for k in range(4):
                share(zz, k).wait_send()
            for copy in plane_copies(zz, way)[:2]:
                copy.wait_send()
            cross(zz, 0, way).wait_send()
            cross(zz, 1, way).wait_send()
        if relayed:
            onward(way, lambda down: hop(zz, down, way).wait_send())
        if via:
            for k in (1, 2, 3):
                onward(way, lambda down, k=k: hop_via(zz, k, down).wait_send())
        if mode == "swap" and way != 0:
            send(x_ref.at[zz], blk(z, b), zs.at[0, zz], zr.at[z], (zz, b, c)).wait_send()

    def shared(zz, k):
        received(blk(zz, columns[k], 1 - c), pr.at[zz, 4 + k])

    def end():
        pltpu.make_async_copy(own(), blk(mine, b), own_sem).wait()

    return {
        "start": start,
        "line": line_arrive,
        "plane": plane_arrive,
        "cross": cross_arrive,
        "shared": shared,
        "drain": drain,
        "end": end,
    }


def gather(spot, mode, x_ref, out_ref, sems):
    parts = gather_parts(spot, x_ref, out_ref, sems, mode)
    flat = mode == "plane"
    planar = mode != "line"
    steps = 1 if flat else spot.lines

    def each(d, fn):
        if flat:
            fn(0, 0)
        else:
            spot.each(d, fn)

    def drain(zz, way):
        if planar:
            for k in range(4):
                parts["shared"](zz, k)
        parts["drain"](zz, way)

    parts["start"]()
    yield
    for s in range(1, steps + 2):
        if s < steps:
            each(s, parts["line"])
        if planar and 0 <= s - 1 < steps:
            each(s - 1, parts["plane"])
        if planar and 0 <= s - 2 < steps:
            each(s - 2, parts["cross"])
        yield
    for d in range(steps):
        each(d, drain)
    parts["end"]()
    yield


def reduce_scratch(mode, lines, rows, cols, dtype=BF16):
    n = 1 if mode == "plane" else lines
    out = []
    if mode != "line":
        out += [
            pltpu.VMEM((n, 4, rows, cols), dtype),
            pltpu.VMEM((n, 2, rows // 2, cols), dtype),
            pltpu.VMEM((n, 2, rows, cols), dtype),
            DMA((n, 8)),
            DMA((n, 8)),
        ]
    if mode == "line":
        out += [pltpu.VMEM((2, lines, rows, cols), dtype), pltpu.VMEM((lines, rows, cols), dtype)]
    if mode == "all":
        out += [pltpu.VMEM((lines, rows, cols), dtype)]
    if mode != "plane":
        out += [DMA((2, lines)), DMA((2, lines))]
    return out


def add_into(dst, *parts, chunk=16):
    rows = dst.shape[0]

    @pl.loop(0, rows // chunk)
    def _(i):
        at = pl.ds(pl.multiple_of(i * chunk, chunk), chunk)
        total = parts[0][at].astype(F32)
        for part in parts[1:]:
            total = total + part[at].astype(F32)
        dst[at] = total.astype(dst.dtype)


def reduce_parts(spot, mode, term, out_ref, scratch):
    z, b, c, xn, yn = spot.z, spot.b, spot.c, spot.xn, spot.yn
    here = (z, b, c)
    scratch = list(scratch)
    pair, crossed, met, ps, pr = scratch[:5]
    passed = scratch[5] if mode == "all" else out_ref
    zs, zr = scratch[-2:]
    rows = pair.shape[-2]
    lo, hi = pl.ds(0, rows // 2), pl.ds(rows // 2, rows // 2)

    def total(zz):
        return met.at[zz, 0]

    def share(zz, k):
        return send(
            term(zz, k, 1 - c), pair.at[zz, k], ps.at[zz, k], pr.at[zz, k], (z, b, 1 - c)
        )

    def cross(zz, k):
        piece = pair.at[zz, 3, (lo, hi)[k]]
        dev = (z, (yn, xn)[k], c)
        return send(piece, crossed.at[zz, k], ps.at[zz, 4 + k], pr.at[zz, 4 + k], dev)

    def meet(zz, k):
        dev = (z, (xn, yn)[k], c)
        return send(pair.at[zz, 1 + k], met.at[zz, k], ps.at[zz, 6 + k], pr.at[zz, 6 + k], dev)

    def away(zz):
        return send(total(zz), passed.at[z], zs.at[0, zz], zr.at[0, z], (zz, b, c))

    def received(piece, sem):
        send(piece, piece, ps.at[0, 0], sem, here).wait_recv()

    def start(zz, way):
        for k in (3, 1, 2, 0):
            share(zz, k).start()

    def first(zz, way):
        for k in (3, 1, 2):
            received(pair.at[zz, k], pr.at[zz, k])
            add_into(pair.at[zz, k], pair.at[zz, k], term(zz, k, c))
            if k == 3:
                cross(zz, 0).start()
                cross(zz, 1).start()

    def second(zz, way):
        received(crossed.at[zz, 0], pr.at[zz, 4])
        add_into(pair.at[zz, 1, lo], pair.at[zz, 1, lo], crossed.at[zz, 0])
        meet(zz, 0).start()
        received(crossed.at[zz, 1], pr.at[zz, 5])
        add_into(pair.at[zz, 2, hi], pair.at[zz, 2, hi], crossed.at[zz, 1])
        meet(zz, 1).start()

    def third(zz, way):
        received(pair.at[zz, 0], pr.at[zz, 0])
        received(met.at[zz, 0], pr.at[zz, 6])
        received(met.at[zz, 1], pr.at[zz, 7])
        dst = out_ref if mode == "plane" else total(zz)
        add_into(dst, met.at[zz, 0], met.at[zz, 1], pair.at[zz, 0], term(zz, 0, c))
        if mode != "plane":

            @pl.when(zz != z)
            def _():
                away(zz).start()

    def end():
        if mode == "plane":
            return
        for d in range(1, spot.lines):
            spot.each(d, lambda zz, way: received(passed.at[zz], zr.at[0, zz]))
        if mode == "swap":
            add_into(out_ref.at[z], total(z))
            return
        for edge in range(spot.lines):

            @pl.when(z == edge)
            def _():
                others = [passed.at[q] for q in range(spot.lines) if q != edge]
                add_into(out_ref, total(edge), *others)

    def sent(zz, way):
        for k in range(4):
            share(zz, k).wait_send()

    def drain(zz, way):
        for k in range(2):
            cross(zz, k).wait_send()
            meet(zz, k).wait_send()
        if mode != "plane" and way != 0:
            away(zz).wait_send()

    return {
        "start": start,
        "first": first,
        "second": second,
        "third": third,
        "sent": sent,
        "end": end,
        "drain": drain,
    }


def reduce(spot, mode, p_ref, out_ref, scratch):
    flat = mode == "plane"
    steps = 1 if flat else spot.lines

    columns = (spot.b, spot.xn, spot.yn, spot.dg)

    def term(zz, k, cc):
        return p_ref.at[columns[k], cc] if flat else p_ref.at[zz, columns[k], cc]

    def each(d, fn):
        if flat:
            fn(0, 0)
        else:
            spot.each(d, fn)

    parts = reduce_parts(spot, mode, term, out_ref, scratch)
    order = list(range(steps - 1, -1, -1))
    for d in order:
        each(d, parts["start"])
    yield
    for s in range(steps + 2):
        for lag, name in enumerate(("first", "second", "third")):
            if 0 <= s - lag < steps:
                each(order[s - lag], parts[name])
        yield
    parts["end"]()
    for d in range(steps):
        each(d, parts["sent"])
        each(d, parts["drain"])
    yield


def reduce_line(spot, p_ref, out_ref, scratch):
    passed, total_ref, zs, zr = scratch
    z, b, c, lines = spot.z, spot.b, spot.c, spot.lines
    here = (z, b, c)

    def received(down, zz):
        piece = passed.at[down, zz]
        send(piece, piece, zs.at[0, 0], zr.at[down, zz], here).wait_recv()

    def hop(src, zz, down):
        return send(
            src.at[zz], passed.at[down, zz], zs.at[down, zz], zr.at[down, zz], (z + 1 - 2 * down, b, c)
        )

    def step(zz, way):
        down = 1 if way > 0 else 0
        first_one = (z == lines - 1) if down else (z == 0)

        @pl.when(jnp.logical_not(first_one))
        def _():
            received(down, zz)
            add_into(total_ref.at[zz], p_ref.at[zz], passed.at[down, zz])
            hop(total_ref, zz, down).start()

        @pl.when(first_one)
        def _():
            hop(p_ref, zz, down).start()

    for d in range(lines - 1, 0, -1):
        spot.each(d, step)
        yield

    @pl.when(z > 0)
    def _():
        received(0, z)

    @pl.when(z < lines - 1)
    def _():
        received(1, z)

    @pl.when(z == 0)
    def _():
        add_into(out_ref, p_ref.at[z], passed.at[1, z])

    @pl.when(z == lines - 1)
    def _():
        add_into(out_ref, p_ref.at[z], passed.at[0, z])

    @pl.when((z > 0) & (z < lines - 1))
    def _():
        add_into(out_ref, p_ref.at[z], passed.at[0, z], passed.at[1, z])

    for d in range(1, lines):
        spot.each(d, lambda zz, way: hop(total_ref, zz, 1 if way > 0 else 0).wait_send())
    yield


def dot_tn(left, right):
    return lax.dot_general(left, right, (((0,), (0,)), ((), ())), preferred_element_type=F32)


def products_scratch(count, width, ff):
    return [
        pltpu.VMEM((3, count, ff), BF16),
        pltpu.VMEM((2, count, 256), BF16),
        pltpu.VMEM((2, 2, 256, ff), F32),
        pltpu.VMEM((2, ff, 256), F32),
        DMA((3,)),
        DMA((2,)),
        DMA((2, 2)),
        DMA((2,)),
    ]


def products(ins, outs, scratch):
    x_ref, dy_ref, a_ref, dg_ref, du_ref = ins
    gate_out, up_out, down_out = outs
    near, tile, wide, tall, n_sem, t_sem, w_sem, d_sem = scratch
    half = x_ref.shape[1] // 256

    def columns(n):
        return pl.ds((n % half) * 256, 256)

    def load(n):
        src = x_ref if n < half else dy_ref
        return pltpu.make_async_copy(src.at[:, columns(n)], tile.at[n % 2], t_sem.at[n % 2])

    def store(n):
        q = n % 2
        if n < half:
            return [
                pltpu.make_async_copy(wide.at[q, 0], gate_out.at[columns(n)], w_sem.at[q, 0]),
                pltpu.make_async_copy(wide.at[q, 1], up_out.at[columns(n)], w_sem.at[q, 1]),
            ]
        return [pltpu.make_async_copy(tall.at[q], down_out.at[:, columns(n)], d_sem.at[q])]

    near_loads = [
        pltpu.make_async_copy(src, near.at[i], n_sem.at[i])
        for i, src in enumerate((a_ref, dg_ref, du_ref))
    ]
    for copy in near_loads:
        copy.start()
    load(0).start()
    yield
    for copy in near_loads:
        copy.wait()
    for n in range(2 * half):
        load(n).wait()
        if n + 1 < 2 * half:
            load(n + 1).start()
        if n % half >= 2:
            for copy in store(n - 2):
                copy.wait()
        q = n % 2
        if n < half:
            wide[q, 0] = dot_tn(tile[q], near[1])
            wide[q, 1] = dot_tn(tile[q], near[2])
        else:
            tall[q] = dot_tn(near[0], tile[q])
        for copy in store(n):
            copy.start()
        if n % 3 == 2:
            yield
    for n in (half - 2, half - 1, 2 * half - 2, 2 * half - 1):
        for copy in store(n):
            copy.wait()
    yield


def run_steps(makers):
    live = list(makers)
    while live:
        for g in list(live):
            try:
                next(g)
            except StopIteration:
                live.remove(g)

def exchange(name, cid, jobs):
    lines = lax.axis_size("line")
    cells = lax.axis_size("plane") * lax.axis_size("core")
    if cells != 8 or lines != 4:
        return [exchange_by_xla(kind, mode, x, lines, cells) for kind, mode, x in jobs]
    far, near = pl.BlockSpec(memory_space=pl.ANY), pl.BlockSpec(memory_space=pltpu.VMEM)
    args, in_specs, out_shapes, out_specs, scratch, counts = [], [], [], [], [], []
    for kind, mode, x in jobs:
        if kind == "products":
            width, ff = x[0].shape[1], x[2].shape[1]
            args += x
            in_specs += [far] * 5
            out_shapes += [jax.ShapeDtypeStruct((width, ff), F32)] * 2
            out_shapes.append(jax.ShapeDtypeStruct((ff, width), F32))
            out_specs += [far] * 3
            own = products_scratch(x[0].shape[0], width, ff)
            counts.append((5, 3, len(own)))
            scratch += own
            continue
        rows, cols = x.shape[-2:]
        spec = near if kind == "reduce" else far
        args.append(x)
        in_specs.append(spec)
        if kind == "gather":
            lead = {"line": (lines,), "plane": (4, 2)}.get(mode, (lines, 4, 2))
            out_shapes.append(jax.ShapeDtypeStruct((*lead, rows, cols), x.dtype))
            own = gather_sems(mode, lines)
        else:
            if mode == "swap":
                out_shapes.append(jax.ShapeDtypeStruct((lines, rows, cols), x.dtype))
            else:
                out_shapes.append(jax.ShapeDtypeStruct((rows, cols), F32))
            own = reduce_scratch(mode, lines, rows, cols, x.dtype)
        out_specs.append(spec)
        scratch += own
        counts.append((1, 1, len(own)))
    kinds = [(kind, mode) for kind, mode, _ in jobs]

    def body(*refs):
        spot = Spot(lines)
        spot.greet()
        ins, outs, rest = 0, len(args), len(args) + len(out_shapes)
        makers = []
        for (kind, mode), (n_in, n_out, n_rest) in zip(kinds, counts):
            i, o, w = refs[ins : ins + n_in], refs[outs : outs + n_out], refs[rest : rest + n_rest]
            ins, outs, rest = ins + n_in, outs + n_out, rest + n_rest
            if kind == "products":
                makers.append(products(i, o, w))
            elif kind == "gather":
                makers.append(gather(spot, mode, i[0], o[0], w))
            elif mode == "line":
                makers.append(reduce_line(spot, i[0], o[0], w))
            else:
                makers.append(reduce(spot, mode, i[0], o[0], w))
        run_steps(makers)

    outs = pl.pallas_call(
        body,
        out_shape=tuple(out_shapes),
        in_specs=in_specs,
        out_specs=tuple(out_specs),
        scratch_shapes=scratch,
        compiler_params=pltpu.CompilerParams(
            collective_id=cid, has_side_effects=True, vmem_limit_bytes=62 << 20
        ),
        name=name,
    )(*args)
    results, at = [], 0
    for _, n_out, _ in counts:
        results.append(outs[at] if n_out == 1 else outs[at : at + n_out])
        at += n_out
    return results


def exchange_by_xla(kind, mode, x, lines, cells):
    if kind == "products":
        hidden, grad_slots, acts, grad_gate, grad_up = x
        return dot(hidden.T, grad_gate), dot(hidden.T, grad_up), dot(acts.T, grad_slots)
    rows, cols = x.shape[-2:]
    if kind == "gather":
        if mode == "swap":
            x = lax.all_to_all(x, LINE, split_axis=0, concat_axis=0, tiled=True)
            return lax.all_gather(x, PLANE, axis=1)
        return lax.all_gather(x, {"line": LINE, "plane": PLANE, "all": ALL}[mode])
    if mode == "swap":
        x = x.reshape(lines, cells, rows, cols).transpose(1, 0, 2, 3)
        x = lax.psum_scatter(x, PLANE, scatter_dimension=0, tiled=True)
        x = x.reshape(lines, rows, cols)
        return lax.all_to_all(x, LINE, split_axis=0, concat_axis=0, tiled=True)
    x = x.reshape(-1, cols)
    axes = {"line": LINE, "plane": PLANE, "all": ALL}[mode]
    return lax.psum_scatter(x, axes, scatter_dimension=0, tiled=True).astype(F32)


def padded(flat, unit):
    size = -(-flat.shape[0] // unit) * unit
    return jnp.pad(flat, (0, size - flat.shape[0])).reshape(-1, 128)


def pick_order(z, i):
    far = z // 2
    near = z * (1 - far) + (3 - z) * far
    place = (near + i) % 2 if i < 2 else i
    return place * (1 - far) + (3 - place) * far


def dot_nt(left, right):
    return lax.dot_general(left, right, (((1,), (1,)), ((), ())), preferred_element_type=F32)


def experts_body(capacity, *refs):
    lines = 4
    (h_ref, tall, own_w_ref, sel_ref, spread_ref, gate_ref, up_ref, down_ref) = refs[:8]
    (hall, py, dw_all, w_ref, sum_ref, x_out, dy_out, a_out, dg_out, du_out) = refs[8:18]
    rest = list(refs[18:])
    h_sems, w_sems, dw_sems = rest[:7], rest[7:14], rest[14:21]
    sum_scratch = rest[21:29]
    (wg, wu, wd, hb, tb, xs, zs, dys, acts, dgs, dus, rs, ys) = rest[29:42]
    (stage, stage_y, slot_w, acc, dw_ref, w_sem, l_sem, o_sem, p_sem) = rest[42:]
    spot = Spot(lines)
    z, b, c, xn, yn, dg_spot = spot.z, spot.b, spot.c, spot.xn, spot.yn, spot.dg
    me = (z * 4 + b) * 2 + c
    pair = 2 * capacity
    spot.greet()
    steps_h = gather_parts(spot, h_ref, hall, h_sems, even=True)
    steps_w = gather_parts(spot, own_w_ref, w_ref, w_sems)
    steps_dw = gather_parts(spot, dw_ref, dw_all, dw_sems)
    both = (steps_w, steps_h)
    columns = (b, xn, yn, dg_spot)
    turn = [0]

    def term(zz, k, cc):
        return stage.at[turn[0] % 2, k, cc]

    steps_r = reduce_parts(spot, "all", term, sum_ref, sum_scratch)

    def sums(name, i):
        turn[0] = i
        steps_r[name](pick_order(z, i), 1)

    def comm_dw(name, d):
        spot.each(d, steps_dw[name])

    loads = [
        pltpu.make_async_copy(gate_ref, wg, w_sem.at[0]),
        pltpu.make_async_copy(up_ref, wu, w_sem.at[1]),
        pltpu.make_async_copy(down_ref, wd, w_sem.at[2]),
    ]

    def comm(*names):
        for s in both:
            for name in names:
                part, d = name.split()
                spot.each(int(d), s[part])

    def load(i, k, n):
        zz, bb = pick_order(z, i), columns[k]
        return [
            pltpu.make_async_copy(hall.at[zz, bb], hb.at[n % 2], l_sem.at[0, n % 2]),
            pltpu.make_async_copy(tall.at[zz, bb], tb.at[n % 2], l_sem.at[1, n % 2]),
        ]

    def fetch(i, k, n):
        zz = pick_order(z, i)
        for s in both:
            s["shared"](zz, k)
        for copy in load(i, k, n):
            copy.start()

    def pick(i, k, n):
        zz, bb = pick_order(z, i), columns[k]
        at = pl.ds(pl.multiple_of(bb * pair, 16), pair)
        which = zz * 4 + bb
        for copy in load(i, k, n):
            copy.wait()
        rows = hb.shape[2]
        width = hb.shape[3]
        mine = jnp.concatenate(
            [w_ref[zz, bb, 0, pl.ds(me, 1), :], w_ref[zz, bb, 1, pl.ds(me, 1), :]], axis=1
        )
        select = sel_ref[which]
        per_slot = jnp.sum(select.astype(F32) * mine, axis=1, keepdims=True)
        slot_w[i % 2, at, :] = jnp.broadcast_to(per_slot, (pair, 128))

        @pl.loop(0, width // 512)
        def _(j):
            part = pl.ds(pl.multiple_of(j * 512, 512), 512)
            h = hb[n % 2, :, :, part].reshape(2 * rows, 512)
            t = tb[n % 2, :, :, part].reshape(2 * rows, 512)
            xs[i % 2, at, part] = jnp.dot(select, h, preferred_element_type=F32).astype(BF16)
            t = jnp.dot(select, t, preferred_element_type=F32)
            zs[i % 2, at, part] = t.astype(BF16)
            dys[i % 2, at, part] = (per_slot * t).astype(BF16)

    def keep(i):
        zz = pick_order(z, i)
        q = i % 2
        return [
            pltpu.make_async_copy(xs.at[q], x_out.at[zz], o_sem.at[q, 0]),
            pltpu.make_async_copy(dys.at[q], dy_out.at[zz], o_sem.at[q, 1]),
            pltpu.make_async_copy(acts.at[q], a_out.at[zz], o_sem.at[q, 2]),
            pltpu.make_async_copy(dgs.at[q], dg_out.at[zz], o_sem.at[q, 3]),
            pltpu.make_async_copy(dus.at[q], du_out.at[zz], o_sem.at[q, 4]),
        ]

    def inner(i):
        q = i % 2

        @pl.loop(0, wg.shape[1] // 256)
        def _(j):
            part = pl.ds(pl.multiple_of(j * 256, 256), 256)
            g = jnp.dot(xs[q], wg[:, part], preferred_element_type=F32)
            u = jnp.dot(xs[q], wu[:, part], preferred_element_type=F32)
            da = dot_nt(dys[q], wd[part, :])
            sig = jax.nn.sigmoid(g)
            silu = g * sig
            acts[q, :, part] = (silu * u).astype(BF16)
            dgs[q, :, part] = (da * u * sig * (1.0 + g * (1.0 - sig))).astype(BF16)
            dus[q, :, part] = (da * silu).astype(BF16)

        for copy in keep(i):
            copy.start()

    def outer(i):
        q = i % 2
        acc[...] = jnp.zeros_like(acc)

        @pl.loop(0, wg.shape[0] // 256)
        def _(j):
            part = pl.ds(pl.multiple_of(j * 256, 256), 256)
            r = dot_nt(dgs[q], wg[part, :]) + dot_nt(dus[q], wu[part, :])
            rs[:, part] = r.astype(BF16)
            y = jnp.dot(acts[q], wd[:, part], preferred_element_type=F32)
            y = y.astype(BF16).astype(F32)
            met = y * zs[q, :, part].astype(F32)
            acc[...] += met[:, :128] + met[:, 128:]
            ys[:, part] = (slot_w[q, :, 0:1] * y).astype(BF16)

    def put(zz, bb, m):
        return pltpu.make_async_copy(stage_y.at[m % 2], py.at[zz, bb], p_sem.at[m % 2])

    def place(i, k, m):
        zz, bb = pick_order(z, i), columns[k]
        at = pl.ds(pl.multiple_of(bb * pair, 16), pair)
        which = zz * 4 + bb
        if m >= 2:
            put(zz, bb, m).wait()
        dw_slot = jnp.sum(acc[at, :], axis=1, keepdims=True)
        dw_ref[pl.ds(which, 1), :] = jnp.sum(
            sel_ref[which].astype(F32) * dw_slot, axis=0, keepdims=True
        )
        spread = spread_ref[which]
        rows = stage.shape[3]

        @pl.loop(0, rs.shape[1] // 512)
        def _(j):
            part = pl.ds(pl.multiple_of(j * 512, 512), 512)
            full = jnp.dot(spread, rs[at, part], preferred_element_type=F32)
            stage[i % 2, k, :, :, part] = full.astype(BF16).reshape(2, rows, 512)
            full = jnp.dot(spread, ys[at, part], preferred_element_type=F32)
            stage_y[m % 2, :, :, part] = full.astype(BF16).reshape(2, rows, 512)

        put(zz, bb, m).start()

    def places(i):
        for n, k in enumerate((3, 1, 2, 0)):
            place(i, k, 4 * i + n)

    for s in both:
        s["start"]()
    for copy in loads:
        copy.start()
    for s in both:
        s["end"]()
    fetch(0, 0, 0)
    comm("line 1", "plane 0")
    fetch(0, 1, 1)
    pick(0, 0, 0)
    fetch(0, 2, 2)
    pick(0, 1, 1)
    comm("line 2", "plane 1", "cross 0")
    fetch(1, 0, 3)
    pick(0, 2, 2)
    fetch(0, 3, 4)
    pick(1, 0, 3)
    for copy in loads:
        copy.wait()
    fetch(1, 1, 5)
    pick(0, 3, 4)
    inner(0)
    comm("line 3", "plane 2", "cross 1")
    fetch(1, 2, 6)
    pick(1, 1, 5)
    outer(0)
    fetch(1, 3, 7)
    pick(1, 2, 6)
    places(0)
    comm("plane 3")
    pick(1, 3, 7)
    sums("start", 0)
    inner(1)
    for copy in keep(0):
        copy.wait()
    fetch(2, 0, 8)
    comm("cross 2")
    fetch(2, 1, 9)
    pick(2, 0, 8)
    sums("first", 0)
    outer(1)
    fetch(2, 2, 10)
    pick(2, 1, 9)
    sums("second", 0)
    places(1)
    comm("cross 3")
    fetch(2, 3, 11)
    pick(2, 2, 10)
    sums("start", 1)
    fetch(3, 0, 12)
    pick(2, 3, 11)
    inner(2)
    for copy in keep(1):
        copy.wait()
    sums("third", 0)
    fetch(3, 1, 13)
    pick(3, 0, 12)
    sums("first", 1)
    outer(2)
    fetch(3, 2, 14)
    pick(3, 1, 13)
    sums("second", 1)
    sums("sent", 0)
    places(2)
    fetch(3, 3, 15)
    pick(3, 2, 14)
    sums("start", 2)
    pick(3, 3, 15)
    sums("third", 1)
    inner(3)
    sums("first", 2)
    outer(3)
    sums("second", 2)
    sums("sent", 1)
    places(3)
    steps_dw["start"]()
    sums("start", 3)
    sums("third", 2)
    comm_dw("line", 1)
    comm_dw("plane", 0)
    sums("first", 3)
    comm_dw("line", 2)
    comm_dw("plane", 1)
    comm_dw("cross", 0)
    sums("second", 3)
    comm_dw("line", 3)
    comm_dw("plane", 2)
    comm_dw("cross", 1)
    comm_dw("plane", 3)
    comm_dw("cross", 2)
    comm_dw("cross", 3)
    sums("third", 3)
    steps_r["end"]()
    for m in (0, 1):
        put(z, b, m).wait()
    for i in (2, 3):
        for copy in keep(i):
            copy.wait()
        sums("sent", i)
    for d in range(lines):
        comm(f"drain {d}")
        comm_dw("drain", d)
        spot.each(d, steps_r["drain"])
        for k in range(4):
            spot.each(d, lambda zz, way, k=k: steps_dw["shared"](zz, k))
    steps_dw["end"]()


def experts_call(hidden_two, cotangent_all, own_weights, routes_all, gate, up, down, capacity):
    lines, experts = 4, 32
    rows, width = hidden_two.shape
    ff = gate.shape[1]
    pair = 2 * capacity
    group = 4 * pair
    me = (lax.axis_index("line") * 4 + lax.axis_index("plane")) * 2 + lax.axis_index("core")
    mine = jnp.any(routes_all == me, axis=1).reshape(experts, rows)
    rank = jnp.cumsum(mine.astype(jnp.int32), axis=1) - 1
    slot = rank + (jnp.arange(experts, dtype=jnp.int32) % 2 * capacity)[:, None]
    slot = jnp.where(mine, slot, -1).reshape(experts // 2, 2 * rows)
    places = jnp.arange(pair, dtype=jnp.int32)
    select = (slot[:, None, :] == places[None, :, None]).astype(BF16)
    spread = (slot[:, :, None] == places[None, None, :]).astype(BF16)
    anywhere = pl.BlockSpec(memory_space=pl.ANY)
    near = pl.BlockSpec(memory_space=pltpu.VMEM)
    all_rows = jax.ShapeDtypeStruct((lines, 4, 2, rows, width), BF16)
    wide = jax.ShapeDtypeStruct((lines, group, width), BF16)
    thin = jax.ShapeDtypeStruct((lines, group, ff), BF16)
    return pl.pallas_call(
        functools.partial(experts_body, capacity),
        out_shape=(
            all_rows,
            all_rows,
            jax.ShapeDtypeStruct((lines, 4, 2, experts // 2, 2 * rows), F32),
            jax.ShapeDtypeStruct((lines, 4, 2, experts, rows), F32),
            jax.ShapeDtypeStruct((rows, width), F32),
            wide,
            wide,
            thin,
            thin,
            thin,
        ),
        in_specs=[anywhere, anywhere, near, near, near, anywhere, anywhere, anywhere],
        out_specs=(*[anywhere] * 3, near, near, *[anywhere] * 5),
        scratch_shapes=[
            *gather_sems("all", lines),
            *gather_sems("all", lines),
            *gather_sems("all", lines),
            *reduce_scratch("all", lines, rows, width),
            pltpu.VMEM((width, ff), BF16),
            pltpu.VMEM((width, ff), BF16),
            pltpu.VMEM((ff, width), BF16),
            pltpu.VMEM((2, 2, rows, width), BF16),
            pltpu.VMEM((2, 2, rows, width), BF16),
            pltpu.VMEM((2, group, width), BF16),
            pltpu.VMEM((2, group, width), BF16),
            pltpu.VMEM((2, group, width), BF16),
            pltpu.VMEM((2, group, ff), BF16),
            pltpu.VMEM((2, group, ff), BF16),
            pltpu.VMEM((2, group, ff), BF16),
            pltpu.VMEM((group, width), BF16),
            pltpu.VMEM((group, width), BF16),
            pltpu.VMEM((2, 4, 2, rows, width), BF16),
            pltpu.VMEM((2, 2, rows, width), BF16),
            pltpu.VMEM((2, group, 128), F32),
            pltpu.VMEM((group, 128), F32),
            pltpu.VMEM((experts // 2, 2 * rows), F32),
            DMA((3,)),
            DMA((2, 2)),
            DMA((2, 5)),
            DMA((2,)),
        ],
        compiler_params=pltpu.CompilerParams(
            collective_id=2, has_side_effects=True, vmem_limit_bytes=67_000_000
        ),
        name="experts",
    )(hidden_two, cotangent_all, own_weights, select, spread, gate, up, down)


def experts_by_xla(
    hidden_two, cotangent, own_weights, routes_all, gate, up, down, capacity, me, experts
):
    rows = hidden_two.shape[0]
    hidden_all = lax.all_gather(hidden_two, ALL, axis=0, tiled=True)
    gathered = lax.all_gather(own_weights, ALL)
    expert_ids = jnp.arange(experts, dtype=jnp.int32)
    weights_all = gathered.transpose(0, 2, 1).reshape(experts * rows, experts)
    mine = jnp.any(routes_all == me, axis=1).reshape(experts, rows)
    weight_mine = jnp.sum(jnp.where(expert_ids == me, weights_all, 0.0), axis=1).reshape(
        experts, rows
    )
    rank = jnp.cumsum(mine.astype(jnp.int32), axis=1) - 1
    slots = jnp.arange(capacity, dtype=jnp.int32)
    select = (rank[:, None, :] == slots[None, :, None]) & mine[:, None, :]
    select_low = select.astype(BF16)
    slot_weight = jnp.sum(jnp.where(select, weight_mine[:, None, :], 0.0), axis=2).reshape(-1, 1)

    def pick(values):
        return jnp.einsum(
            "sjt,std->sjd",
            select_low,
            values.reshape(experts, rows, D),
            preferred_element_type=F32,
        ).reshape(experts * capacity, D)

    def place(values):
        return (
            jnp.einsum(
                "sjt,sjd->std",
                select_low,
                values.reshape(experts, capacity, D),
                preferred_element_type=F32,
            )
            .astype(BF16)
            .reshape(experts * rows, D)
        )

    expert_rows = pick(hidden_all).astype(BF16)
    own_width = D // experts
    own_columns = lax.dynamic_slice_in_dim(hidden_all, me * own_width, own_width, axis=1)
    expert_rows, own_columns, cotangent = lax.optimization_barrier(
        (expert_rows, own_columns, cotangent)
    )
    cotangent_all = lax.all_gather(cotangent, ALL, axis=0, tiled=True)
    grad_rows_out = pick(cotangent_all)
    grad_slots = (slot_weight * grad_rows_out).astype(BF16)
    gate_act = dot(expert_rows, gate)
    up_act = dot(expert_rows, up)
    gate_sig = jax.nn.sigmoid(gate_act)
    gate_silu = gate_act * gate_sig
    expert_hidden = (gate_silu * up_act).astype(BF16)
    grad_expert_hidden = dot(grad_slots, down.T)
    grad_gate_act = (
        grad_expert_hidden * up_act * gate_sig * (1.0 + gate_act * (1.0 - gate_sig))
    ).astype(BF16)
    grad_up_act = (grad_expert_hidden * gate_silu).astype(BF16)
    grad_rows_in = (dot(grad_gate_act, gate.T) + dot(grad_up_act, up.T)).astype(BF16)
    expert_out = dot(expert_hidden, down).astype(BF16).astype(F32)
    grad_weight_slot = jnp.sum(grad_rows_out * expert_out, axis=1).reshape(experts, capacity)
    grad_weight_mine = jnp.sum(jnp.where(select, grad_weight_slot[:, :, None], 0.0), axis=1)
    out_rows = (slot_weight * expert_out).astype(BF16)

    placed = place(grad_rows_in).reshape(experts, rows, D)
    grad_weight, grad_rows_sum = exchange(
        "sum_rows", 3, [("gather", "all", grad_weight_mine), ("reduce", "all", placed)]
    )
    placed_out = place(lax.optimization_barrier((out_rows, grad_rows_sum))[0])
    return (
        own_columns,
        placed_out,
        grad_weight,
        gathered,
        grad_rows_sum,
        expert_rows,
        grad_slots,
        expert_hidden,
        grad_gate_act,
        grad_up_act,
    )


def on_device(
    tokens,
    lengths,
    routes,
    cotangent,
    query_weight,
    key_weight,
    value_weight,
    output_weight,
    router_weight,
    norm_gains,
    gate_weight,
    up_weight,
    down_weight,
):
    rows = tokens.shape[0]
    lines = lax.axis_size("line")
    cells = lax.axis_size("plane") * lax.axis_size("core")
    experts = lines * cells
    capacity = (3 * rows * TOP + 2 * experts - 1) // (2 * experts)
    score_scale = HEAD_DIM ** (-0.5)
    large = experts > 32
    own_rows = query_weight.shape[0]
    line = lax.axis_index("line")
    me = (line * lax.axis_size("plane") + lax.axis_index("plane")) * lax.axis_size(
        "core"
    ) + lax.axis_index("core")

    packed = jnp.concatenate(
        [
            query_weight.reshape(own_rows, lines, Q_COLS),
            key_weight.reshape(own_rows, lines, HEAD_DIM),
            value_weight.reshape(own_rows, lines, HEAD_DIM),
        ],
        axis=2,
    ).transpose(1, 0, 2)
    width = packed.shape[2]
    floats = padded(jnp.concatenate([router_weight.reshape(-1), norm_gains]), 32 * 128)
    whole_numbers = padded(jnp.concatenate([routes.reshape(-1), lengths.reshape(-1)]), 16 * 128)
    floats_all, numbers_all, weight_qkv, line_tokens, weight_o = exchange(
        "gather_inputs",
        0,
        [
            ("gather", "all", floats),
            ("gather", "all", whole_numbers),
            ("gather", "swap", packed),
            ("gather", "line", tokens),
            ("gather", "plane", output_weight),
        ],
    )
    weight_qkv = weight_qkv.reshape(lines * cells * own_rows, width)
    weight_o = weight_o.reshape(cells * output_weight.shape[0], D)
    floats_all = floats_all.reshape(experts, -1)
    router_size = own_rows * experts
    router = floats_all[:, :router_size].reshape(D, experts)
    gains = floats_all[:, router_size : router_size + norm_gains.shape[0]].reshape(-1).astype(F32)
    numbers_all = numbers_all.reshape(experts, -1)
    routes_all = numbers_all[:, : rows * TOP].reshape(experts * rows, TOP)
    lengths_all = numbers_all[:, rows * TOP : rows * TOP + lengths.shape[1]]
    line_lengths = lax.dynamic_slice_in_dim(
        lengths_all.reshape(lines, cells, -1), me % cells, 1, axis=1
    )[:, 0]
    gain_attn = gains[:D]
    gain_ffn = gains[D : 2 * D]
    gain_query = gains[2 * D : 2 * D + HEAD_DIM]
    gain_key = gains[2 * D + HEAD_DIM :]

    inputs = line_tokens.reshape(lines * rows, D).astype(F32)
    attn_scale = rms_scale(inputs)
    attn_normed = inputs * attn_scale
    hidden_one = (attn_normed * gain_attn).astype(BF16)
    proj = dot(hidden_one, weight_qkv)
    query_proj = proj[:, :Q_COLS].reshape(lines, rows, GROUPS, HEAD_DIM)
    key_proj = proj[:, Q_COLS : Q_COLS + HEAD_DIM].reshape(lines, rows, HEAD_DIM)
    value_proj = proj[:, Q_COLS + HEAD_DIM :].astype(BF16).reshape(lines, rows, HEAD_DIM)
    query_scale = rms_scale(query_proj)
    query_normed = query_proj * query_scale
    key_scale = rms_scale(key_proj)
    key_normed = key_proj * key_scale
    segment, positions = jax.vmap(lambda row: sequence_layout(row, rows))(line_lengths)
    cosine, sine_table = rope_tables(positions, HEAD_DIM)
    query_rot = rotate(
        query_normed * gain_query, cosine[:, :, None], sine_table[:, :, None]
    ).astype(BF16)
    key_rot = rotate(key_normed * gain_key, cosine, sine_table).astype(BF16)
    allowed = (segment[:, :, None] == segment[:, None, :]) & (
        positions[:, None, :] <= positions[:, :, None]
    )
    mixed_heads, log_total = attend(query_rot, key_rot, value_proj, allowed, score_scale)
    mixed_low = mixed_heads.reshape(lines * rows, Q_COLS).astype(BF16)
    projected = dot(mixed_low, weight_o).astype(BF16).reshape(lines, rows, D)
    jobs = [("reduce", "line", projected)]
    if not large:
        jobs.append(("gather", "all", cotangent))
    projected, *cotangent_all = exchange("sum_residual", 1, jobs)
    cotangent_all = None if large else cotangent_all[0]
    own_inputs = tokens.astype(F32)
    residual = own_inputs + projected
    ffn_scale = rms_scale(residual)
    ffn_normed = residual * ffn_scale
    hidden_two = (ffn_normed * gain_ffn).astype(BF16)

    expert_ids = jnp.arange(experts, dtype=jnp.int32)
    named = jnp.any(routes[:, :, None] == expert_ids, axis=1).T
    logits = lax.dot_general(
        router, hidden_two, (((0,), (1,)), ((), ())), preferred_element_type=F32
    )
    masked = jnp.where(named, logits, masked_score)
    exponent = jnp.where(named, jnp.exp(masked - jnp.max(masked, axis=0, keepdims=True)), 0.0)
    own_weights = exponent / jnp.sum(exponent, axis=0, keepdims=True)
    weights = (gate_weight[0], up_weight[0], down_weight[0])
    if large:
        done = experts_by_xla(
            hidden_two, cotangent, own_weights, routes_all, *weights, capacity, me, experts
        )
    else:
        done = experts_call(
            hidden_two, cotangent_all, own_weights, routes_all, *weights, capacity
        )
    hidden_all, placed_out, grad_weight, weights_all, grad_rows_sum = done[:5]
    weights_all = weights_all.reshape(experts, experts, rows).transpose(1, 0, 2)
    weights_all = weights_all.reshape(experts, experts * rows)
    kept = [v.reshape(-1, v.shape[-1]) for v in done[5:]]
    if large:
        own_columns = hidden_all
    else:
        hidden_all = hidden_all.reshape(experts * rows, D)
        own_columns = lax.dynamic_slice_in_dim(hidden_all, me * own_rows, own_rows, axis=1)
    grad_weight = grad_weight.reshape(experts, experts * rows)

    grad_logits = weights_all * (
        grad_weight - jnp.sum(weights_all * grad_weight, axis=0, keepdims=True)
    )
    grad_logits = grad_logits.astype(BF16)
    router_grad = lax.dot_general(
        own_columns, grad_logits, (((0,), (1,)), ((), ())), preferred_element_type=F32
    )
    own_grad_logits = lax.dynamic_slice_in_dim(grad_logits, me * rows, rows, axis=1).T

    grad_out = cotangent.astype(F32)
    grad_hidden_two = dot(own_grad_logits, router.T) + grad_rows_sum.astype(F32)
    grad_gain_ffn = jnp.sum(grad_hidden_two * ffn_normed, axis=0)
    grad_residual = grad_out + norm_back(grad_hidden_two * gain_ffn, ffn_normed, ffn_scale)
    grad_attn, out_sum, (grad_gate, grad_up, grad_down) = exchange(
        "gather_grad",
        4,
        [
            ("gather", "line", grad_residual.astype(BF16)),
            ("reduce", "all", placed_out.reshape(lines, -1, 2, rows, D)),
            ("products", "", kept),
        ],
    )
    block_out = (residual + out_sum).astype(BF16)
    grad_attn = grad_attn.reshape(lines * rows, D)
    output_part = dot(mixed_low.T, grad_attn).astype(BF16)
    grad_mixed = dot(grad_attn, weight_o.T).astype(BF16).reshape(lines, rows, GROUPS, HEAD_DIM)
    grad_query_rot, grad_key_rot, grad_value_rot = attend_back(
        query_rot, key_rot, value_proj, allowed, score_scale, log_total, grad_mixed
    )
    grad_value_proj = grad_value_rot.astype(BF16)
    grad_query_gained = rotate(grad_query_rot, cosine[:, :, None], -sine_table[:, :, None])
    grad_gain_query = jnp.sum(grad_query_gained * query_normed, axis=(0, 1, 2))
    grad_query_proj = norm_back(grad_query_gained * gain_query, query_normed, query_scale).astype(
        BF16
    )
    grad_key_gained = rotate(grad_key_rot, cosine, -sine_table)
    grad_gain_key = jnp.sum(grad_key_gained * key_normed, axis=(0, 1))
    grad_key_proj = norm_back(grad_key_gained * gain_key, key_normed, key_scale).astype(BF16)
    grad_proj = jnp.concatenate(
        [
            grad_query_proj.reshape(lines * rows, Q_COLS),
            grad_key_proj.reshape(lines * rows, HEAD_DIM),
            grad_value_proj.reshape(lines * rows, HEAD_DIM),
        ],
        axis=1,
    )
    hidden_one_part = dot(grad_proj, weight_qkv.T)
    grad_gain_attn = jnp.sum(hidden_one_part * attn_normed, axis=0)
    qkv_part = dot(hidden_one.T, grad_proj).astype(BF16)
    gains_local = jnp.concatenate([grad_gain_attn, grad_gain_ffn, grad_gain_query, grad_gain_key])
    gains_all, grad_hidden_one, qkv_part, output_grad = exchange(
        "sum_gradients",
        5,
        [
            ("gather", "all", padded(gains_local, 16 * 128)),
            ("reduce", "line", hidden_one_part.astype(BF16).reshape(lines, rows, D)),
            ("reduce", "swap", qkv_part.reshape(lines, -1, 2, own_rows, width)),
            ("reduce", "plane", output_part.reshape(-1, 2, output_weight.shape[0], D)),
        ],
    )
    own_scale = rms_scale(own_inputs)
    own_normed = own_inputs * own_scale
    input_grad = grad_residual + norm_back(grad_hidden_one * gain_attn, own_normed, own_scale)
    qkv_part = qkv_part.transpose(1, 0, 2).astype(F32)
    query_grad = qkv_part[:, :, :Q_COLS].reshape(own_rows, lines * Q_COLS)
    key_grad = qkv_part[:, :, Q_COLS : Q_COLS + HEAD_DIM].reshape(own_rows, lines * HEAD_DIM)
    value_grad = qkv_part[:, :, Q_COLS + HEAD_DIM :].reshape(own_rows, lines * HEAD_DIM)
    share = norm_gains.shape[0]
    gains_all = gains_all.reshape(experts, -1)
    gains_all = lax.dynamic_slice_in_dim(gains_all, me * share, share, axis=1)
    gains_grad = jnp.sum(gains_all, axis=0)
    return (
        block_out,
        input_grad,
        query_grad,
        key_grad,
        value_grad,
        output_grad,
        router_grad,
        gains_grad,
        grad_gate[None],
        grad_up[None],
        grad_down[None],
    )


def solution(mesh):
    chips = mesh.shape["expert"]
    cores = mesh.shape["shard"]
    inner = Mesh(
        mesh.devices.reshape(KV_HEADS, chips // KV_HEADS, cores), ("line", "plane", "core")
    )
    return jax.shard_map(
        on_device,
        mesh=inner,
        in_specs=(
            P(ALL, None),
            P(ALL, None),
            P(ALL, None),
            P(ALL, None),
            P(ALL, None),
            P(ALL, None),
            P(ALL, None),
            P(ALL, None),
            P(ALL, None),
            P(ALL),
            P(ALL, None, None),
            P(ALL, None, None),
            P(ALL, None, None),
        ),
        out_specs=(
            P(ALL, None),
            P(ALL, None),
            P(ALL, None),
            P(ALL, None),
            P(ALL, None),
            P(ALL, None),
            P(ALL, None),
            P(ALL),
            P(ALL, None, None),
            P(ALL, None, None),
            P(ALL, None, None),
        ),
        check_vma=False,
    )
```

```python
import functools

import jax
import jax.numpy as jnp
from jax import lax
from jax.experimental import pallas as pl
from jax.experimental.pallas import tpu as pltpu
from jax.sharding import Mesh
from jax.sharding import PartitionSpec as P

D = 2048
HEADS = 32
KV_HEADS = 4
HEAD_DIM = 128
TOP = 8

epsilon = 1e-06
rope_base = 1000000.0
masked_score = -1e30

GROUPS = HEADS // KV_HEADS
Q_COLS = GROUPS * HEAD_DIM
LINE = "line"
PLANE = ("plane", "core")
ALL = ("line", "plane", "core")
F32 = jnp.float32
BF16 = jnp.bfloat16
MESH = pl.DeviceIdType.MESH
DMA = pltpu.SemaphoreType.DMA


def dot(left, right):
    return jnp.dot(left, right, preferred_element_type=F32)


def rms_scale(values):
    return lax.rsqrt(jnp.mean(values * values, axis=-1, keepdims=True) + epsilon)


def norm_back(upstream, normed, scale_rows):
    return scale_rows * (upstream - normed * jnp.mean(upstream * normed, axis=-1, keepdims=True))


def sequence_layout(lengths_row, row_count):
    seq_ends = jnp.cumsum(lengths_row)
    places = jnp.arange(row_count, dtype=jnp.int32)
    segment = jnp.sum((places[:, None] >= seq_ends[None, :]).astype(jnp.int32), axis=1)
    starts = seq_ends - lengths_row
    member = segment[:, None] == jnp.arange(lengths_row.shape[0], dtype=jnp.int32)[None, :]
    seg_start = jnp.sum(jnp.where(member, starts[None, :], 0), axis=1)
    return (segment, places - seg_start)


def rope_tables(positions, head_dim):
    half_dim = head_dim // 2
    inverse = rope_base ** (-2.0 * jnp.arange(half_dim, dtype=F32) / head_dim)
    angles = positions.astype(F32)[..., None] * inverse
    return (jnp.cos(angles), jnp.sin(angles))


def rotate(values, cosine, sine_table):
    half_dim = values.shape[-1] // 2
    first_half = values[..., :half_dim]
    second_half = values[..., half_dim:]
    return jnp.concatenate(
        [
            first_half * cosine - second_half * sine_table,
            second_half * cosine + first_half * sine_table,
        ],
        axis=-1,
    )


def masked_scores(query, keys, allowed, score_scale):
    scores = jnp.einsum("bqgd,bsd->bgqs", query, keys, preferred_element_type=F32) * score_scale
    return jnp.where(allowed[:, None], scores, masked_score)


def attend(query, keys, values_in, allowed, score_scale):
    scores = masked_scores(query, keys, allowed, score_scale)
    top_score = jnp.max(scores, axis=-1, keepdims=True)
    exponent = jnp.exp(scores - top_score)
    row_total = jnp.sum(exponent, axis=-1, keepdims=True)
    attn_probs = (exponent / row_total).astype(BF16)
    mixed_heads = jnp.einsum("bgqs,bsd->bqgd", attn_probs, values_in, preferred_element_type=F32)
    return (mixed_heads, top_score + jnp.log(row_total))


def attend_back(query, keys, values_in, allowed, score_scale, log_total, grad_mixed):
    scores = masked_scores(query, keys, allowed, score_scale)
    attn_probs = jnp.exp(scores - log_total)
    grad_probs = jnp.einsum("bqgd,bsd->bgqs", grad_mixed, values_in, preferred_element_type=F32)
    grad_scores = (
        attn_probs * (grad_probs - jnp.sum(attn_probs * grad_probs, axis=-1, keepdims=True))
    ).astype(BF16)
    grad_query = (
        jnp.einsum("bgqs,bsd->bqgd", grad_scores, keys, preferred_element_type=F32) * score_scale
    )
    grad_keys = (
        jnp.einsum("bgqs,bqgd->bsd", grad_scores, query, preferred_element_type=F32) * score_scale
    )
    grad_values = jnp.einsum(
        "bgqs,bqgd->bsd", attn_probs.astype(BF16), grad_mixed, preferred_element_type=F32
    )
    return (grad_query, grad_keys, grad_values)


class Spot:
    def __init__(self, lines):
        self.lines = lines
        self.z = lax.axis_index("line")
        self.b = lax.axis_index("plane")
        self.c = lax.axis_index("core")
        self.xn = self.b + 1 - 2 * (self.b % 2)
        self.yn = (self.b + 2) % 4
        self.dg = 3 - self.b

    def each(self, d, fn):
        if d == 0:
            fn(self.z, 0)
            return

        @pl.when(self.z - d >= 0)
        def _():
            fn(self.z - d, 1)

        @pl.when(self.z + d < self.lines)
        def _():
            fn(self.z + d, -1)

    def greet(self):
        sem = pltpu.get_barrier_semaphore()

        def tell(dev):
            pl.semaphore_signal(sem, inc=1, device_id=dev, device_id_type=MESH)

        tell((self.z, self.xn, self.c))
        tell((self.z, self.yn, self.c))
        tell((self.z, self.b, 1 - self.c))
        for d in range(1, self.lines):
            self.each(d, lambda zz, way: tell((zz, self.b, self.c)))
        pl.semaphore_wait(sem, self.lines + 2)


def send(src, dst, ssem, rsem, dev):
    return pltpu.make_async_remote_copy(
        src_ref=src, dst_ref=dst, send_sem=ssem, recv_sem=rsem, device_id=dev, device_id_type=MESH
    )


def gather_sems(mode, lines):
    n = 1 if mode == "plane" else lines
    return [DMA, DMA((2, n)), DMA((n,)), DMA((n, 8)), DMA((n, 8)), DMA((2, n, 3)), DMA((n, 3))]


def gather_parts(spot, x_ref, out_ref, sems, mode="all", even=False):
    own_sem, zs, zr, ps, pr, vs, vr = sems
    z, b, c, xn, yn, dg, lines = spot.z, spot.b, spot.c, spot.xn, spot.yn, spot.dg, spot.lines
    here = (z, b, c)
    rows = out_ref.shape[-2]
    flat = mode == "plane"
    planar = mode != "line"
    relayed = mode in ("all", "line")
    via = rows // 4 if even else 0
    last = pl.ds(rows - via, via)
    columns = (b, xn, yn, dg)

    def span(way):
        return rows if way == 0 else rows - via

    def lo(way):
        return pl.ds(0, span(way) // 2)

    def hi(way):
        return pl.ds(span(way) // 2, span(way) // 2)

    def blk(zz, bb, cc=c):
        if flat:
            return out_ref.at[bb, cc]
        return out_ref.at[zz, bb, cc] if planar else out_ref.at[zz]

    mine = 0 if flat else z

    def own():
        return x_ref.at[z] if mode == "swap" else x_ref

    def source(zz, way):
        return own() if way == 0 else blk(zz, b)

    def onward(way, fn):
        if way >= 0:

            @pl.when(z < lines - 1)
            def _():
                fn(0)

        if way <= 0:

            @pl.when(z > 0)
            def _():
                fn(1)

    def hop(zz, down, way):
        return send(source(zz, way), blk(zz, b), zs.at[down, zz], zr.at[zz], (z + 1 - 2 * down, b, c))

    def hop_via(zz, k, down):
        piece = blk(zz, columns[k]).at[last]
        return send(
            piece, piece, vs.at[down, zz, k - 1], vr.at[zz, k - 1], (z + 1 - 2 * down, b, c)
        )

    def plane_copies(zz, way):
        s, d = source(zz, way), blk(zz, b)
        whole = (s, d)
        if via and way != 0:
            s, d = s.at[pl.ds(0, span(way))], d.at[pl.ds(0, span(way))]
        return [
            send(s, d, ps.at[zz, 0], pr.at[zz, 0], (z, xn, c)),
            send(s, d, ps.at[zz, 1], pr.at[zz, 1], (z, yn, c)),
            send(*whole, ps.at[zz, 4], pr.at[zz, 4], (z, b, 1 - c)),
        ]

    def cross(zz, k, way):
        if k == 0:
            piece = blk(zz, yn).at[lo(way)]
            return send(piece, piece, ps.at[zz, 2], pr.at[zz, 2], (z, xn, c))
        piece = blk(zz, xn).at[hi(way)]
        return send(piece, piece, ps.at[zz, 3], pr.at[zz, 3], (z, yn, c))

    def share(zz, k):
        piece = blk(zz, columns[k])
        return send(piece, piece, ps.at[zz, 4 + k], pr.at[zz, 4 + k], (z, b, 1 - c))

    def received(piece, sem):
        send(piece, piece, own_sem, sem, here).wait_recv()

    def over_line(zz, k, way):
        if not via:
            return
        if way != 0:
            received(blk(zz, columns[k]).at[last], vr.at[zz, k - 1])
        onward(way, lambda down: hop_via(zz, k, down).start())

    def start():
        pltpu.make_async_copy(own(), blk(mine, b), own_sem).start()
        if relayed:
            onward(0, lambda down: hop(z, down, 0).start())
        if mode == "swap":
            for d in range(lines - 1, 0, -1):
                spot.each(
                    d,
                    lambda zz, way: send(
                        x_ref.at[zz], blk(z, b), zs.at[0, zz], zr.at[z], (zz, b, c)
                    ).start(),
                )
        if planar:
            for copy in plane_copies(mine, 0):
                copy.start()

    def line_arrive(zz, way):
        received(blk(zz, b), zr.at[zz])
        if relayed:
            onward(way, lambda down: hop(zz, down, way).start())
        if planar:
            for copy in plane_copies(zz, way):
                copy.start()

    def plane_arrive(zz, way):
        part = pl.ds(0, span(way))
        received(blk(zz, xn).at[part], pr.at[zz, 0])
        cross(zz, 1, way).start()
        received(blk(zz, yn).at[part], pr.at[zz, 1])
        cross(zz, 0, way).start()
        over_line(zz, 1, way)
        over_line(zz, 2, way)
        share(zz, 1).start()
        share(zz, 2).start()

    def cross_arrive(zz, way):
        received(blk(zz, dg).at[lo(way)], pr.at[zz, 2])
        received(blk(zz, dg).at[hi(way)], pr.at[zz, 3])
        over_line(zz, 3, way)
        share(zz, 3).start()

    def drain(zz, way):
        if planar:
            for k in range(4):
                share(zz, k).wait_send()
            for copy in plane_copies(zz, way)[:2]:
                copy.wait_send()
            cross(zz, 0, way).wait_send()
            cross(zz, 1, way).wait_send()
        if relayed:
            onward(way, lambda down: hop(zz, down, way).wait_send())
        if via:
            for k in (1, 2, 3):
                onward(way, lambda down, k=k: hop_via(zz, k, down).wait_send())
        if mode == "swap" and way != 0:
            send(x_ref.at[zz], blk(z, b), zs.at[0, zz], zr.at[z], (zz, b, c)).wait_send()

    def shared(zz, k):
        received(blk(zz, columns[k], 1 - c), pr.at[zz, 4 + k])

    def end():
        pltpu.make_async_copy(own(), blk(mine, b), own_sem).wait()

    return {
        "start": start,
        "line": line_arrive,
        "plane": plane_arrive,
        "cross": cross_arrive,
        "shared": shared,
        "drain": drain,
        "end": end,
    }


def gather(spot, mode, x_ref, out_ref, sems):
    parts = gather_parts(spot, x_ref, out_ref, sems, mode)
    flat = mode == "plane"
    planar = mode != "line"
    steps = 1 if flat else spot.lines

    def each(d, fn):
        if flat:
            fn(0, 0)
        else:
            spot.each(d, fn)

    def drain(zz, way):
        if planar:
            for k in range(4):
                parts["shared"](zz, k)
        parts["drain"](zz, way)

    parts["start"]()
    yield
    for s in range(1, steps + 2):
        if s < steps:
            each(s, parts["line"])
        if planar and 0 <= s - 1 < steps:
            each(s - 1, parts["plane"])
        if planar and 0 <= s - 2 < steps:
            each(s - 2, parts["cross"])
        yield
    for d in range(steps):
        each(d, drain)
    parts["end"]()
    yield


def reduce_scratch(mode, lines, rows, cols, dtype=BF16):
    n = 1 if mode == "plane" else lines
    out = []
    if mode != "line":
        out += [
            pltpu.VMEM((n, 4, rows, cols), dtype),
            pltpu.VMEM((n, 2, rows // 2, cols), dtype),
            pltpu.VMEM((n, 2, rows, cols), dtype),
            DMA((n, 8)),
            DMA((n, 8)),
        ]
    if mode == "line":
        out += [pltpu.VMEM((2, lines, rows, cols), dtype), pltpu.VMEM((lines, rows, cols), dtype)]
    if mode == "all":
        out += [pltpu.VMEM((lines, rows, cols), dtype)]
    if mode != "plane":
        out += [DMA((2, lines)), DMA((2, lines))]
    return out


def add_into(dst, *parts, chunk=16):
    rows = dst.shape[0]

    @pl.loop(0, rows // chunk)
    def _(i):
        at = pl.ds(pl.multiple_of(i * chunk, chunk), chunk)
        total = parts[0][at].astype(F32)
        for part in parts[1:]:
            total = total + part[at].astype(F32)
        dst[at] = total.astype(dst.dtype)


def reduce_parts(spot, mode, term, out_ref, scratch):
    z, b, c, xn, yn = spot.z, spot.b, spot.c, spot.xn, spot.yn
    here = (z, b, c)
    scratch = list(scratch)
    pair, crossed, met, ps, pr = scratch[:5]
    passed = scratch[5] if mode == "all" else out_ref
    zs, zr = scratch[-2:]
    rows = pair.shape[-2]
    lo, hi = pl.ds(0, rows // 2), pl.ds(rows // 2, rows // 2)

    def total(zz):
        return met.at[zz, 0]

    def share(zz, k):
        return send(
            term(zz, k, 1 - c), pair.at[zz, k], ps.at[zz, k], pr.at[zz, k], (z, b, 1 - c)
        )

    def cross(zz, k):
        piece = pair.at[zz, 3, (lo, hi)[k]]
        dev = (z, (yn, xn)[k], c)
        return send(piece, crossed.at[zz, k], ps.at[zz, 4 + k], pr.at[zz, 4 + k], dev)

    def meet(zz, k):
        dev = (z, (xn, yn)[k], c)
        return send(pair.at[zz, 1 + k], met.at[zz, k], ps.at[zz, 6 + k], pr.at[zz, 6 + k], dev)

    def away(zz):
        return send(total(zz), passed.at[z], zs.at[0, zz], zr.at[0, z], (zz, b, c))

    def received(piece, sem):
        send(piece, piece, ps.at[0, 0], sem, here).wait_recv()

    def start_one(zz, k):
        share(zz, k).start()

    def first_one(zz, k):
        received(pair.at[zz, k], pr.at[zz, k])
        add_into(pair.at[zz, k], pair.at[zz, k], term(zz, k, c))
        if k == 3:
            cross(zz, 0).start()
            cross(zz, 1).start()

    def start(zz, way):
        for k in (3, 1, 2, 0):
            start_one(zz, k)

    def first(zz, way):
        for k in (3, 1, 2):
            first_one(zz, k)

    def second(zz, way):
        received(crossed.at[zz, 0], pr.at[zz, 4])
        add_into(pair.at[zz, 1, lo], pair.at[zz, 1, lo], crossed.at[zz, 0])
        meet(zz, 0).start()
        received(crossed.at[zz, 1], pr.at[zz, 5])
        add_into(pair.at[zz, 2, hi], pair.at[zz, 2, hi], crossed.at[zz, 1])
        meet(zz, 1).start()

    def third(zz, way):
        received(pair.at[zz, 0], pr.at[zz, 0])
        received(met.at[zz, 0], pr.at[zz, 6])
        received(met.at[zz, 1], pr.at[zz, 7])
        dst = out_ref if mode == "plane" else total(zz)
        add_into(dst, met.at[zz, 0], met.at[zz, 1], pair.at[zz, 0], term(zz, 0, c))
        if mode != "plane":

            @pl.when(zz != z)
            def _():
                away(zz).start()

    def end():
        if mode == "plane":
            return
        for d in range(1, spot.lines):
            spot.each(d, lambda zz, way: received(passed.at[zz], zr.at[0, zz]))
        if mode == "swap":
            add_into(out_ref.at[z], total(z))
            return
        for edge in range(spot.lines):

            @pl.when(z == edge)
            def _():
                others = [passed.at[q] for q in range(spot.lines) if q != edge]
                add_into(out_ref, total(edge), *others)

    def sent(zz, way):
        for k in range(4):
            share(zz, k).wait_send()

    def drain(zz, way):
        for k in range(2):
            cross(zz, k).wait_send()
            meet(zz, k).wait_send()
        if mode != "plane" and way != 0:
            away(zz).wait_send()

    return {
        "start": start,
        "first": first,
        "start one": start_one,
        "first one": first_one,
        "second": second,
        "third": third,
        "sent": sent,
        "end": end,
        "drain": drain,
    }


def reduce(spot, mode, p_ref, out_ref, scratch):
    flat = mode == "plane"
    steps = 1 if flat else spot.lines

    columns = (spot.b, spot.xn, spot.yn, spot.dg)

    def term(zz, k, cc):
        return p_ref.at[columns[k], cc] if flat else p_ref.at[zz, columns[k], cc]

    def each(d, fn):
        if flat:
            fn(0, 0)
        else:
            spot.each(d, fn)

    parts = reduce_parts(spot, mode, term, out_ref, scratch)
    order = list(range(steps - 1, -1, -1))
    for d in order:
        each(d, parts["start"])
    yield
    for s in range(steps + 2):
        for lag, name in enumerate(("first", "second", "third")):
            if 0 <= s - lag < steps:
                each(order[s - lag], parts[name])
        yield
    parts["end"]()
    for d in range(steps):
        each(d, parts["sent"])
        each(d, parts["drain"])
    yield


def reduce_line(spot, p_ref, out_ref, scratch):
    passed, total_ref, zs, zr = scratch
    z, b, c, lines = spot.z, spot.b, spot.c, spot.lines
    here = (z, b, c)

    def received(down, zz):
        piece = passed.at[down, zz]
        send(piece, piece, zs.at[0, 0], zr.at[down, zz], here).wait_recv()

    def hop(src, zz, down):
        return send(
            src.at[zz], passed.at[down, zz], zs.at[down, zz], zr.at[down, zz], (z + 1 - 2 * down, b, c)
        )

    def step(zz, way):
        down = 1 if way > 0 else 0
        first_one = (z == lines - 1) if down else (z == 0)

        @pl.when(jnp.logical_not(first_one))
        def _():
            received(down, zz)
            add_into(total_ref.at[zz], p_ref.at[zz], passed.at[down, zz])
            hop(total_ref, zz, down).start()

        @pl.when(first_one)
        def _():
            hop(p_ref, zz, down).start()

    for d in range(lines - 1, 0, -1):
        spot.each(d, step)
        yield

    @pl.when(z > 0)
    def _():
        received(0, z)

    @pl.when(z < lines - 1)
    def _():
        received(1, z)

    @pl.when(z == 0)
    def _():
        add_into(out_ref, p_ref.at[z], passed.at[1, z])

    @pl.when(z == lines - 1)
    def _():
        add_into(out_ref, p_ref.at[z], passed.at[0, z])

    @pl.when((z > 0) & (z < lines - 1))
    def _():
        add_into(out_ref, p_ref.at[z], passed.at[0, z], passed.at[1, z])

    for d in range(1, lines):
        spot.each(d, lambda zz, way: hop(total_ref, zz, 1 if way > 0 else 0).wait_send())
    yield


def dot_tn(left, right):
    return lax.dot_general(left, right, (((0,), (0,)), ((), ())), preferred_element_type=F32)


def products_scratch(count, width, ff):
    return [
        pltpu.VMEM((3, count, ff), BF16),
        pltpu.VMEM((2, count, 256), BF16),
        pltpu.VMEM((2, 2, 256, ff), BF16),
        pltpu.VMEM((2, ff, 256), BF16),
        DMA((3,)),
        DMA((2,)),
        DMA((2, 2)),
        DMA((2,)),
    ]


def products(ins, outs, scratch):
    x_ref, dy_ref, a_ref, dg_ref, du_ref = ins
    gate_out, up_out, down_out = outs
    near, tile, wide, tall, n_sem, t_sem, w_sem, d_sem = scratch
    half = x_ref.shape[1] // 256

    def columns(n):
        return pl.ds((n % half) * 256, 256)

    def load(n):
        src = x_ref if n < half else dy_ref
        return pltpu.make_async_copy(src.at[:, columns(n)], tile.at[n % 2], t_sem.at[n % 2])

    def store(n):
        q = n % 2
        if n < half:
            return [
                pltpu.make_async_copy(wide.at[q, 0], gate_out.at[columns(n)], w_sem.at[q, 0]),
                pltpu.make_async_copy(wide.at[q, 1], up_out.at[columns(n)], w_sem.at[q, 1]),
            ]
        return [pltpu.make_async_copy(tall.at[q], down_out.at[:, columns(n)], d_sem.at[q])]

    near_loads = [
        pltpu.make_async_copy(src, near.at[i], n_sem.at[i])
        for i, src in enumerate((a_ref, dg_ref, du_ref))
    ]
    for copy in near_loads:
        copy.start()
    load(0).start()
    yield
    for copy in near_loads:
        copy.wait()
    for n in range(2 * half):
        load(n).wait()
        if n + 1 < 2 * half:
            load(n + 1).start()
        if n % half >= 2:
            for copy in store(n - 2):
                copy.wait()
        q = n % 2
        if n < half:
            wide[q, 0] = dot_tn(tile[q], near[1]).astype(BF16)
            wide[q, 1] = dot_tn(tile[q], near[2]).astype(BF16)
        else:
            tall[q] = dot_tn(near[0], tile[q]).astype(BF16)
        for copy in store(n):
            copy.start()
        if n % 3 == 2:
            yield
    for n in (half - 2, half - 1, 2 * half - 2, 2 * half - 1):
        for copy in store(n):
            copy.wait()
    yield


def run_steps(makers):
    live = list(makers)
    while live:
        for g in list(live):
            try:
                next(g)
            except StopIteration:
                live.remove(g)

def exchange(name, cid, jobs):
    lines = lax.axis_size("line")
    cells = lax.axis_size("plane") * lax.axis_size("core")
    if cells != 8 or lines != 4:
        return [exchange_by_xla(kind, mode, x, lines, cells) for kind, mode, x in jobs]
    far, near = pl.BlockSpec(memory_space=pl.ANY), pl.BlockSpec(memory_space=pltpu.VMEM)
    args, in_specs, out_shapes, out_specs, scratch, counts = [], [], [], [], [], []
    for kind, mode, x in jobs:
        if kind == "products":
            width, ff = x[0].shape[1], x[2].shape[1]
            args += x
            in_specs += [far] * 5
            out_shapes += [jax.ShapeDtypeStruct((width, ff), BF16)] * 2
            out_shapes.append(jax.ShapeDtypeStruct((ff, width), BF16))
            out_specs += [far] * 3
            own = products_scratch(x[0].shape[0], width, ff)
            counts.append((5, 3, len(own)))
            scratch += own
            continue
        rows, cols = x.shape[-2:]
        spec = near if kind == "reduce" else far
        args.append(x)
        in_specs.append(spec)
        if kind == "gather":
            lead = {"line": (lines,), "plane": (4, 2)}.get(mode, (lines, 4, 2))
            out_shapes.append(jax.ShapeDtypeStruct((*lead, rows, cols), x.dtype))
            own = gather_sems(mode, lines)
        else:
            if mode == "swap":
                out_shapes.append(jax.ShapeDtypeStruct((lines, rows, cols), x.dtype))
            else:
                out_shapes.append(jax.ShapeDtypeStruct((rows, cols), F32))
            own = reduce_scratch(mode, lines, rows, cols, x.dtype)
        out_specs.append(spec)
        scratch += own
        counts.append((1, 1, len(own)))
    kinds = [(kind, mode) for kind, mode, _ in jobs]

    def body(*refs):
        spot = Spot(lines)
        spot.greet()
        ins, outs, rest = 0, len(args), len(args) + len(out_shapes)
        makers = []
        for (kind, mode), (n_in, n_out, n_rest) in zip(kinds, counts):
            i, o, w = refs[ins : ins + n_in], refs[outs : outs + n_out], refs[rest : rest + n_rest]
            ins, outs, rest = ins + n_in, outs + n_out, rest + n_rest
            if kind == "products":
                makers.append(products(i, o, w))
            elif kind == "gather":
                makers.append(gather(spot, mode, i[0], o[0], w))
            elif mode == "line":
                makers.append(reduce_line(spot, i[0], o[0], w))
            else:
                makers.append(reduce(spot, mode, i[0], o[0], w))
        run_steps(makers)

    outs = pl.pallas_call(
        body,
        out_shape=tuple(out_shapes),
        in_specs=in_specs,
        out_specs=tuple(out_specs),
        scratch_shapes=scratch,
        compiler_params=pltpu.CompilerParams(
            collective_id=cid, has_side_effects=True, vmem_limit_bytes=62 << 20
        ),
        name=name,
    )(*args)
    results, at = [], 0
    for _, n_out, _ in counts:
        results.append(outs[at] if n_out == 1 else outs[at : at + n_out])
        at += n_out
    return results


def exchange_by_xla(kind, mode, x, lines, cells):
    if kind == "products":
        hidden, grad_slots, acts, grad_gate, grad_up = x
        return dot(hidden.T, grad_gate), dot(hidden.T, grad_up), dot(acts.T, grad_slots)
    rows, cols = x.shape[-2:]
    if kind == "gather":
        if mode == "swap":
            x = lax.all_to_all(x, LINE, split_axis=0, concat_axis=0, tiled=True)
            return lax.all_gather(x, PLANE, axis=1)
        return lax.all_gather(x, {"line": LINE, "plane": PLANE, "all": ALL}[mode])
    if mode == "swap":
        x = x.reshape(lines, cells, rows, cols).transpose(1, 0, 2, 3)
        x = lax.psum_scatter(x, PLANE, scatter_dimension=0, tiled=True)
        x = x.reshape(lines, rows, cols)
        return lax.all_to_all(x, LINE, split_axis=0, concat_axis=0, tiled=True)
    x = x.reshape(-1, cols)
    axes = {"line": LINE, "plane": PLANE, "all": ALL}[mode]
    return lax.psum_scatter(x, axes, scatter_dimension=0, tiled=True).astype(F32)


def padded(flat, unit):
    size = -(-flat.shape[0] // unit) * unit
    return jnp.pad(flat, (0, size - flat.shape[0])).reshape(-1, 128)


def pick_order(z, i):
    far = z // 2
    near = z * (1 - far) + (3 - z) * far
    place = (near + i) % 2 if i < 2 else i
    return place * (1 - far) + (3 - place) * far


def dot_nt(left, right):
    return lax.dot_general(left, right, (((1,), (1,)), ((), ())), preferred_element_type=F32)


def experts_body(capacity, *refs):
    lines = 4
    (h_ref, tall, own_w_ref, sel_ref, spread_ref, gate_ref, up_ref, down_ref) = refs[:8]
    (hall, py, dw_all, w_ref, sum_ref, x_out, dy_out, a_out, dg_out, du_out) = refs[8:18]
    rest = list(refs[18:])
    h_sems, w_sems, dw_sems = rest[:7], rest[7:14], rest[14:21]
    sum_scratch = rest[21:29]
    (wg, wu, wd, hb, tb, xs, zs, dys, acts, dgs, dus, rs, ys) = rest[29:42]
    (stage, stage_y, slot_w, acc, dw_ref, w_sem, l_sem, o_sem, p_sem) = rest[42:]
    spot = Spot(lines)
    z, b, c, xn, yn, dg_spot = spot.z, spot.b, spot.c, spot.xn, spot.yn, spot.dg
    me = (z * 4 + b) * 2 + c
    pair = 2 * capacity
    spot.greet()
    steps_h = gather_parts(spot, h_ref, hall, h_sems, even=True)
    steps_w = gather_parts(spot, own_w_ref, w_ref, w_sems)
    steps_dw = gather_parts(spot, dw_ref, dw_all, dw_sems)
    both = (steps_w, steps_h)
    columns = (b, xn, yn, dg_spot)
    turn = [0]

    def term(zz, k, cc):
        return stage.at[turn[0] % 2, k, cc]

    steps_r = reduce_parts(spot, "all", term, sum_ref, sum_scratch)

    def sums(name, i, k=1):
        turn[0] = i
        steps_r[name](pick_order(z, i), k)

    def comm_dw(name, d):
        spot.each(d, steps_dw[name])

    loads = [
        pltpu.make_async_copy(gate_ref, wg, w_sem.at[0]),
        pltpu.make_async_copy(up_ref, wu, w_sem.at[1]),
        pltpu.make_async_copy(down_ref, wd, w_sem.at[2]),
    ]

    def comm(*names):
        for s in both:
            for name in names:
                part, d = name.split()
                spot.each(int(d), s[part])

    def load(n):
        i, k = n // 4, n % 4
        zz, bb = pick_order(z, i), columns[k]
        return [
            pltpu.make_async_copy(hall.at[zz, bb], hb.at[n % 3], l_sem.at[0, n % 3]),
            pltpu.make_async_copy(tall.at[zz, bb], tb.at[n % 3], l_sem.at[1, n % 3]),
        ]

    def fetch(n):
        i, k = n // 4, n % 4
        zz = pick_order(z, i)
        for s in both:
            s["shared"](zz, k)
        for copy in load(n):
            copy.start()

    def pick(n):
        i, k = n // 4, n % 4
        zz, bb = pick_order(z, i), columns[k]
        at = pl.ds(pl.multiple_of(bb * pair, 16), pair)
        which = zz * 4 + bb
        for copy in load(n):
            copy.wait()
        rows = hb.shape[2]
        width = hb.shape[3]
        mine = jnp.concatenate(
            [w_ref[zz, bb, 0, pl.ds(me, 1), :], w_ref[zz, bb, 1, pl.ds(me, 1), :]], axis=1
        )
        select = sel_ref[which]
        per_slot = jnp.sum(select.astype(F32) * mine, axis=1, keepdims=True)
        slot_w[i % 2, at, :] = jnp.broadcast_to(per_slot, (pair, 128))

        @pl.loop(0, width // 512)
        def _(j):
            part = pl.ds(pl.multiple_of(j * 512, 512), 512)
            h = hb[n % 3, :, :, part].reshape(2 * rows, 512)
            t = tb[n % 3, :, :, part].reshape(2 * rows, 512)
            xs[i % 2, at, part] = jnp.dot(select, h, preferred_element_type=F32).astype(BF16)
            t = jnp.dot(select, t, preferred_element_type=F32)
            zs[i % 2, at, part] = t.astype(BF16)
            dys[i % 2, at, part] = (per_slot * t).astype(BF16)

    def keep(i):
        zz = pick_order(z, i)
        q = i % 2
        return [
            pltpu.make_async_copy(xs.at[q], x_out.at[zz], o_sem.at[q, 0]),
            pltpu.make_async_copy(dys.at[q], dy_out.at[zz], o_sem.at[q, 1]),
            pltpu.make_async_copy(acts.at[q], a_out.at[zz], o_sem.at[q, 2]),
            pltpu.make_async_copy(dgs.at[q], dg_out.at[zz], o_sem.at[q, 3]),
            pltpu.make_async_copy(dus.at[q], du_out.at[zz], o_sem.at[q, 4]),
        ]

    def inner(i):
        q = i % 2

        @pl.loop(0, wg.shape[1] // 256)
        def _(j):
            part = pl.ds(pl.multiple_of(j * 256, 256), 256)
            g = jnp.dot(xs[q], wg[:, part], preferred_element_type=F32)
            u = jnp.dot(xs[q], wu[:, part], preferred_element_type=F32)
            da = dot_nt(dys[q], wd[part, :])
            sig = jax.nn.sigmoid(g)
            silu = g * sig
            acts[q, :, part] = (silu * u).astype(BF16)
            dgs[q, :, part] = (da * u * sig * (1.0 + g * (1.0 - sig))).astype(BF16)
            dus[q, :, part] = (da * silu).astype(BF16)

        for copy in keep(i):
            copy.start()

    def outer(i):
        q = i % 2
        acc[...] = jnp.zeros_like(acc)

        @pl.loop(0, wg.shape[0] // 256)
        def _(j):
            part = pl.ds(pl.multiple_of(j * 256, 256), 256)
            r = dot_nt(dgs[q], wg[part, :]) + dot_nt(dus[q], wu[part, :])
            rs[:, part] = r.astype(BF16)
            y = jnp.dot(acts[q], wd[:, part], preferred_element_type=F32)
            y = y.astype(BF16).astype(F32)
            met = y * zs[q, :, part].astype(F32)
            acc[...] += met[:, :128] + met[:, 128:]
            ys[:, part] = (slot_w[q, :, 0:1] * y).astype(BF16)

    def put(zz, bb, m):
        return pltpu.make_async_copy(stage_y.at[m % 2], py.at[zz, bb], p_sem.at[m % 2])

    def place(i, k, m):
        zz, bb = pick_order(z, i), columns[k]
        at = pl.ds(pl.multiple_of(bb * pair, 16), pair)
        which = zz * 4 + bb
        if m >= 2:
            put(zz, bb, m).wait()
        dw_slot = jnp.sum(acc[at, :], axis=1, keepdims=True)
        dw_ref[pl.ds(which, 1), :] = jnp.sum(
            sel_ref[which].astype(F32) * dw_slot, axis=0, keepdims=True
        )
        spread = spread_ref[which]
        rows = stage.shape[3]

        @pl.loop(0, rs.shape[1] // 512)
        def _(j):
            part = pl.ds(pl.multiple_of(j * 512, 512), 512)
            full = jnp.dot(spread, rs[at, part], preferred_element_type=F32)
            stage[i % 2, k, :, :, part] = full.astype(BF16).reshape(2, rows, 512)
            full = jnp.dot(spread, ys[at, part], preferred_element_type=F32)
            stage_y[m % 2, :, :, part] = full.astype(BF16).reshape(2, rows, 512)

        put(zz, bb, m).start()

    def places(i):
        order = (3, 1, 2, 0)
        for n, k in enumerate(order):
            place(i, k, 4 * i + n)
            if n >= 1:
                sums("start one", i, order[n - 1])
            if n >= 2:
                sums("first one", i, order[n - 2])
        sums("start one", i, 0)
        sums("first one", i, 2)

    def kept(i):
        for copy in keep(i):
            copy.wait()

    for s in both:
        s["start"]()
    for copy in loads:
        copy.start()
    for s in both:
        s["end"]()
    fetch(0)
    comm("line 1", "plane 0")
    fetch(1)
    fetch(2)
    pick(0)
    pick(1)
    comm("cross 0")
    fetch(3)
    pick(2)
    comm("line 2")
    fetch(4)
    pick(3)
    for copy in loads:
        copy.wait()
    inner(0)
    comm("plane 1")
    fetch(5)
    fetch(6)
    pick(4)
    outer(0)
    pick(5)
    pick(6)
    comm("line 3", "cross 1")
    fetch(7)
    places(0)
    pick(7)
    inner(1)
    kept(0)
    comm("plane 2")
    fetch(8)
    fetch(9)
    fetch(10)
    pick(8)
    pick(9)
    pick(10)
    sums("second", 0)
    outer(1)
    comm("cross 2")
    fetch(11)
    places(1)
    sums("third", 0)
    comm("plane 3")
    fetch(12)
    fetch(13)
    pick(11)
    inner(2)
    kept(1)
    sums("second", 1)
    fetch(14)
    pick(12)
    pick(13)
    pick(14)
    outer(2)
    comm("cross 3")
    fetch(15)
    sums("sent", 0)
    places(2)
    sums("third", 1)
    pick(15)
    inner(3)
    sums("second", 2)
    outer(3)
    sums("sent", 1)
    places(3)
    steps_dw["start"]()
    sums("third", 2)
    sums("second", 3)
    comm_dw("line", 1)
    comm_dw("plane", 0)
    comm_dw("line", 2)
    comm_dw("plane", 1)
    comm_dw("cross", 0)
    comm_dw("line", 3)
    comm_dw("plane", 2)
    comm_dw("cross", 1)
    sums("third", 3)
    comm_dw("plane", 3)
    comm_dw("cross", 2)
    comm_dw("cross", 3)
    steps_r["end"]()
    for m in (0, 1):
        put(z, b, m).wait()
    for i in (2, 3):
        kept(i)
        sums("sent", i)
    for d in range(lines):
        comm(f"drain {d}")
        comm_dw("drain", d)
        spot.each(d, steps_r["drain"])
        for k in range(4):
            spot.each(d, lambda zz, way, k=k: steps_dw["shared"](zz, k))
    steps_dw["end"]()


def experts_call(hidden_two, cotangent_all, own_weights, routes_all, gate, up, down, capacity):
    lines, experts = 4, 32
    rows, width = hidden_two.shape
    ff = gate.shape[1]
    pair = 2 * capacity
    group = 4 * pair
    me = (lax.axis_index("line") * 4 + lax.axis_index("plane")) * 2 + lax.axis_index("core")
    mine = jnp.any(routes_all == me, axis=1).reshape(experts, rows)
    rank = jnp.cumsum(mine.astype(jnp.int32), axis=1) - 1
    slot = rank + (jnp.arange(experts, dtype=jnp.int32) % 2 * capacity)[:, None]
    slot = jnp.where(mine, slot, -1).reshape(experts // 2, 2 * rows)
    places = jnp.arange(pair, dtype=jnp.int32)
    select = (slot[:, None, :] == places[None, :, None]).astype(BF16)
    spread = (slot[:, :, None] == places[None, None, :]).astype(BF16)
    anywhere = pl.BlockSpec(memory_space=pl.ANY)
    near = pl.BlockSpec(memory_space=pltpu.VMEM)
    all_rows = jax.ShapeDtypeStruct((lines, 4, 2, rows, width), BF16)
    wide = jax.ShapeDtypeStruct((lines, group, width), BF16)
    thin = jax.ShapeDtypeStruct((lines, group, ff), BF16)
    return pl.pallas_call(
        functools.partial(experts_body, capacity),
        out_shape=(
            all_rows,
            all_rows,
            jax.ShapeDtypeStruct((lines, 4, 2, experts // 2, 2 * rows), F32),
            jax.ShapeDtypeStruct((lines, 4, 2, experts, rows), F32),
            jax.ShapeDtypeStruct((rows, width), F32),
            wide,
            wide,
            thin,
            thin,
            thin,
        ),
        in_specs=[anywhere, anywhere, near, near, near, anywhere, anywhere, anywhere],
        out_specs=(*[anywhere] * 3, near, near, *[anywhere] * 5),
        scratch_shapes=[
            *gather_sems("all", lines),
            *gather_sems("all", lines),
            *gather_sems("all", lines),
            *reduce_scratch("all", lines, rows, width),
            pltpu.VMEM((width, ff), BF16),
            pltpu.VMEM((width, ff), BF16),
            pltpu.VMEM((ff, width), BF16),
            pltpu.VMEM((3, 2, rows, width), BF16),
            pltpu.VMEM((3, 2, rows, width), BF16),
            pltpu.VMEM((2, group, width), BF16),
            pltpu.VMEM((2, group, width), BF16),
            pltpu.VMEM((2, group, width), BF16),
            pltpu.VMEM((2, group, ff), BF16),
            pltpu.VMEM((2, group, ff), BF16),
            pltpu.VMEM((2, group, ff), BF16),
            pltpu.VMEM((group, width), BF16),
            pltpu.VMEM((group, width), BF16),
            pltpu.VMEM((2, 4, 2, rows, width), BF16),
            pltpu.VMEM((2, 2, rows, width), BF16),
            pltpu.VMEM((2, group, 128), F32),
            pltpu.VMEM((group, 128), F32),
            pltpu.VMEM((experts // 2, 2 * rows), F32),
            DMA((3,)),
            DMA((2, 3)),
            DMA((2, 5)),
            DMA((2,)),
        ],
        compiler_params=pltpu.CompilerParams(
            collective_id=2, has_side_effects=True, vmem_limit_bytes=67_000_000
        ),
        name="experts",
    )(hidden_two, cotangent_all, own_weights, select, spread, gate, up, down)


def experts_by_xla(
    hidden_two, cotangent, own_weights, routes_all, gate, up, down, capacity, me, experts
):
    rows = hidden_two.shape[0]
    hidden_all = lax.all_gather(hidden_two, ALL, axis=0, tiled=True)
    gathered = lax.all_gather(own_weights, ALL)
    expert_ids = jnp.arange(experts, dtype=jnp.int32)
    weights_all = gathered.transpose(0, 2, 1).reshape(experts * rows, experts)
    mine = jnp.any(routes_all == me, axis=1).reshape(experts, rows)
    weight_mine = jnp.sum(jnp.where(expert_ids == me, weights_all, 0.0), axis=1).reshape(
        experts, rows
    )
    rank = jnp.cumsum(mine.astype(jnp.int32), axis=1) - 1
    slots = jnp.arange(capacity, dtype=jnp.int32)
    select = (rank[:, None, :] == slots[None, :, None]) & mine[:, None, :]
    select_low = select.astype(BF16)
    slot_weight = jnp.sum(jnp.where(select, weight_mine[:, None, :], 0.0), axis=2).reshape(-1, 1)

    def pick(values):
        return jnp.einsum(
            "sjt,std->sjd",
            select_low,
            values.reshape(experts, rows, D),
            preferred_element_type=F32,
        ).reshape(experts * capacity, D)

    def place(values):
        return (
            jnp.einsum(
                "sjt,sjd->std",
                select_low,
                values.reshape(experts, capacity, D),
                preferred_element_type=F32,
            )
            .astype(BF16)
            .reshape(experts * rows, D)
        )

    expert_rows = pick(hidden_all).astype(BF16)
    own_width = D // experts
    own_columns = lax.dynamic_slice_in_dim(hidden_all, me * own_width, own_width, axis=1)
    expert_rows, own_columns, cotangent = lax.optimization_barrier(
        (expert_rows, own_columns, cotangent)
    )
    cotangent_all = lax.all_gather(cotangent, ALL, axis=0, tiled=True)
    grad_rows_out = pick(cotangent_all)
    grad_slots = (slot_weight * grad_rows_out).astype(BF16)
    gate_act = dot(expert_rows, gate)
    up_act = dot(expert_rows, up)
    gate_sig = jax.nn.sigmoid(gate_act)
    gate_silu = gate_act * gate_sig
    expert_hidden = (gate_silu * up_act).astype(BF16)
    grad_expert_hidden = dot(grad_slots, down.T)
    grad_gate_act = (
        grad_expert_hidden * up_act * gate_sig * (1.0 + gate_act * (1.0 - gate_sig))
    ).astype(BF16)
    grad_up_act = (grad_expert_hidden * gate_silu).astype(BF16)
    grad_rows_in = (dot(grad_gate_act, gate.T) + dot(grad_up_act, up.T)).astype(BF16)
    expert_out = dot(expert_hidden, down).astype(BF16).astype(F32)
    grad_weight_slot = jnp.sum(grad_rows_out * expert_out, axis=1).reshape(experts, capacity)
    grad_weight_mine = jnp.sum(jnp.where(select, grad_weight_slot[:, :, None], 0.0), axis=1)
    out_rows = (slot_weight * expert_out).astype(BF16)

    placed = place(grad_rows_in).reshape(experts, rows, D)
    grad_weight, grad_rows_sum = exchange(
        "sum_rows", 3, [("gather", "all", grad_weight_mine), ("reduce", "all", placed)]
    )
    placed_out = place(lax.optimization_barrier((out_rows, grad_rows_sum))[0])
    return (
        own_columns,
        placed_out,
        grad_weight,
        gathered,
        grad_rows_sum,
        expert_rows,
        grad_slots,
        expert_hidden,
        grad_gate_act,
        grad_up_act,
    )


def on_device(
    tokens,
    lengths,
    routes,
    cotangent,
    query_weight,
    key_weight,
    value_weight,
    output_weight,
    router_weight,
    norm_gains,
    gate_weight,
    up_weight,
    down_weight,
):
    rows = tokens.shape[0]
    lines = lax.axis_size("line")
    cells = lax.axis_size("plane") * lax.axis_size("core")
    experts = lines * cells
    capacity = (3 * rows * TOP + 2 * experts - 1) // (2 * experts)
    score_scale = HEAD_DIM ** (-0.5)
    large = experts > 32
    own_rows = query_weight.shape[0]
    line = lax.axis_index("line")
    me = (line * lax.axis_size("plane") + lax.axis_index("plane")) * lax.axis_size(
        "core"
    ) + lax.axis_index("core")

    packed = jnp.concatenate(
        [
            query_weight.reshape(own_rows, lines, Q_COLS),
            key_weight.reshape(own_rows, lines, HEAD_DIM),
            value_weight.reshape(own_rows, lines, HEAD_DIM),
        ],
        axis=2,
    ).transpose(1, 0, 2)
    width = packed.shape[2]
    floats = padded(jnp.concatenate([router_weight.reshape(-1), norm_gains]), 32 * 128)
    whole_numbers = padded(jnp.concatenate([routes.reshape(-1), lengths.reshape(-1)]), 16 * 128)
    floats_all, numbers_all, weight_qkv, line_tokens, weight_o = exchange(
        "gather_inputs",
        0,
        [
            ("gather", "all", floats),
            ("gather", "all", whole_numbers),
            ("gather", "swap", packed),
            ("gather", "line", tokens),
            ("gather", "plane", output_weight),
        ],
    )
    weight_qkv = weight_qkv.reshape(lines * cells * own_rows, width)
    weight_o = weight_o.reshape(cells * output_weight.shape[0], D)
    floats_all = floats_all.reshape(experts, -1)
    router_size = own_rows * experts
    router = floats_all[:, :router_size].reshape(D, experts)
    gains = floats_all[:, router_size : router_size + norm_gains.shape[0]].reshape(-1).astype(F32)
    numbers_all = numbers_all.reshape(experts, -1)
    routes_all = numbers_all[:, : rows * TOP].reshape(experts * rows, TOP)
    lengths_all = numbers_all[:, rows * TOP : rows * TOP + lengths.shape[1]]
    line_lengths = lax.dynamic_slice_in_dim(
        lengths_all.reshape(lines, cells, -1), me % cells, 1, axis=1
    )[:, 0]
    gain_attn = gains[:D]
    gain_ffn = gains[D : 2 * D]
    gain_query = gains[2 * D : 2 * D + HEAD_DIM]
    gain_key = gains[2 * D + HEAD_DIM :]

    inputs = line_tokens.reshape(lines * rows, D).astype(F32)
    attn_scale = rms_scale(inputs)
    attn_normed = inputs * attn_scale
    hidden_one = (attn_normed * gain_attn).astype(BF16)
    proj = dot(hidden_one, weight_qkv)
    query_proj = proj[:, :Q_COLS].reshape(lines, rows, GROUPS, HEAD_DIM)
    key_proj = proj[:, Q_COLS : Q_COLS + HEAD_DIM].reshape(lines, rows, HEAD_DIM)
    value_proj = proj[:, Q_COLS + HEAD_DIM :].astype(BF16).reshape(lines, rows, HEAD_DIM)
    query_scale = rms_scale(query_proj)
    query_normed = query_proj * query_scale
    key_scale = rms_scale(key_proj)
    key_normed = key_proj * key_scale
    segment, positions = jax.vmap(lambda row: sequence_layout(row, rows))(line_lengths)
    cosine, sine_table = rope_tables(positions, HEAD_DIM)
    query_rot = rotate(
        query_normed * gain_query, cosine[:, :, None], sine_table[:, :, None]
    ).astype(BF16)
    key_rot = rotate(key_normed * gain_key, cosine, sine_table).astype(BF16)
    allowed = (segment[:, :, None] == segment[:, None, :]) & (
        positions[:, None, :] <= positions[:, :, None]
    )
    mixed_heads, log_total = attend(query_rot, key_rot, value_proj, allowed, score_scale)
    mixed_low = mixed_heads.reshape(lines * rows, Q_COLS).astype(BF16)
    projected = dot(mixed_low, weight_o).astype(BF16).reshape(lines, rows, D)
    jobs = [("reduce", "line", projected)]
    if not large:
        jobs.insert(0, ("gather", "all", cotangent))
    *cotangent_all, projected = exchange("sum_residual", 1, jobs)
    cotangent_all = None if large else cotangent_all[0]
    own_inputs = tokens.astype(F32)
    residual = own_inputs + projected
    ffn_scale = rms_scale(residual)
    ffn_normed = residual * ffn_scale
    hidden_two = (ffn_normed * gain_ffn).astype(BF16)

    expert_ids = jnp.arange(experts, dtype=jnp.int32)
    named = jnp.any(routes[:, :, None] == expert_ids, axis=1).T
    logits = lax.dot_general(
        router, hidden_two, (((0,), (1,)), ((), ())), preferred_element_type=F32
    )
    masked = jnp.where(named, logits, masked_score)
    exponent = jnp.where(named, jnp.exp(masked - jnp.max(masked, axis=0, keepdims=True)), 0.0)
    own_weights = exponent / jnp.sum(exponent, axis=0, keepdims=True)
    weights = (gate_weight[0], up_weight[0], down_weight[0])
    if large:
        done = experts_by_xla(
            hidden_two, cotangent, own_weights, routes_all, *weights, capacity, me, experts
        )
    else:
        done = experts_call(
            hidden_two, cotangent_all, own_weights, routes_all, *weights, capacity
        )
    hidden_all, placed_out, grad_weight, weights_all, grad_rows_sum = done[:5]
    weights_all = weights_all.reshape(experts, experts, rows).transpose(1, 0, 2)
    weights_all = weights_all.reshape(experts, experts * rows)
    kept = [v.reshape(-1, v.shape[-1]) for v in done[5:]]
    if large:
        own_columns = hidden_all
    else:
        hidden_all = hidden_all.reshape(experts * rows, D)
        own_columns = lax.dynamic_slice_in_dim(hidden_all, me * own_rows, own_rows, axis=1)
    grad_weight = grad_weight.reshape(experts, experts * rows)

    grad_logits = weights_all * (
        grad_weight - jnp.sum(weights_all * grad_weight, axis=0, keepdims=True)
    )
    grad_logits = grad_logits.astype(BF16)
    router_grad = lax.dot_general(
        own_columns, grad_logits, (((0,), (1,)), ((), ())), preferred_element_type=F32
    )
    own_grad_logits = lax.dynamic_slice_in_dim(grad_logits, me * rows, rows, axis=1).T

    grad_out = cotangent.astype(F32)
    grad_hidden_two = dot(own_grad_logits, router.T) + grad_rows_sum.astype(F32)
    grad_gain_ffn = jnp.sum(grad_hidden_two * ffn_normed, axis=0)
    grad_residual = grad_out + norm_back(grad_hidden_two * gain_ffn, ffn_normed, ffn_scale)
    grad_attn, out_sum, (grad_gate, grad_up, grad_down) = exchange(
        "gather_grad",
        4,
        [
            ("gather", "line", grad_residual.astype(BF16)),
            ("reduce", "all", placed_out.reshape(lines, -1, 2, rows, D)),
            ("products", "", kept),
        ],
    )
    block_out = (residual + out_sum).astype(BF16)
    grad_attn = grad_attn.reshape(lines * rows, D)
    output_part = dot(mixed_low.T, grad_attn).astype(BF16)
    grad_mixed = dot(grad_attn, weight_o.T).astype(BF16).reshape(lines, rows, GROUPS, HEAD_DIM)
    grad_query_rot, grad_key_rot, grad_value_rot = attend_back(
        query_rot, key_rot, value_proj, allowed, score_scale, log_total, grad_mixed
    )
    grad_value_proj = grad_value_rot.astype(BF16)
    grad_query_gained = rotate(grad_query_rot, cosine[:, :, None], -sine_table[:, :, None])
    grad_gain_query = jnp.sum(grad_query_gained * query_normed, axis=(0, 1, 2))
    grad_query_proj = norm_back(grad_query_gained * gain_query, query_normed, query_scale).astype(
        BF16
    )
    grad_key_gained = rotate(grad_key_rot, cosine, -sine_table)
    grad_gain_key = jnp.sum(grad_key_gained * key_normed, axis=(0, 1))
    grad_key_proj = norm_back(grad_key_gained * gain_key, key_normed, key_scale).astype(BF16)
    grad_proj = jnp.concatenate(
        [
            grad_query_proj.reshape(lines * rows, Q_COLS),
            grad_key_proj.reshape(lines * rows, HEAD_DIM),
            grad_value_proj.reshape(lines * rows, HEAD_DIM),
        ],
        axis=1,
    )
    hidden_one_part = dot(grad_proj, weight_qkv.T)
    grad_gain_attn = jnp.sum(hidden_one_part * attn_normed, axis=0)
    qkv_part = dot(hidden_one.T, grad_proj).astype(BF16)
    gains_local = jnp.concatenate([grad_gain_attn, grad_gain_ffn, grad_gain_query, grad_gain_key])
    gains_all, grad_hidden_one, qkv_part, output_grad = exchange(
        "sum_gradients",
        5,
        [
            ("gather", "all", padded(gains_local, 16 * 128)),
            ("reduce", "line", hidden_one_part.astype(BF16).reshape(lines, rows, D)),
            ("reduce", "swap", qkv_part.reshape(lines, -1, 2, own_rows, width)),
            ("reduce", "plane", output_part.reshape(-1, 2, output_weight.shape[0], D)),
        ],
    )
    own_scale = rms_scale(own_inputs)
    own_normed = own_inputs * own_scale
    input_grad = grad_residual + norm_back(grad_hidden_one * gain_attn, own_normed, own_scale)
    qkv_part = qkv_part.transpose(1, 0, 2).astype(F32)
    query_grad = qkv_part[:, :, :Q_COLS].reshape(own_rows, lines * Q_COLS)
    key_grad = qkv_part[:, :, Q_COLS : Q_COLS + HEAD_DIM].reshape(own_rows, lines * HEAD_DIM)
    value_grad = qkv_part[:, :, Q_COLS + HEAD_DIM :].reshape(own_rows, lines * HEAD_DIM)
    share = norm_gains.shape[0]
    gains_all = gains_all.reshape(experts, -1)
    gains_all = lax.dynamic_slice_in_dim(gains_all, me * share, share, axis=1)
    gains_grad = jnp.sum(gains_all, axis=0)
    return (
        block_out,
        input_grad,
        query_grad,
        key_grad,
        value_grad,
        output_grad,
        router_grad,
        gains_grad,
        grad_gate[None].astype(F32),
        grad_up[None].astype(F32),
        grad_down[None].astype(F32),
    )


def solution(mesh):
    chips = mesh.shape["expert"]
    cores = mesh.shape["shard"]
    inner = Mesh(
        mesh.devices.reshape(KV_HEADS, chips // KV_HEADS, cores), ("line", "plane", "core")
    )
    return jax.shard_map(
        on_device,
        mesh=inner,
        in_specs=(
            P(ALL, None),
            P(ALL, None),
            P(ALL, None),
            P(ALL, None),
            P(ALL, None),
            P(ALL, None),
            P(ALL, None),
            P(ALL, None),
            P(ALL, None),
            P(ALL),
            P(ALL, None, None),
            P(ALL, None, None),
            P(ALL, None, None),
        ),
        out_specs=(
            P(ALL, None),
            P(ALL, None),
            P(ALL, None),
            P(ALL, None),
            P(ALL, None),
            P(ALL, None),
            P(ALL, None),
            P(ALL),
            P(ALL, None, None),
            P(ALL, None, None),
            P(ALL, None, None),
        ),
        check_vma=False,
    )
```

```python
import functools

import jax
import jax.numpy as jnp
from jax import lax
from jax.experimental import pallas as pl
from jax.experimental.pallas import tpu as pltpu
from jax.sharding import Mesh
from jax.sharding import PartitionSpec as P

D = 2048
HEADS = 32
KV_HEADS = 4
HEAD_DIM = 128
TOP = 8

epsilon = 1e-06
rope_base = 1000000.0
masked_score = -1e30

GROUPS = HEADS // KV_HEADS
Q_COLS = GROUPS * HEAD_DIM
LINE = "line"
PLANE = ("plane", "core")
ALL = ("line", "plane", "core")
F32 = jnp.float32
BF16 = jnp.bfloat16
MESH = pl.DeviceIdType.MESH
DMA = pltpu.SemaphoreType.DMA


def dot(left, right):
    return jnp.dot(left, right, preferred_element_type=F32)


def rms_scale(values):
    return lax.rsqrt(jnp.mean(values * values, axis=-1, keepdims=True) + epsilon)


def norm_back(upstream, normed, scale_rows):
    return scale_rows * (upstream - normed * jnp.mean(upstream * normed, axis=-1, keepdims=True))


def sequence_layout(lengths_row, row_count):
    seq_ends = jnp.cumsum(lengths_row)
    places = jnp.arange(row_count, dtype=jnp.int32)
    segment = jnp.sum((places[:, None] >= seq_ends[None, :]).astype(jnp.int32), axis=1)
    starts = seq_ends - lengths_row
    member = segment[:, None] == jnp.arange(lengths_row.shape[0], dtype=jnp.int32)[None, :]
    seg_start = jnp.sum(jnp.where(member, starts[None, :], 0), axis=1)
    return (segment, places - seg_start)


def rope_tables(positions, head_dim):
    half_dim = head_dim // 2
    inverse = rope_base ** (-2.0 * jnp.arange(half_dim, dtype=F32) / head_dim)
    angles = positions.astype(F32)[..., None] * inverse
    return (jnp.cos(angles), jnp.sin(angles))


def rotate(values, cosine, sine_table):
    half_dim = values.shape[-1] // 2
    first_half = values[..., :half_dim]
    second_half = values[..., half_dim:]
    return jnp.concatenate(
        [
            first_half * cosine - second_half * sine_table,
            second_half * cosine + first_half * sine_table,
        ],
        axis=-1,
    )


def masked_scores(query, keys, allowed, score_scale):
    scores = jnp.einsum("bqgd,bsd->bgqs", query, keys, preferred_element_type=F32) * score_scale
    return jnp.where(allowed[:, None], scores, masked_score)


def attend(query, keys, values_in, allowed, score_scale):
    scores = masked_scores(query, keys, allowed, score_scale)
    top_score = jnp.max(scores, axis=-1, keepdims=True)
    exponent = jnp.exp(scores - top_score)
    row_total = jnp.sum(exponent, axis=-1, keepdims=True)
    attn_probs = (exponent / row_total).astype(BF16)
    mixed_heads = jnp.einsum("bgqs,bsd->bqgd", attn_probs, values_in, preferred_element_type=F32)
    return (mixed_heads, top_score + jnp.log(row_total))


def attend_back(query, keys, values_in, allowed, score_scale, log_total, grad_mixed):
    scores = masked_scores(query, keys, allowed, score_scale)
    attn_probs = jnp.exp(scores - log_total)
    grad_probs = jnp.einsum("bqgd,bsd->bgqs", grad_mixed, values_in, preferred_element_type=F32)
    grad_scores = (
        attn_probs * (grad_probs - jnp.sum(attn_probs * grad_probs, axis=-1, keepdims=True))
    ).astype(BF16)
    grad_query = (
        jnp.einsum("bgqs,bsd->bqgd", grad_scores, keys, preferred_element_type=F32) * score_scale
    )
    grad_keys = (
        jnp.einsum("bgqs,bqgd->bsd", grad_scores, query, preferred_element_type=F32) * score_scale
    )
    grad_values = jnp.einsum(
        "bgqs,bqgd->bsd", attn_probs.astype(BF16), grad_mixed, preferred_element_type=F32
    )
    return (grad_query, grad_keys, grad_values)


class Spot:
    def __init__(self, lines):
        self.lines = lines
        self.z = lax.axis_index("line")
        self.b = lax.axis_index("plane")
        self.c = lax.axis_index("core")
        self.xn = self.b + 1 - 2 * (self.b % 2)
        self.yn = (self.b + 2) % 4
        self.dg = 3 - self.b

    def each(self, d, fn):
        if d == 0:
            fn(self.z, 0)
            return

        @pl.when(self.z - d >= 0)
        def _():
            fn(self.z - d, 1)

        @pl.when(self.z + d < self.lines)
        def _():
            fn(self.z + d, -1)

    def greet(self):
        sem = pltpu.get_barrier_semaphore()

        def tell(dev):
            pl.semaphore_signal(sem, inc=1, device_id=dev, device_id_type=MESH)

        tell((self.z, self.xn, self.c))
        tell((self.z, self.yn, self.c))
        tell((self.z, self.b, 1 - self.c))
        for d in range(1, self.lines):
            self.each(d, lambda zz, way: tell((zz, self.b, self.c)))
        pl.semaphore_wait(sem, self.lines + 2)


def send(src, dst, ssem, rsem, dev):
    return pltpu.make_async_remote_copy(
        src_ref=src, dst_ref=dst, send_sem=ssem, recv_sem=rsem, device_id=dev, device_id_type=MESH
    )


def gather_sems(mode, lines):
    n = 1 if mode == "plane" else lines
    return [DMA, DMA((2, n)), DMA((n,)), DMA((n, 8)), DMA((n, 8)), DMA((2, n, 3)), DMA((n, 3))]


def gather_parts(spot, x_ref, out_ref, sems, mode="all", even=False):
    own_sem, zs, zr, ps, pr, vs, vr = sems
    z, b, c, xn, yn, dg, lines = spot.z, spot.b, spot.c, spot.xn, spot.yn, spot.dg, spot.lines
    here = (z, b, c)
    rows = out_ref.shape[-2]
    flat = mode == "plane"
    planar = mode != "line"
    relayed = mode in ("all", "line")
    via = rows // 4 if even else 0
    last = pl.ds(rows - via, via)
    columns = (b, xn, yn, dg)

    def span(way):
        return rows if way == 0 else rows - via

    def lo(way):
        return pl.ds(0, span(way) // 2)

    def hi(way):
        return pl.ds(span(way) // 2, span(way) // 2)

    def blk(zz, bb, cc=c):
        if flat:
            return out_ref.at[bb, cc]
        return out_ref.at[zz, bb, cc] if planar else out_ref.at[zz]

    mine = 0 if flat else z

    def own():
        return x_ref.at[z] if mode == "swap" else x_ref

    def source(zz, way):
        return own() if way == 0 else blk(zz, b)

    def onward(way, fn):
        if way >= 0:

            @pl.when(z < lines - 1)
            def _():
                fn(0)

        if way <= 0:

            @pl.when(z > 0)
            def _():
                fn(1)

    def hop(zz, down, way):
        return send(source(zz, way), blk(zz, b), zs.at[down, zz], zr.at[zz], (z + 1 - 2 * down, b, c))

    def hop_via(zz, k, down):
        piece = blk(zz, columns[k]).at[last]
        return send(
            piece, piece, vs.at[down, zz, k - 1], vr.at[zz, k - 1], (z + 1 - 2 * down, b, c)
        )

    def plane_copies(zz, way):
        s, d = source(zz, way), blk(zz, b)
        whole = (s, d)
        if via and way != 0:
            s, d = s.at[pl.ds(0, span(way))], d.at[pl.ds(0, span(way))]
        return [
            send(s, d, ps.at[zz, 0], pr.at[zz, 0], (z, xn, c)),
            send(s, d, ps.at[zz, 1], pr.at[zz, 1], (z, yn, c)),
            send(*whole, ps.at[zz, 4], pr.at[zz, 4], (z, b, 1 - c)),
        ]

    def cross(zz, k, way):
        if k == 0:
            piece = blk(zz, yn).at[lo(way)]
            return send(piece, piece, ps.at[zz, 2], pr.at[zz, 2], (z, xn, c))
        piece = blk(zz, xn).at[hi(way)]
        return send(piece, piece, ps.at[zz, 3], pr.at[zz, 3], (z, yn, c))

    def share(zz, k):
        piece = blk(zz, columns[k])
        return send(piece, piece, ps.at[zz, 4 + k], pr.at[zz, 4 + k], (z, b, 1 - c))

    def received(piece, sem):
        send(piece, piece, own_sem, sem, here).wait_recv()

    def over_line(zz, k, way):
        if not via:
            return
        if way != 0:
            received(blk(zz, columns[k]).at[last], vr.at[zz, k - 1])
        onward(way, lambda down: hop_via(zz, k, down).start())

    def start():
        pltpu.make_async_copy(own(), blk(mine, b), own_sem).start()
        if relayed:
            onward(0, lambda down: hop(z, down, 0).start())
        if mode == "swap":
            for d in range(lines - 1, 0, -1):
                spot.each(
                    d,
                    lambda zz, way: send(
                        x_ref.at[zz], blk(z, b), zs.at[0, zz], zr.at[z], (zz, b, c)
                    ).start(),
                )
        if planar:
            for copy in plane_copies(mine, 0):
                copy.start()

    def line_arrive(zz, way):
        received(blk(zz, b), zr.at[zz])
        if relayed:
            onward(way, lambda down: hop(zz, down, way).start())
        if planar:
            for copy in plane_copies(zz, way):
                copy.start()

    def plane_arrive(zz, way):
        part = pl.ds(0, span(way))
        received(blk(zz, xn).at[part], pr.at[zz, 0])
        cross(zz, 1, way).start()
        received(blk(zz, yn).at[part], pr.at[zz, 1])
        cross(zz, 0, way).start()
        over_line(zz, 1, way)
        over_line(zz, 2, way)
        share(zz, 1).start()
        share(zz, 2).start()

    def cross_arrive(zz, way):
        received(blk(zz, dg).at[lo(way)], pr.at[zz, 2])
        received(blk(zz, dg).at[hi(way)], pr.at[zz, 3])
        over_line(zz, 3, way)
        share(zz, 3).start()

    def drain(zz, way):
        if planar:
            for k in range(4):
                share(zz, k).wait_send()
            for copy in plane_copies(zz, way)[:2]:
                copy.wait_send()
            cross(zz, 0, way).wait_send()
            cross(zz, 1, way).wait_send()
        if relayed:
            onward(way, lambda down: hop(zz, down, way).wait_send())
        if via:
            for k in (1, 2, 3):
                onward(way, lambda down, k=k: hop_via(zz, k, down).wait_send())
        if mode == "swap" and way != 0:
            send(x_ref.at[zz], blk(z, b), zs.at[0, zz], zr.at[z], (zz, b, c)).wait_send()

    def shared(zz, k):
        received(blk(zz, columns[k], 1 - c), pr.at[zz, 4 + k])

    def end():
        pltpu.make_async_copy(own(), blk(mine, b), own_sem).wait()

    return {
        "start": start,
        "line": line_arrive,
        "plane": plane_arrive,
        "cross": cross_arrive,
        "shared": shared,
        "drain": drain,
        "end": end,
    }


def gather(spot, mode, x_ref, out_ref, sems):
    parts = gather_parts(spot, x_ref, out_ref, sems, mode)
    flat = mode == "plane"
    planar = mode != "line"
    steps = 1 if flat else spot.lines

    def each(d, fn):
        if flat:
            fn(0, 0)
        else:
            spot.each(d, fn)

    def drain(zz, way):
        if planar:
            for k in range(4):
                parts["shared"](zz, k)
        parts["drain"](zz, way)

    parts["start"]()
    yield
    for s in range(1, steps + 2 if planar else steps):
        if s < steps:
            each(s, parts["line"])
        if planar and 0 <= s - 1 < steps:
            each(s - 1, parts["plane"])
        if planar and 0 <= s - 2 < steps:
            each(s - 2, parts["cross"])
        yield
    for d in range(steps):
        each(d, drain)
    parts["end"]()
    yield


def reduce_scratch(mode, lines, rows, cols, dtype=BF16):
    n = 1 if mode == "plane" else lines
    out = []
    if mode != "line":
        out += [
            pltpu.VMEM((n, 4, rows, cols), dtype),
            pltpu.VMEM((n, 2, rows // 2, cols), dtype),
            pltpu.VMEM((n, 2, rows, cols), dtype),
            DMA((n, 8)),
            DMA((n, 8)),
        ]
    if mode == "line":
        out += [pltpu.VMEM((2, lines, rows, cols), dtype), pltpu.VMEM((lines, rows, cols), dtype)]
    if mode == "all":
        out += [pltpu.VMEM((lines, rows, cols), dtype)]
    if mode != "plane":
        out += [DMA((2, lines)), DMA((2, lines))]
    return out


def add_into(dst, *parts, chunk=16):
    rows = dst.shape[0]

    @pl.loop(0, rows // chunk)
    def _(i):
        at = pl.ds(pl.multiple_of(i * chunk, chunk), chunk)
        total = parts[0][at].astype(F32)
        for part in parts[1:]:
            total = total + part[at].astype(F32)
        dst[at] = total.astype(dst.dtype)


def reduce_parts(spot, mode, term, out_ref, scratch):
    z, b, c, xn, yn = spot.z, spot.b, spot.c, spot.xn, spot.yn
    here = (z, b, c)
    scratch = list(scratch)
    pair, crossed, met, ps, pr = scratch[:5]
    passed = scratch[5] if mode == "all" else out_ref
    zs, zr = scratch[-2:]
    rows = pair.shape[-2]
    lo, hi = pl.ds(0, rows // 2), pl.ds(rows // 2, rows // 2)

    def total(zz):
        return met.at[zz, 0]

    def share(zz, k):
        return send(
            term(zz, k, 1 - c), pair.at[zz, k], ps.at[zz, k], pr.at[zz, k], (z, b, 1 - c)
        )

    def cross(zz, k):
        piece = pair.at[zz, 3, (lo, hi)[k]]
        dev = (z, (yn, xn)[k], c)
        return send(piece, crossed.at[zz, k], ps.at[zz, 4 + k], pr.at[zz, 4 + k], dev)

    def meet(zz, k):
        dev = (z, (xn, yn)[k], c)
        return send(pair.at[zz, 1 + k], met.at[zz, k], ps.at[zz, 6 + k], pr.at[zz, 6 + k], dev)

    def away(zz):
        return send(total(zz), passed.at[z], zs.at[0, zz], zr.at[0, z], (zz, b, c))

    def received(piece, sem):
        send(piece, piece, ps.at[0, 0], sem, here).wait_recv()

    def start_one(zz, k):
        share(zz, k).start()

    def first_one(zz, k):
        received(pair.at[zz, k], pr.at[zz, k])
        add_into(pair.at[zz, k], pair.at[zz, k], term(zz, k, c))
        if k == 3:
            cross(zz, 0).start()
            cross(zz, 1).start()

    def start(zz, way):
        for k in (3, 1, 2, 0):
            start_one(zz, k)

    def first(zz, way):
        for k in (3, 1, 2):
            first_one(zz, k)

    def second(zz, way):
        received(crossed.at[zz, 0], pr.at[zz, 4])
        add_into(pair.at[zz, 1, lo], pair.at[zz, 1, lo], crossed.at[zz, 0])
        meet(zz, 0).start()
        received(crossed.at[zz, 1], pr.at[zz, 5])
        add_into(pair.at[zz, 2, hi], pair.at[zz, 2, hi], crossed.at[zz, 1])
        meet(zz, 1).start()

    def third(zz, way):
        received(pair.at[zz, 0], pr.at[zz, 0])
        received(met.at[zz, 0], pr.at[zz, 6])
        received(met.at[zz, 1], pr.at[zz, 7])
        dst = out_ref if mode == "plane" else total(zz)
        add_into(dst, met.at[zz, 0], met.at[zz, 1], pair.at[zz, 0], term(zz, 0, c))
        if mode != "plane":

            @pl.when(zz != z)
            def _():
                away(zz).start()

    def end():
        if mode == "plane":
            return
        for d in range(1, spot.lines):
            spot.each(d, lambda zz, way: received(passed.at[zz], zr.at[0, zz]))
        if mode == "swap":
            add_into(out_ref.at[z], total(z))
            return
        for edge in range(spot.lines):

            @pl.when(z == edge)
            def _():
                others = [passed.at[q] for q in range(spot.lines) if q != edge]
                add_into(out_ref, total(edge), *others)

    def sent(zz, way):
        for k in range(4):
            share(zz, k).wait_send()

    def drain(zz, way):
        for k in range(2):
            cross(zz, k).wait_send()
            meet(zz, k).wait_send()
        if mode != "plane" and way != 0:
            away(zz).wait_send()

    return {
        "start": start,
        "first": first,
        "start one": start_one,
        "first one": first_one,
        "second": second,
        "third": third,
        "sent": sent,
        "end": end,
        "drain": drain,
    }


def reduce(spot, mode, p_ref, out_ref, scratch):
    flat = mode == "plane"
    steps = 1 if flat else spot.lines

    columns = (spot.b, spot.xn, spot.yn, spot.dg)

    def term(zz, k, cc):
        return p_ref.at[columns[k], cc] if flat else p_ref.at[zz, columns[k], cc]

    def each(d, fn):
        if flat:
            fn(0, 0)
        else:
            spot.each(d, fn)

    parts = reduce_parts(spot, mode, term, out_ref, scratch)
    order = list(range(steps - 1, -1, -1))
    for d in order:
        each(d, parts["start"])
    yield
    for s in range(steps + 2):
        for lag, name in enumerate(("first", "second", "third")):
            if 0 <= s - lag < steps:
                each(order[s - lag], parts[name])
                yield
    parts["end"]()
    for d in range(steps):
        each(d, parts["sent"])
        each(d, parts["drain"])
    yield


def reduce_line(spot, p_ref, out_ref, scratch):
    passed, total_ref, zs, zr = scratch
    z, b, c, lines = spot.z, spot.b, spot.c, spot.lines
    here = (z, b, c)

    def received(down, zz):
        piece = passed.at[down, zz]
        send(piece, piece, zs.at[0, 0], zr.at[down, zz], here).wait_recv()

    def hop(src, zz, down):
        return send(
            src.at[zz], passed.at[down, zz], zs.at[down, zz], zr.at[down, zz], (z + 1 - 2 * down, b, c)
        )

    def step(zz, way):
        down = 1 if way > 0 else 0
        first_one = (z == lines - 1) if down else (z == 0)

        @pl.when(jnp.logical_not(first_one))
        def _():
            received(down, zz)
            add_into(total_ref.at[zz], p_ref.at[zz], passed.at[down, zz])
            hop(total_ref, zz, down).start()

        @pl.when(first_one)
        def _():
            hop(p_ref, zz, down).start()

    for d in range(lines - 1, 0, -1):
        spot.each(d, step)
        yield

    @pl.when(z > 0)
    def _():
        received(0, z)

    @pl.when(z < lines - 1)
    def _():
        received(1, z)

    @pl.when(z == 0)
    def _():
        add_into(out_ref, p_ref.at[z], passed.at[1, z])

    @pl.when(z == lines - 1)
    def _():
        add_into(out_ref, p_ref.at[z], passed.at[0, z])

    @pl.when((z > 0) & (z < lines - 1))
    def _():
        add_into(out_ref, p_ref.at[z], passed.at[0, z], passed.at[1, z])

    for d in range(1, lines):
        spot.each(d, lambda zz, way: hop(total_ref, zz, 1 if way > 0 else 0).wait_send())
    yield


def dot_tn(left, right):
    return lax.dot_general(left, right, (((0,), (0,)), ((), ())), preferred_element_type=F32)


def products_scratch(count, width, ff):
    return [
        pltpu.VMEM((3, count, ff), BF16),
        pltpu.VMEM((2, count, 256), BF16),
        pltpu.VMEM((2, 2, 256, ff), BF16),
        pltpu.VMEM((2, ff, 256), BF16),
        DMA((3,)),
        DMA((2,)),
        DMA((2, 2)),
        DMA((2,)),
    ]


def products(ins, outs, scratch):
    x_ref, dy_ref, a_ref, dg_ref, du_ref = ins
    gate_out, up_out, down_out = outs
    near, tile, wide, tall, n_sem, t_sem, w_sem, d_sem = scratch
    half = x_ref.shape[1] // 256

    def columns(n):
        return pl.ds((n % half) * 256, 256)

    def load(n):
        src = x_ref if n < half else dy_ref
        return pltpu.make_async_copy(src.at[:, columns(n)], tile.at[n % 2], t_sem.at[n % 2])

    def store(n):
        q = n % 2
        if n < half:
            return [
                pltpu.make_async_copy(wide.at[q, 0], gate_out.at[columns(n)], w_sem.at[q, 0]),
                pltpu.make_async_copy(wide.at[q, 1], up_out.at[columns(n)], w_sem.at[q, 1]),
            ]
        return [pltpu.make_async_copy(tall.at[q], down_out.at[:, columns(n)], d_sem.at[q])]

    near_loads = [
        pltpu.make_async_copy(src, near.at[i], n_sem.at[i])
        for i, src in enumerate((a_ref, dg_ref, du_ref))
    ]
    for copy in near_loads:
        copy.start()
    load(0).start()
    yield
    for copy in near_loads:
        copy.wait()
    for n in range(2 * half):
        load(n).wait()
        if n + 1 < 2 * half:
            load(n + 1).start()
        if n % half >= 2:
            for copy in store(n - 2):
                copy.wait()
        q = n % 2
        if n < half:
            wide[q, 0] = dot_tn(tile[q], near[1]).astype(BF16)
            wide[q, 1] = dot_tn(tile[q], near[2]).astype(BF16)
        else:
            tall[q] = dot_tn(near[0], tile[q]).astype(BF16)
        for copy in store(n):
            copy.start()
        if n % 3 == 2:
            yield
    for n in (half - 2, half - 1, 2 * half - 2, 2 * half - 1):
        for copy in store(n):
            copy.wait()
    yield


def run_steps(makers):
    live = list(makers)
    while live:
        for g in list(live):
            try:
                next(g)
            except StopIteration:
                live.remove(g)

def backward_scratch(lines, rows, width):
    return [
        *gather_sems("line", lines),
        pltpu.VMEM((Q_COLS, width), BF16),
        pltpu.VMEM((lines, rows, width), BF16),
        pltpu.VMEM((lines * rows, Q_COLS), BF16),
        pltpu.VMEM((GROUPS * rows, HEAD_DIM), BF16),
        pltpu.VMEM((GROUPS * rows, HEAD_DIM), BF16),
        DMA((2,)),
    ]


def backward(spot, ins, outs, scratch):
    (own_ref, wo_ref, q_ref, k_ref, v_ref, lse_ref, mask_ref, cos_ref, sin_ref, proj_ref, gain_ref) = ins
    rows_ref, out_ref, gain_out = outs
    wo, near, mixed, query, upstream, sem = scratch[-6:]
    lines, rows = near.shape[:2]
    score_scale = HEAD_DIM ** (-0.5)
    bring = pltpu.make_async_copy(wo_ref, wo, sem.at[0])
    bring.start()
    gain_out[...] = jnp.zeros_like(gain_out)
    yield from gather(spot, "line", own_ref, rows_ref, scratch[:-6])
    load = pltpu.make_async_copy(rows_ref, near, sem.at[1])
    load.start()
    bring.wait()
    load.wait()
    for j in range(Q_COLS // 256):
        part = pl.ds(j * 256, 256)
        full = dot_nt(near[...].reshape(lines * rows, near.shape[2]), wo[part, :])
        mixed[:, part] = full.astype(BF16)
        if j % 2:
            yield

    def norm_part(i, grad, columns, which):
        turned = grad * cos_ref[i] + pltpu.roll(grad, HEAD_DIM // 2, axis=1) * sin_ref[i]
        x = proj_ref[i, :, columns]
        scale = rms_scale(x)
        normed = x * scale
        at = pl.ds(which, 1)
        gain_out[at, :] = gain_out[at, :] + jnp.sum(turned * normed, axis=0, keepdims=True)
        up = turned * gain_ref[at, :]
        out_ref[i, :, columns] = norm_back(up, normed, scale).astype(BF16)

    for i in range(lines):
        keys, values = k_ref[i], v_ref[i]
        for h in range(GROUPS):
            at, columns = pl.ds(h * rows, rows), pl.ds(h * HEAD_DIM, HEAD_DIM)
            query[at, :] = q_ref[i, :, columns]
            upstream[at, :] = mixed[pl.ds(i * rows, rows), columns]
        scores = dot_nt(query[...], keys) * score_scale
        allowed = jnp.concatenate([mask_ref[i]] * GROUPS, axis=0) > 0.5
        probs = jnp.where(allowed, jnp.exp(scores - lse_ref[i]), 0.0)
        grad_probs = dot_nt(upstream[...], values)
        mean = jnp.sum(probs * grad_probs, axis=1, keepdims=True)
        grad_scores = (probs * (grad_probs - mean)).astype(BF16)
        grad_query = jnp.dot(grad_scores, keys, preferred_element_type=F32) * score_scale
        grad_keys = dot_tn(grad_scores, query[...]) * score_scale
        grad_values = dot_tn(probs.astype(BF16), upstream[...])
        yield
        for h in range(GROUPS):
            part = grad_query[h * rows : (h + 1) * rows]
            norm_part(i, part, pl.ds(h * HEAD_DIM, HEAD_DIM), 0)
        norm_part(i, grad_keys, pl.ds(Q_COLS, HEAD_DIM), 1)
        out_ref[i, :, pl.ds(Q_COLS + HEAD_DIM, HEAD_DIM)] = grad_values.astype(BF16)
        yield


def exchange(name, cid, jobs):
    lines = lax.axis_size("line")
    cells = lax.axis_size("plane") * lax.axis_size("core")
    if cells != 8 or lines != 4:
        return [exchange_by_xla(kind, mode, x, lines, cells) for kind, mode, x in jobs]
    far, near = pl.BlockSpec(memory_space=pl.ANY), pl.BlockSpec(memory_space=pltpu.VMEM)
    args, in_specs, out_shapes, out_specs, scratch, counts = [], [], [], [], [], []
    for kind, mode, x in jobs:
        if kind == "products":
            width, ff = x[0].shape[1], x[2].shape[1]
            args += x
            in_specs += [far] * 5
            out_shapes += [jax.ShapeDtypeStruct((width, ff), BF16)] * 2
            out_shapes.append(jax.ShapeDtypeStruct((ff, width), BF16))
            out_specs += [far] * 3
            own = products_scratch(x[0].shape[0], width, ff)
            counts.append((5, 3, len(own)))
            scratch += own
            continue
        if kind == "backward":
            rows, width = x[0].shape
            args += x
            in_specs += [far] * 2 + [near] * 9
            out_shapes.append(jax.ShapeDtypeStruct((lines, rows, width), BF16))
            out_shapes.append(jax.ShapeDtypeStruct((lines, rows, x[9].shape[2]), BF16))
            out_shapes.append(jax.ShapeDtypeStruct((8, HEAD_DIM), F32))
            out_specs += [far, near, near]
            own = backward_scratch(lines, rows, width)
            counts.append((11, 3, len(own)))
            scratch += own
            continue
        rows, cols = x.shape[-2:]
        spec = near if kind == "reduce" else far
        args.append(x)
        in_specs.append(spec)
        if kind == "gather":
            lead = {"line": (lines,), "plane": (4, 2)}.get(mode, (lines, 4, 2))
            out_shapes.append(jax.ShapeDtypeStruct((*lead, rows, cols), x.dtype))
            own = gather_sems(mode, lines)
        else:
            if mode == "swap":
                out_shapes.append(jax.ShapeDtypeStruct((lines, rows, cols), x.dtype))
            else:
                out_shapes.append(jax.ShapeDtypeStruct((rows, cols), F32))
            own = reduce_scratch(mode, lines, rows, cols, x.dtype)
        out_specs.append(spec)
        scratch += own
        counts.append((1, 1, len(own)))
    kinds = [(kind, mode) for kind, mode, _ in jobs]

    def body(*refs):
        spot = Spot(lines)
        spot.greet()
        ins, outs, rest = 0, len(args), len(args) + len(out_shapes)
        makers = []
        for (kind, mode), (n_in, n_out, n_rest) in zip(kinds, counts):
            i, o, w = refs[ins : ins + n_in], refs[outs : outs + n_out], refs[rest : rest + n_rest]
            ins, outs, rest = ins + n_in, outs + n_out, rest + n_rest
            if kind == "products":
                makers.append(products(i, o, w))
            elif kind == "backward":
                makers.append(backward(spot, i, o, w))
            elif kind == "gather":
                makers.append(gather(spot, mode, i[0], o[0], w))
            elif mode == "line":
                makers.append(reduce_line(spot, i[0], o[0], w))
            else:
                makers.append(reduce(spot, mode, i[0], o[0], w))
        run_steps(makers)

    outs = pl.pallas_call(
        body,
        out_shape=tuple(out_shapes),
        in_specs=in_specs,
        out_specs=tuple(out_specs),
        scratch_shapes=scratch,
        compiler_params=pltpu.CompilerParams(
            collective_id=cid, has_side_effects=True, vmem_limit_bytes=67_000_000
        ),
        name=name,
    )(*args)
    results, at = [], 0
    for _, n_out, _ in counts:
        results.append(outs[at] if n_out == 1 else outs[at : at + n_out])
        at += n_out
    return results


def exchange_by_xla(kind, mode, x, lines, cells):
    if kind == "products":
        hidden, grad_slots, acts, grad_gate, grad_up = x
        return dot(hidden.T, grad_gate), dot(hidden.T, grad_up), dot(acts.T, grad_slots)
    rows, cols = x.shape[-2:]
    if kind == "gather":
        if mode == "swap":
            x = lax.all_to_all(x, LINE, split_axis=0, concat_axis=0, tiled=True)
            return lax.all_gather(x, PLANE, axis=1)
        return lax.all_gather(x, {"line": LINE, "plane": PLANE, "all": ALL}[mode])
    if mode == "swap":
        x = x.reshape(lines, cells, rows, cols).transpose(1, 0, 2, 3)
        x = lax.psum_scatter(x, PLANE, scatter_dimension=0, tiled=True)
        x = x.reshape(lines, rows, cols)
        return lax.all_to_all(x, LINE, split_axis=0, concat_axis=0, tiled=True)
    x = x.reshape(-1, cols)
    axes = {"line": LINE, "plane": PLANE, "all": ALL}[mode]
    return lax.psum_scatter(x, axes, scatter_dimension=0, tiled=True).astype(F32)


def padded(flat, unit):
    size = -(-flat.shape[0] // unit) * unit
    return jnp.pad(flat, (0, size - flat.shape[0])).reshape(-1, 128)


def pick_order(z, i):
    far = z // 2
    near = z * (1 - far) + (3 - z) * far
    place = (near + i) % 2 if i < 2 else i
    return place * (1 - far) + (3 - place) * far


def dot_nt(left, right):
    return lax.dot_general(left, right, (((1,), (1,)), ((), ())), preferred_element_type=F32)


def experts_body(capacity, *refs):
    lines = 4
    (h_ref, tall, own_w_ref, sel_ref, spread_ref, gate_ref, up_ref, down_ref) = refs[:8]
    (hall, py, dw_all, w_ref, sum_ref, x_out, dy_out, a_out, dg_out, du_out) = refs[8:18]
    rest = list(refs[18:])
    h_sems, w_sems, dw_sems = rest[:7], rest[7:14], rest[14:21]
    sum_scratch = rest[21:29]
    (wg, wu, wd, hb, tb, xs, zs, dys, acts, dgs, dus, rs, ys) = rest[29:42]
    (stage, stage_y, slot_w, acc, dw_ref, w_sem, l_sem, o_sem, p_sem) = rest[42:]
    spot = Spot(lines)
    z, b, c, xn, yn, dg_spot = spot.z, spot.b, spot.c, spot.xn, spot.yn, spot.dg
    me = (z * 4 + b) * 2 + c
    pair = 2 * capacity
    spot.greet()
    steps_h = gather_parts(spot, h_ref, hall, h_sems, even=True)
    steps_w = gather_parts(spot, own_w_ref, w_ref, w_sems)
    steps_dw = gather_parts(spot, dw_ref, dw_all, dw_sems)
    both = (steps_w, steps_h)
    columns = (b, xn, yn, dg_spot)
    turn = [0]

    def term(zz, k, cc):
        return stage.at[turn[0] % 2, k, cc]

    steps_r = reduce_parts(spot, "all", term, sum_ref, sum_scratch)

    def sums(name, i, k=1):
        turn[0] = i
        steps_r[name](pick_order(z, i), k)

    def comm_dw(name, d):
        spot.each(d, steps_dw[name])

    loads = [
        pltpu.make_async_copy(gate_ref, wg, w_sem.at[0]),
        pltpu.make_async_copy(up_ref, wu, w_sem.at[1]),
        pltpu.make_async_copy(down_ref, wd, w_sem.at[2]),
    ]

    def comm(*names):
        for s in both:
            for name in names:
                part, d = name.split()
                spot.each(int(d), s[part])

    def load(n):
        i, k = n // 4, n % 4
        zz, bb = pick_order(z, i), columns[k]
        return [
            pltpu.make_async_copy(hall.at[zz, bb], hb.at[n % 3], l_sem.at[0, n % 3]),
            pltpu.make_async_copy(tall.at[zz, bb], tb.at[n % 3], l_sem.at[1, n % 3]),
        ]

    def fetch(n):
        i, k = n // 4, n % 4
        zz = pick_order(z, i)
        for s in both:
            s["shared"](zz, k)
        for copy in load(n):
            copy.start()

    def pick(n):
        i, k = n // 4, n % 4
        zz, bb = pick_order(z, i), columns[k]
        at = pl.ds(pl.multiple_of(bb * pair, 16), pair)
        which = zz * 4 + bb
        for copy in load(n):
            copy.wait()
        rows = hb.shape[2]
        width = hb.shape[3]
        mine = jnp.concatenate(
            [w_ref[zz, bb, 0, pl.ds(me, 1), :], w_ref[zz, bb, 1, pl.ds(me, 1), :]], axis=1
        )
        select = sel_ref[which]
        per_slot = jnp.sum(select.astype(F32) * mine, axis=1, keepdims=True)
        slot_w[i % 2, at, :] = jnp.broadcast_to(per_slot, (pair, 128))

        @pl.loop(0, width // 512)
        def _(j):
            part = pl.ds(pl.multiple_of(j * 512, 512), 512)
            h = hb[n % 3, :, :, part].reshape(2 * rows, 512)
            t = tb[n % 3, :, :, part].reshape(2 * rows, 512)
            xs[i % 2, at, part] = jnp.dot(select, h, preferred_element_type=F32).astype(BF16)
            t = jnp.dot(select, t, preferred_element_type=F32)
            zs[i % 2, at, part] = t.astype(BF16)
            dys[i % 2, at, part] = (per_slot * t).astype(BF16)

    def keep(i):
        zz = pick_order(z, i)
        q = i % 2
        return [
            pltpu.make_async_copy(xs.at[q], x_out.at[zz], o_sem.at[q, 0]),
            pltpu.make_async_copy(dys.at[q], dy_out.at[zz], o_sem.at[q, 1]),
            pltpu.make_async_copy(acts.at[q], a_out.at[zz], o_sem.at[q, 2]),
            pltpu.make_async_copy(dgs.at[q], dg_out.at[zz], o_sem.at[q, 3]),
            pltpu.make_async_copy(dus.at[q], du_out.at[zz], o_sem.at[q, 4]),
        ]

    def inner(i):
        q = i % 2

        @pl.loop(0, wg.shape[1] // 256)
        def _(j):
            part = pl.ds(pl.multiple_of(j * 256, 256), 256)
            g = jnp.dot(xs[q], wg[:, part], preferred_element_type=F32)
            u = jnp.dot(xs[q], wu[:, part], preferred_element_type=F32)
            da = dot_nt(dys[q], wd[part, :])
            sig = jax.nn.sigmoid(g)
            silu = g * sig
            acts[q, :, part] = (silu * u).astype(BF16)
            dgs[q, :, part] = (da * u * sig * (1.0 + g * (1.0 - sig))).astype(BF16)
            dus[q, :, part] = (da * silu).astype(BF16)

        for copy in keep(i):
            copy.start()

    def outer(i):
        q = i % 2
        acc[...] = jnp.zeros_like(acc)

        @pl.loop(0, wg.shape[0] // 256)
        def _(j):
            part = pl.ds(pl.multiple_of(j * 256, 256), 256)
            r = dot_nt(dgs[q], wg[part, :]) + dot_nt(dus[q], wu[part, :])
            rs[:, part] = r.astype(BF16)
            y = jnp.dot(acts[q], wd[:, part], preferred_element_type=F32)
            y = y.astype(BF16).astype(F32)
            met = y * zs[q, :, part].astype(F32)
            acc[...] += met[:, :128] + met[:, 128:]
            ys[:, part] = (slot_w[q, :, 0:1] * y).astype(BF16)

    def put(zz, bb, m):
        return pltpu.make_async_copy(stage_y.at[m % 2], py.at[zz, bb], p_sem.at[m % 2])

    def place(i, k, m):
        zz, bb = pick_order(z, i), columns[k]
        at = pl.ds(pl.multiple_of(bb * pair, 16), pair)
        which = zz * 4 + bb
        if m >= 2:
            put(zz, bb, m).wait()
        dw_slot = jnp.sum(acc[at, :], axis=1, keepdims=True)
        dw_ref[pl.ds(which, 1), :] = jnp.sum(
            sel_ref[which].astype(F32) * dw_slot, axis=0, keepdims=True
        )
        spread = spread_ref[which]
        rows = stage.shape[3]

        @pl.loop(0, rs.shape[1] // 512)
        def _(j):
            part = pl.ds(pl.multiple_of(j * 512, 512), 512)
            full = jnp.dot(spread, rs[at, part], preferred_element_type=F32)
            stage[i % 2, k, :, :, part] = full.astype(BF16).reshape(2, rows, 512)
            full = jnp.dot(spread, ys[at, part], preferred_element_type=F32)
            stage_y[m % 2, :, :, part] = full.astype(BF16).reshape(2, rows, 512)

        put(zz, bb, m).start()

    def places(i):
        order = (3, 1, 2, 0)
        for n, k in enumerate(order):
            place(i, k, 4 * i + n)
            if n >= 1:
                sums("start one", i, order[n - 1])
            if n >= 2:
                sums("first one", i, order[n - 2])
        sums("start one", i, 0)
        sums("first one", i, 2)

    def kept(i):
        for copy in keep(i):
            copy.wait()

    for s in both:
        s["start"]()
    for copy in loads:
        copy.start()
    for s in both:
        s["end"]()
    fetch(0)
    comm("line 1", "plane 0")
    fetch(1)
    fetch(2)
    pick(0)
    pick(1)
    comm("cross 0")
    fetch(3)
    pick(2)
    comm("line 2")
    fetch(4)
    pick(3)
    for copy in loads:
        copy.wait()
    inner(0)
    comm("plane 1")
    fetch(5)
    fetch(6)
    pick(4)
    outer(0)
    pick(5)
    pick(6)
    comm("line 3", "cross 1")
    fetch(7)
    places(0)
    pick(7)
    inner(1)
    kept(0)
    comm("plane 2")
    fetch(8)
    fetch(9)
    fetch(10)
    pick(8)
    pick(9)
    pick(10)
    sums("second", 0)
    outer(1)
    comm("cross 2")
    fetch(11)
    places(1)
    sums("third", 0)
    comm("plane 3")
    fetch(12)
    fetch(13)
    pick(11)
    inner(2)
    kept(1)
    sums("second", 1)
    fetch(14)
    pick(12)
    pick(13)
    pick(14)
    outer(2)
    comm("cross 3")
    fetch(15)
    sums("sent", 0)
    places(2)
    sums("third", 1)
    pick(15)
    inner(3)
    sums("second", 2)
    outer(3)
    sums("sent", 1)
    places(3)
    steps_dw["start"]()
    sums("third", 2)
    sums("second", 3)
    comm_dw("line", 1)
    comm_dw("plane", 0)
    comm_dw("line", 2)
    comm_dw("plane", 1)
    comm_dw("cross", 0)
    comm_dw("line", 3)
    comm_dw("plane", 2)
    comm_dw("cross", 1)
    sums("third", 3)
    comm_dw("plane", 3)
    comm_dw("cross", 2)
    comm_dw("cross", 3)
    steps_r["end"]()
    for m in (0, 1):
        put(z, b, m).wait()
    for i in (2, 3):
        kept(i)
        sums("sent", i)
    for d in range(lines):
        comm(f"drain {d}")
        comm_dw("drain", d)
        spot.each(d, steps_r["drain"])
        for k in range(4):
            spot.each(d, lambda zz, way, k=k: steps_dw["shared"](zz, k))
    steps_dw["end"]()


def experts_call(hidden_two, cotangent_all, own_weights, routes_all, gate, up, down, capacity):
    lines, experts = 4, 32
    rows, width = hidden_two.shape
    ff = gate.shape[1]
    pair = 2 * capacity
    group = 4 * pair
    me = (lax.axis_index("line") * 4 + lax.axis_index("plane")) * 2 + lax.axis_index("core")
    mine = jnp.any(routes_all == me, axis=1).reshape(experts, rows)
    rank = jnp.cumsum(mine.astype(jnp.int32), axis=1) - 1
    slot = rank + (jnp.arange(experts, dtype=jnp.int32) % 2 * capacity)[:, None]
    slot = jnp.where(mine, slot, -1).reshape(experts // 2, 2 * rows)
    places = jnp.arange(pair, dtype=jnp.int32)
    select = (slot[:, None, :] == places[None, :, None]).astype(BF16)
    spread = (slot[:, :, None] == places[None, None, :]).astype(BF16)
    anywhere = pl.BlockSpec(memory_space=pl.ANY)
    near = pl.BlockSpec(memory_space=pltpu.VMEM)
    all_rows = jax.ShapeDtypeStruct((lines, 4, 2, rows, width), BF16)
    wide = jax.ShapeDtypeStruct((lines, group, width), BF16)
    thin = jax.ShapeDtypeStruct((lines, group, ff), BF16)
    return pl.pallas_call(
        functools.partial(experts_body, capacity),
        out_shape=(
            all_rows,
            all_rows,
            jax.ShapeDtypeStruct((lines, 4, 2, experts // 2, 2 * rows), F32),
            jax.ShapeDtypeStruct((lines, 4, 2, experts, rows), F32),
            jax.ShapeDtypeStruct((rows, width), F32),
            wide,
            wide,
            thin,
            thin,
            thin,
        ),
        in_specs=[anywhere, anywhere, near, near, near, anywhere, anywhere, anywhere],
        out_specs=(*[anywhere] * 3, near, near, *[anywhere] * 5),
        scratch_shapes=[
            *gather_sems("all", lines),
            *gather_sems("all", lines),
            *gather_sems("all", lines),
            *reduce_scratch("all", lines, rows, width),
            pltpu.VMEM((width, ff), BF16),
            pltpu.VMEM((width, ff), BF16),
            pltpu.VMEM((ff, width), BF16),
            pltpu.VMEM((3, 2, rows, width), BF16),
            pltpu.VMEM((3, 2, rows, width), BF16),
            pltpu.VMEM((2, group, width), BF16),
            pltpu.VMEM((2, group, width), BF16),
            pltpu.VMEM((2, group, width), BF16),
            pltpu.VMEM((2, group, ff), BF16),
            pltpu.VMEM((2, group, ff), BF16),
            pltpu.VMEM((2, group, ff), BF16),
            pltpu.VMEM((group, width), BF16),
            pltpu.VMEM((group, width), BF16),
            pltpu.VMEM((2, 4, 2, rows, width), BF16),
            pltpu.VMEM((2, 2, rows, width), BF16),
            pltpu.VMEM((2, group, 128), F32),
            pltpu.VMEM((group, 128), F32),
            pltpu.VMEM((experts // 2, 2 * rows), F32),
            DMA((3,)),
            DMA((2, 3)),
            DMA((2, 5)),
            DMA((2,)),
        ],
        compiler_params=pltpu.CompilerParams(
            collective_id=2, has_side_effects=True, vmem_limit_bytes=67_000_000
        ),
        name="experts",
    )(hidden_two, cotangent_all, own_weights, select, spread, gate, up, down)


def experts_by_xla(
    hidden_two, cotangent, own_weights, routes_all, gate, up, down, capacity, me, experts
):
    rows = hidden_two.shape[0]
    hidden_all = lax.all_gather(hidden_two, ALL, axis=0, tiled=True)
    gathered = lax.all_gather(own_weights, ALL)
    expert_ids = jnp.arange(experts, dtype=jnp.int32)
    weights_all = gathered.transpose(0, 2, 1).reshape(experts * rows, experts)
    mine = jnp.any(routes_all == me, axis=1).reshape(experts, rows)
    weight_mine = jnp.sum(jnp.where(expert_ids == me, weights_all, 0.0), axis=1).reshape(
        experts, rows
    )
    rank = jnp.cumsum(mine.astype(jnp.int32), axis=1) - 1
    slots = jnp.arange(capacity, dtype=jnp.int32)
    select = (rank[:, None, :] == slots[None, :, None]) & mine[:, None, :]
    select_low = select.astype(BF16)
    slot_weight = jnp.sum(jnp.where(select, weight_mine[:, None, :], 0.0), axis=2).reshape(-1, 1)

    def pick(values):
        return jnp.einsum(
            "sjt,std->sjd",
            select_low,
            values.reshape(experts, rows, D),
            preferred_element_type=F32,
        ).reshape(experts * capacity, D)

    def place(values):
        return (
            jnp.einsum(
                "sjt,sjd->std",
                select_low,
                values.reshape(experts, capacity, D),
                preferred_element_type=F32,
            )
            .astype(BF16)
            .reshape(experts * rows, D)
        )

    expert_rows = pick(hidden_all).astype(BF16)
    own_width = D // experts
    own_columns = lax.dynamic_slice_in_dim(hidden_all, me * own_width, own_width, axis=1)
    expert_rows, own_columns, cotangent = lax.optimization_barrier(
        (expert_rows, own_columns, cotangent)
    )
    cotangent_all = lax.all_gather(cotangent, ALL, axis=0, tiled=True)
    grad_rows_out = pick(cotangent_all)
    grad_slots = (slot_weight * grad_rows_out).astype(BF16)
    gate_act = dot(expert_rows, gate)
    up_act = dot(expert_rows, up)
    gate_sig = jax.nn.sigmoid(gate_act)
    gate_silu = gate_act * gate_sig
    expert_hidden = (gate_silu * up_act).astype(BF16)
    grad_expert_hidden = dot(grad_slots, down.T)
    grad_gate_act = (
        grad_expert_hidden * up_act * gate_sig * (1.0 + gate_act * (1.0 - gate_sig))
    ).astype(BF16)
    grad_up_act = (grad_expert_hidden * gate_silu).astype(BF16)
    grad_rows_in = (dot(grad_gate_act, gate.T) + dot(grad_up_act, up.T)).astype(BF16)
    expert_out = dot(expert_hidden, down).astype(BF16).astype(F32)
    grad_weight_slot = jnp.sum(grad_rows_out * expert_out, axis=1).reshape(experts, capacity)
    grad_weight_mine = jnp.sum(jnp.where(select, grad_weight_slot[:, :, None], 0.0), axis=1)
    out_rows = (slot_weight * expert_out).astype(BF16)

    placed = place(grad_rows_in).reshape(experts, rows, D)
    grad_weight, grad_rows_sum = exchange(
        "sum_rows", 3, [("gather", "all", grad_weight_mine), ("reduce", "all", placed)]
    )
    placed_out = place(lax.optimization_barrier((out_rows, grad_rows_sum))[0])
    return (
        own_columns,
        placed_out,
        grad_weight,
        gathered,
        grad_rows_sum,
        expert_rows,
        grad_slots,
        expert_hidden,
        grad_gate_act,
        grad_up_act,
    )


def on_device(
    tokens,
    lengths,
    routes,
    cotangent,
    query_weight,
    key_weight,
    value_weight,
    output_weight,
    router_weight,
    norm_gains,
    gate_weight,
    up_weight,
    down_weight,
):
    rows = tokens.shape[0]
    lines = lax.axis_size("line")
    cells = lax.axis_size("plane") * lax.axis_size("core")
    experts = lines * cells
    capacity = (3 * rows * TOP + 2 * experts - 1) // (2 * experts)
    score_scale = HEAD_DIM ** (-0.5)
    large = experts > 32
    own_rows = query_weight.shape[0]
    line = lax.axis_index("line")
    me = (line * lax.axis_size("plane") + lax.axis_index("plane")) * lax.axis_size(
        "core"
    ) + lax.axis_index("core")

    packed = jnp.concatenate(
        [
            query_weight.reshape(own_rows, lines, Q_COLS),
            key_weight.reshape(own_rows, lines, HEAD_DIM),
            value_weight.reshape(own_rows, lines, HEAD_DIM),
        ],
        axis=2,
    ).transpose(1, 0, 2)
    width = packed.shape[2]
    floats = padded(jnp.concatenate([router_weight.reshape(-1), norm_gains]), 32 * 128)
    whole_numbers = padded(jnp.concatenate([routes.reshape(-1), lengths.reshape(-1)]), 16 * 128)
    floats_all, numbers_all, weight_qkv, line_tokens, weight_o = exchange(
        "gather_inputs",
        0,
        [
            ("gather", "all", floats),
            ("gather", "all", whole_numbers),
            ("gather", "swap", packed),
            ("gather", "line", tokens),
            ("gather", "plane", output_weight),
        ],
    )
    weight_qkv = weight_qkv.reshape(lines * cells * own_rows, width)
    weight_o = weight_o.reshape(cells * output_weight.shape[0], D)
    floats_all = floats_all.reshape(experts, -1)
    router_size = own_rows * experts
    router = floats_all[:, :router_size].reshape(D, experts)
    gains = floats_all[:, router_size : router_size + norm_gains.shape[0]].reshape(-1).astype(F32)
    numbers_all = numbers_all.reshape(experts, -1)
    routes_all = numbers_all[:, : rows * TOP].reshape(experts * rows, TOP)
    lengths_all = numbers_all[:, rows * TOP : rows * TOP + lengths.shape[1]]
    line_lengths = lax.dynamic_slice_in_dim(
        lengths_all.reshape(lines, cells, -1), me % cells, 1, axis=1
    )[:, 0]
    gain_attn = gains[:D]
    gain_ffn = gains[D : 2 * D]
    gain_query = gains[2 * D : 2 * D + HEAD_DIM]
    gain_key = gains[2 * D + HEAD_DIM :]

    inputs = line_tokens.reshape(lines * rows, D).astype(F32)
    attn_scale = rms_scale(inputs)
    attn_normed = inputs * attn_scale
    hidden_one = (attn_normed * gain_attn).astype(BF16)
    proj = dot(hidden_one, weight_qkv)
    query_proj = proj[:, :Q_COLS].reshape(lines, rows, GROUPS, HEAD_DIM)
    key_proj = proj[:, Q_COLS : Q_COLS + HEAD_DIM].reshape(lines, rows, HEAD_DIM)
    value_proj = proj[:, Q_COLS + HEAD_DIM :].astype(BF16).reshape(lines, rows, HEAD_DIM)
    query_scale = rms_scale(query_proj)
    query_normed = query_proj * query_scale
    key_scale = rms_scale(key_proj)
    key_normed = key_proj * key_scale
    segment, positions = jax.vmap(lambda row: sequence_layout(row, rows))(line_lengths)
    cosine, sine_table = rope_tables(positions, HEAD_DIM)
    query_rot = rotate(
        query_normed * gain_query, cosine[:, :, None], sine_table[:, :, None]
    ).astype(BF16)
    key_rot = rotate(key_normed * gain_key, cosine, sine_table).astype(BF16)
    allowed = (segment[:, :, None] == segment[:, None, :]) & (
        positions[:, None, :] <= positions[:, :, None]
    )
    mixed_heads, log_total = attend(query_rot, key_rot, value_proj, allowed, score_scale)
    mixed_low = mixed_heads.reshape(lines * rows, Q_COLS).astype(BF16)
    projected = dot(mixed_low, weight_o).astype(BF16).reshape(lines, rows, D)
    jobs = [("reduce", "line", projected)]
    if not large:
        jobs.insert(0, ("gather", "all", cotangent))
    *cotangent_all, projected = exchange("sum_residual", 1, jobs)
    cotangent_all = None if large else cotangent_all[0]
    own_inputs = tokens.astype(F32)
    residual = own_inputs + projected
    ffn_scale = rms_scale(residual)
    ffn_normed = residual * ffn_scale
    hidden_two = (ffn_normed * gain_ffn).astype(BF16)

    expert_ids = jnp.arange(experts, dtype=jnp.int32)
    named = jnp.any(routes[:, :, None] == expert_ids, axis=1).T
    logits = lax.dot_general(
        router, hidden_two, (((0,), (1,)), ((), ())), preferred_element_type=F32
    )
    masked = jnp.where(named, logits, masked_score)
    exponent = jnp.where(named, jnp.exp(masked - jnp.max(masked, axis=0, keepdims=True)), 0.0)
    own_weights = exponent / jnp.sum(exponent, axis=0, keepdims=True)
    weights = (gate_weight[0], up_weight[0], down_weight[0])
    if large:
        done = experts_by_xla(
            hidden_two, cotangent, own_weights, routes_all, *weights, capacity, me, experts
        )
    else:
        done = experts_call(
            hidden_two, cotangent_all, own_weights, routes_all, *weights, capacity
        )
    hidden_all, placed_out, grad_weight, weights_all, grad_rows_sum = done[:5]
    weights_all = weights_all.reshape(experts, experts, rows).transpose(1, 0, 2)
    weights_all = weights_all.reshape(experts, experts * rows)
    kept = [v.reshape(-1, v.shape[-1]) for v in done[5:]]
    if large:
        own_columns = hidden_all
    else:
        hidden_all = hidden_all.reshape(experts * rows, D)
        own_columns = lax.dynamic_slice_in_dim(hidden_all, me * own_rows, own_rows, axis=1)
    grad_weight = grad_weight.reshape(experts, experts * rows)

    grad_logits = weights_all * (
        grad_weight - jnp.sum(weights_all * grad_weight, axis=0, keepdims=True)
    )
    grad_logits = grad_logits.astype(BF16)
    router_grad = lax.dot_general(
        own_columns, grad_logits, (((0,), (1,)), ((), ())), preferred_element_type=F32
    )
    own_grad_logits = lax.dynamic_slice_in_dim(grad_logits, me * rows, rows, axis=1).T

    grad_out = cotangent.astype(F32)
    grad_hidden_two = dot(own_grad_logits, router.T) + grad_rows_sum.astype(F32)
    grad_gain_ffn = jnp.sum(grad_hidden_two * ffn_normed, axis=0)
    grad_residual = grad_out + norm_back(grad_hidden_two * gain_ffn, ffn_normed, ffn_scale)
    grad_low = grad_residual.astype(BF16)
    jobs = [
        ("reduce", "all", placed_out.reshape(lines, -1, 2, rows, D)),
        ("products", "", kept),
    ]
    if large:
        jobs.insert(0, ("gather", "line", grad_low))
    else:
        turn_back = [jnp.concatenate([v, w], axis=-1) for v, w in ((cosine, cosine), (sine_table, -sine_table))]
        given = (
            grad_low,
            weight_o,
            query_rot.reshape(lines, rows, Q_COLS),
            key_rot,
            value_proj,
            log_total.reshape(lines, GROUPS * rows, 1),
            allowed.astype(F32),
            *turn_back,
            proj.reshape(lines, rows, width),
            jnp.pad(gains[2 * D :].reshape(2, HEAD_DIM), ((0, 6), (0, 0))),
        )
        jobs.insert(0, ("backward", "", given))
    came, out_sum, (grad_gate, grad_up, grad_down) = exchange("gather_grad", 4, jobs)
    block_out = (residual + out_sum).astype(BF16)
    grad_attn = (came if large else came[0]).reshape(lines * rows, D)
    output_part = dot(mixed_low.T, grad_attn).astype(BF16)
    if large:
        grad_mixed = dot(grad_attn, weight_o.T).astype(BF16).reshape(lines, rows, GROUPS, HEAD_DIM)
        grad_query_rot, grad_key_rot, grad_value_rot = attend_back(
            query_rot, key_rot, value_proj, allowed, score_scale, log_total, grad_mixed
        )
        grad_value_proj = grad_value_rot.astype(BF16)
        grad_query_gained = rotate(grad_query_rot, cosine[:, :, None], -sine_table[:, :, None])
        grad_gain_query = jnp.sum(grad_query_gained * query_normed, axis=(0, 1, 2))
        grad_query_proj = norm_back(grad_query_gained * gain_query, query_normed, query_scale).astype(
            BF16
        )
        grad_key_gained = rotate(grad_key_rot, cosine, -sine_table)
        grad_gain_key = jnp.sum(grad_key_gained * key_normed, axis=(0, 1))
        grad_key_proj = norm_back(grad_key_gained * gain_key, key_normed, key_scale).astype(BF16)
        grad_proj = jnp.concatenate(
            [
                grad_query_proj.reshape(lines * rows, Q_COLS),
                grad_key_proj.reshape(lines * rows, HEAD_DIM),
                grad_value_proj.reshape(lines * rows, HEAD_DIM),
            ],
            axis=1,
        )
    else:
        grad_proj = came[1].reshape(lines * rows, width)
        grad_gain_query, grad_gain_key = came[2][0], came[2][1]
    hidden_one_part = dot(grad_proj, weight_qkv.T)
    grad_gain_attn = jnp.sum(hidden_one_part * attn_normed, axis=0)
    qkv_part = dot(hidden_one.T, grad_proj).astype(BF16)
    gains_local = jnp.concatenate([grad_gain_attn, grad_gain_ffn, grad_gain_query, grad_gain_key])
    gains_all, grad_hidden_one, qkv_part, output_grad = exchange(
        "sum_gradients",
        5,
        [
            ("gather", "all", padded(gains_local, 16 * 128)),
            ("reduce", "line", hidden_one_part.astype(BF16).reshape(lines, rows, D)),
            ("reduce", "swap", qkv_part.reshape(lines, -1, 2, own_rows, width)),
            ("reduce", "plane", output_part.reshape(-1, 2, output_weight.shape[0], D)),
        ],
    )
    own_scale = rms_scale(own_inputs)
    own_normed = own_inputs * own_scale
    input_grad = grad_residual + norm_back(grad_hidden_one * gain_attn, own_normed, own_scale)
    qkv_part = qkv_part.transpose(1, 0, 2).astype(F32)
    query_grad = qkv_part[:, :, :Q_COLS].reshape(own_rows, lines * Q_COLS)
    key_grad = qkv_part[:, :, Q_COLS : Q_COLS + HEAD_DIM].reshape(own_rows, lines * HEAD_DIM)
    value_grad = qkv_part[:, :, Q_COLS + HEAD_DIM :].reshape(own_rows, lines * HEAD_DIM)
    share = norm_gains.shape[0]
    gains_all = gains_all.reshape(experts, -1)
    gains_all = lax.dynamic_slice_in_dim(gains_all, me * share, share, axis=1)
    gains_grad = jnp.sum(gains_all, axis=0)
    return (
        block_out,
        input_grad,
        query_grad,
        key_grad,
        value_grad,
        output_grad,
        router_grad,
        gains_grad,
        grad_gate[None].astype(F32),
        grad_up[None].astype(F32),
        grad_down[None].astype(F32),
    )


def solution(mesh):
    chips = mesh.shape["expert"]
    cores = mesh.shape["shard"]
    inner = Mesh(
        mesh.devices.reshape(KV_HEADS, chips // KV_HEADS, cores), ("line", "plane", "core")
    )
    return jax.shard_map(
        on_device,
        mesh=inner,
        in_specs=(
            P(ALL, None),
            P(ALL, None),
            P(ALL, None),
            P(ALL, None),
            P(ALL, None),
            P(ALL, None),
            P(ALL, None),
            P(ALL, None),
            P(ALL, None),
            P(ALL),
            P(ALL, None, None),
            P(ALL, None, None),
            P(ALL, None, None),
        ),
        out_specs=(
            P(ALL, None),
            P(ALL, None),
            P(ALL, None),
            P(ALL, None),
            P(ALL, None),
            P(ALL, None),
            P(ALL, None),
            P(ALL),
            P(ALL, None, None),
            P(ALL, None, None),
            P(ALL, None, None),
        ),
        check_vma=False,
    )
```

```python
import functools

import jax
import jax.numpy as jnp
from jax import lax
from jax.experimental import pallas as pl
from jax.experimental.pallas import tpu as pltpu
from jax.sharding import Mesh
from jax.sharding import PartitionSpec as P

D = 2048
HEADS = 32
KV_HEADS = 4
HEAD_DIM = 128
TOP = 8

epsilon = 1e-06
rope_base = 1000000.0
masked_score = -1e30

GROUPS = HEADS // KV_HEADS
Q_COLS = GROUPS * HEAD_DIM
LINE = "line"
PLANE = ("plane", "core")
ALL = ("line", "plane", "core")
F32 = jnp.float32
BF16 = jnp.bfloat16
MESH = pl.DeviceIdType.MESH
DMA = pltpu.SemaphoreType.DMA


def dot(left, right):
    return jnp.dot(left, right, preferred_element_type=F32)


def rms_scale(values):
    return lax.rsqrt(jnp.mean(values * values, axis=-1, keepdims=True) + epsilon)


def norm_back(upstream, normed, scale_rows):
    return scale_rows * (upstream - normed * jnp.mean(upstream * normed, axis=-1, keepdims=True))


def sequence_layout(lengths_row, row_count):
    seq_ends = jnp.cumsum(lengths_row)
    places = jnp.arange(row_count, dtype=jnp.int32)
    segment = jnp.sum((places[:, None] >= seq_ends[None, :]).astype(jnp.int32), axis=1)
    starts = seq_ends - lengths_row
    member = segment[:, None] == jnp.arange(lengths_row.shape[0], dtype=jnp.int32)[None, :]
    seg_start = jnp.sum(jnp.where(member, starts[None, :], 0), axis=1)
    return (segment, places - seg_start)


def rope_tables(positions, head_dim):
    half_dim = head_dim // 2
    inverse = rope_base ** (-2.0 * jnp.arange(half_dim, dtype=F32) / head_dim)
    angles = positions.astype(F32)[..., None] * inverse
    return (jnp.cos(angles), jnp.sin(angles))


def rotate(values, cosine, sine_table):
    half_dim = values.shape[-1] // 2
    first_half = values[..., :half_dim]
    second_half = values[..., half_dim:]
    return jnp.concatenate(
        [
            first_half * cosine - second_half * sine_table,
            second_half * cosine + first_half * sine_table,
        ],
        axis=-1,
    )


def masked_scores(query, keys, allowed, score_scale):
    scores = jnp.einsum("bqgd,bsd->bgqs", query, keys, preferred_element_type=F32) * score_scale
    return jnp.where(allowed[:, None], scores, masked_score)


def attend(query, keys, values_in, allowed, score_scale):
    scores = masked_scores(query, keys, allowed, score_scale)
    top_score = jnp.max(scores, axis=-1, keepdims=True)
    exponent = jnp.exp(scores - top_score)
    row_total = jnp.sum(exponent, axis=-1, keepdims=True)
    attn_probs = (exponent / row_total).astype(BF16)
    mixed_heads = jnp.einsum("bgqs,bsd->bqgd", attn_probs, values_in, preferred_element_type=F32)
    return (mixed_heads, top_score + jnp.log(row_total))


def attend_back(query, keys, values_in, allowed, score_scale, log_total, grad_mixed):
    scores = masked_scores(query, keys, allowed, score_scale)
    attn_probs = jnp.exp(scores - log_total)
    grad_probs = jnp.einsum("bqgd,bsd->bgqs", grad_mixed, values_in, preferred_element_type=F32)
    grad_scores = (
        attn_probs * (grad_probs - jnp.sum(attn_probs * grad_probs, axis=-1, keepdims=True))
    ).astype(BF16)
    grad_query = (
        jnp.einsum("bgqs,bsd->bqgd", grad_scores, keys, preferred_element_type=F32) * score_scale
    )
    grad_keys = (
        jnp.einsum("bgqs,bqgd->bsd", grad_scores, query, preferred_element_type=F32) * score_scale
    )
    grad_values = jnp.einsum(
        "bgqs,bqgd->bsd", attn_probs.astype(BF16), grad_mixed, preferred_element_type=F32
    )
    return (grad_query, grad_keys, grad_values)


class Spot:
    def __init__(self, lines):
        self.lines = lines
        self.z = lax.axis_index("line")
        self.b = lax.axis_index("plane")
        self.c = lax.axis_index("core")
        self.xn = self.b + 1 - 2 * (self.b % 2)
        self.yn = (self.b + 2) % 4
        self.dg = 3 - self.b

    def each(self, d, fn):
        if d == 0:
            fn(self.z, 0)
            return

        @pl.when(self.z - d >= 0)
        def _():
            fn(self.z - d, 1)

        @pl.when(self.z + d < self.lines)
        def _():
            fn(self.z + d, -1)

    def greet(self):
        sem = pltpu.get_barrier_semaphore()

        def tell(dev):
            pl.semaphore_signal(sem, inc=1, device_id=dev, device_id_type=MESH)

        tell((self.z, self.xn, self.c))
        tell((self.z, self.yn, self.c))
        tell((self.z, self.b, 1 - self.c))
        for d in range(1, self.lines):
            self.each(d, lambda zz, way: tell((zz, self.b, self.c)))
        pl.semaphore_wait(sem, self.lines + 2)


def send(src, dst, ssem, rsem, dev):
    return pltpu.make_async_remote_copy(
        src_ref=src, dst_ref=dst, send_sem=ssem, recv_sem=rsem, device_id=dev, device_id_type=MESH
    )


def gather_sems(mode, lines):
    n = 1 if mode == "plane" else lines
    return [DMA, DMA((2, n)), DMA((n,)), DMA((n, 8)), DMA((n, 8)), DMA((2, n, 3)), DMA((n, 3))]


def gather_parts(spot, x_ref, out_ref, sems, mode="all", even=False, direct=False):
    own_sem, zs, zr, ps, pr, vs, vr = sems
    z, b, c, xn, yn, dg, lines = spot.z, spot.b, spot.c, spot.xn, spot.yn, spot.dg, spot.lines
    here = (z, b, c)
    rows = out_ref.shape[-2]
    flat = mode == "plane"
    planar = mode != "line"
    relayed = mode in ("all", "line") and not direct
    via = rows // 4 if even else 0
    last = pl.ds(rows - via, via)
    columns = (b, xn, yn, dg)

    def span(way):
        return rows if way == 0 else rows - via

    def lo(way):
        return pl.ds(0, span(way) // 2)

    def hi(way):
        return pl.ds(span(way) // 2, span(way) // 2)

    def blk(zz, bb, cc=c):
        if flat:
            return out_ref.at[bb, cc]
        return out_ref.at[zz, bb, cc] if planar else out_ref.at[zz]

    mine = 0 if flat else z

    def own():
        return x_ref.at[z] if mode == "swap" else x_ref

    def source(zz, way):
        return own() if way == 0 else blk(zz, b)

    def onward(way, fn):
        if way >= 0:

            @pl.when(z < lines - 1)
            def _():
                fn(0)

        if way <= 0:

            @pl.when(z > 0)
            def _():
                fn(1)

    def hop(zz, down, way):
        return send(source(zz, way), blk(zz, b), zs.at[down, zz], zr.at[zz], (z + 1 - 2 * down, b, c))

    def hop_via(zz, k, down):
        piece = blk(zz, columns[k]).at[last]
        return send(
            piece, piece, vs.at[down, zz, k - 1], vr.at[zz, k - 1], (z + 1 - 2 * down, b, c)
        )

    def plane_copies(zz, way):
        s, d = source(zz, way), blk(zz, b)
        whole = (s, d)
        if via and way != 0:
            s, d = s.at[pl.ds(0, span(way))], d.at[pl.ds(0, span(way))]
        return [
            send(s, d, ps.at[zz, 0], pr.at[zz, 0], (z, xn, c)),
            send(s, d, ps.at[zz, 1], pr.at[zz, 1], (z, yn, c)),
            send(*whole, ps.at[zz, 4], pr.at[zz, 4], (z, b, 1 - c)),
        ]

    def cross(zz, k, way):
        if k == 0:
            piece = blk(zz, yn).at[lo(way)]
            return send(piece, piece, ps.at[zz, 2], pr.at[zz, 2], (z, xn, c))
        piece = blk(zz, xn).at[hi(way)]
        return send(piece, piece, ps.at[zz, 3], pr.at[zz, 3], (z, yn, c))

    def share(zz, k):
        piece = blk(zz, columns[k])
        return send(piece, piece, ps.at[zz, 4 + k], pr.at[zz, 4 + k], (z, b, 1 - c))

    def received(piece, sem):
        send(piece, piece, own_sem, sem, here).wait_recv()

    def over_line(zz, k, way):
        if not via:
            return
        if way != 0:
            received(blk(zz, columns[k]).at[last], vr.at[zz, k - 1])
        onward(way, lambda down: hop_via(zz, k, down).start())

    def straight(zz):
        src = x_ref.at[zz] if mode == "swap" else x_ref
        return send(src, blk(z, b), zs.at[0, zz], zr.at[z], (zz, b, c))

    def start():
        pltpu.make_async_copy(own(), blk(mine, b), own_sem).start()
        if relayed:
            onward(0, lambda down: hop(z, down, 0).start())
        if mode == "swap" or direct:
            for d in range(lines - 1, 0, -1):
                spot.each(d, lambda zz, way: straight(zz).start())
        if planar:
            for copy in plane_copies(mine, 0):
                copy.start()

    def line_arrive(zz, way):
        received(blk(zz, b), zr.at[zz])
        if relayed:
            onward(way, lambda down: hop(zz, down, way).start())
        if planar:
            for copy in plane_copies(zz, way):
                copy.start()

    def plane_arrive(zz, way):
        part = pl.ds(0, span(way))
        received(blk(zz, xn).at[part], pr.at[zz, 0])
        cross(zz, 1, way).start()
        received(blk(zz, yn).at[part], pr.at[zz, 1])
        cross(zz, 0, way).start()
        over_line(zz, 1, way)
        over_line(zz, 2, way)
        share(zz, 1).start()
        share(zz, 2).start()

    def cross_arrive(zz, way):
        received(blk(zz, dg).at[lo(way)], pr.at[zz, 2])
        received(blk(zz, dg).at[hi(way)], pr.at[zz, 3])
        over_line(zz, 3, way)
        share(zz, 3).start()

    def drain(zz, way):
        if planar:
            for k in range(4):
                share(zz, k).wait_send()
            for copy in plane_copies(zz, way)[:2]:
                copy.wait_send()
            cross(zz, 0, way).wait_send()
            cross(zz, 1, way).wait_send()
        if relayed:
            onward(way, lambda down: hop(zz, down, way).wait_send())
        if via:
            for k in (1, 2, 3):
                onward(way, lambda down, k=k: hop_via(zz, k, down).wait_send())
        if (mode == "swap" or direct) and way != 0:
            straight(zz).wait_send()

    def shared(zz, k):
        received(blk(zz, columns[k], 1 - c), pr.at[zz, 4 + k])

    def end():
        pltpu.make_async_copy(own(), blk(mine, b), own_sem).wait()

    return {
        "start": start,
        "line": line_arrive,
        "plane": plane_arrive,
        "cross": cross_arrive,
        "shared": shared,
        "drain": drain,
        "end": end,
    }


def gather(spot, mode, x_ref, out_ref, sems):
    parts = gather_parts(spot, x_ref, out_ref, sems, mode)
    flat = mode == "plane"
    planar = mode != "line"
    steps = 1 if flat else spot.lines

    def each(d, fn):
        if flat:
            fn(0, 0)
        else:
            spot.each(d, fn)

    def drain(zz, way):
        if planar:
            for k in range(4):
                parts["shared"](zz, k)
        parts["drain"](zz, way)

    parts["start"]()
    yield
    for s in range(1, steps + 2 if planar else steps):
        if s < steps:
            each(s, parts["line"])
        if planar and 0 <= s - 1 < steps:
            each(s - 1, parts["plane"])
        if planar and 0 <= s - 2 < steps:
            each(s - 2, parts["cross"])
        yield
    for d in range(steps):
        each(d, drain)
    parts["end"]()
    yield


def reduce_scratch(mode, lines, rows, cols, dtype=BF16):
    n = 1 if mode == "plane" else lines
    out = []
    if mode != "line":
        out += [
            pltpu.VMEM((n, 4, rows, cols), dtype),
            pltpu.VMEM((n, 2, rows // 2, cols), dtype),
            pltpu.VMEM((n, 2, rows, cols), dtype),
            DMA((n, 8)),
            DMA((n, 8)),
        ]
    if mode == "line":
        out += [pltpu.VMEM((2, lines, rows, cols), dtype), pltpu.VMEM((lines, rows, cols), dtype)]
    if mode == "all":
        out += [pltpu.VMEM((lines, rows, cols), dtype)]
    if mode != "plane":
        out += [DMA((2, lines)), DMA((2, lines))]
    return out


def add_into(dst, *parts, chunk=16):
    rows = dst.shape[0]

    @pl.loop(0, rows // chunk)
    def _(i):
        at = pl.ds(pl.multiple_of(i * chunk, chunk), chunk)
        total = parts[0][at].astype(F32)
        for part in parts[1:]:
            total = total + part[at].astype(F32)
        dst[at] = total.astype(dst.dtype)


def reduce_parts(spot, mode, term, out_ref, scratch):
    z, b, c, xn, yn = spot.z, spot.b, spot.c, spot.xn, spot.yn
    here = (z, b, c)
    scratch = list(scratch)
    pair, crossed, met, ps, pr = scratch[:5]
    passed = scratch[5] if mode == "all" else out_ref
    zs, zr = scratch[-2:]
    rows = pair.shape[-2]
    lo, hi = pl.ds(0, rows // 2), pl.ds(rows // 2, rows // 2)

    def total(zz):
        return met.at[zz, 0]

    def share(zz, k):
        return send(
            term(zz, k, 1 - c), pair.at[zz, k], ps.at[zz, k], pr.at[zz, k], (z, b, 1 - c)
        )

    def cross(zz, k):
        piece = pair.at[zz, 3, (lo, hi)[k]]
        dev = (z, (yn, xn)[k], c)
        return send(piece, crossed.at[zz, k], ps.at[zz, 4 + k], pr.at[zz, 4 + k], dev)

    def meet(zz, k):
        dev = (z, (xn, yn)[k], c)
        return send(pair.at[zz, 1 + k], met.at[zz, k], ps.at[zz, 6 + k], pr.at[zz, 6 + k], dev)

    def away(zz):
        return send(total(zz), passed.at[z], zs.at[0, zz], zr.at[0, z], (zz, b, c))

    def received(piece, sem):
        send(piece, piece, ps.at[0, 0], sem, here).wait_recv()

    def start_one(zz, k):
        share(zz, k).start()

    def first_one(zz, k):
        received(pair.at[zz, k], pr.at[zz, k])
        add_into(pair.at[zz, k], pair.at[zz, k], term(zz, k, c))
        if k == 3:
            cross(zz, 0).start()
            cross(zz, 1).start()

    def start(zz, way):
        for k in (3, 1, 2, 0):
            start_one(zz, k)

    def first(zz, way):
        for k in (3, 1, 2):
            first_one(zz, k)

    def second(zz, way):
        received(crossed.at[zz, 0], pr.at[zz, 4])
        add_into(pair.at[zz, 1, lo], pair.at[zz, 1, lo], crossed.at[zz, 0])
        meet(zz, 0).start()
        received(crossed.at[zz, 1], pr.at[zz, 5])
        add_into(pair.at[zz, 2, hi], pair.at[zz, 2, hi], crossed.at[zz, 1])
        meet(zz, 1).start()

    def third(zz, way):
        received(pair.at[zz, 0], pr.at[zz, 0])
        received(met.at[zz, 0], pr.at[zz, 6])
        received(met.at[zz, 1], pr.at[zz, 7])
        dst = out_ref if mode == "plane" else total(zz)
        add_into(dst, met.at[zz, 0], met.at[zz, 1], pair.at[zz, 0], term(zz, 0, c))
        if mode != "plane":

            @pl.when(zz != z)
            def _():
                away(zz).start()

    def end():
        if mode == "plane":
            return
        for d in range(1, spot.lines):
            spot.each(d, lambda zz, way: received(passed.at[zz], zr.at[0, zz]))
        if mode == "swap":
            add_into(out_ref.at[z], total(z))
            return
        for edge in range(spot.lines):

            @pl.when(z == edge)
            def _():
                others = [passed.at[q] for q in range(spot.lines) if q != edge]
                add_into(out_ref, total(edge), *others)

    def sent(zz, way):
        for k in range(4):
            share(zz, k).wait_send()

    def drain(zz, way):
        for k in range(2):
            cross(zz, k).wait_send()
            meet(zz, k).wait_send()
        if mode != "plane" and way != 0:
            away(zz).wait_send()

    return {
        "start": start,
        "first": first,
        "start one": start_one,
        "first one": first_one,
        "second": second,
        "third": third,
        "sent": sent,
        "end": end,
        "drain": drain,
    }


def reduce(spot, mode, p_ref, out_ref, scratch):
    flat = mode == "plane"
    steps = 1 if flat else spot.lines

    columns = (spot.b, spot.xn, spot.yn, spot.dg)

    def term(zz, k, cc):
        return p_ref.at[columns[k], cc] if flat else p_ref.at[zz, columns[k], cc]

    def each(d, fn):
        if flat:
            fn(0, 0)
        else:
            spot.each(d, fn)

    parts = reduce_parts(spot, mode, term, out_ref, scratch)
    order = list(range(steps - 1, -1, -1))
    for d in order:
        each(d, parts["start"])
    yield
    for s in range(steps + 2):
        for lag, name in enumerate(("first", "second", "third")):
            if 0 <= s - lag < steps:
                each(order[s - lag], parts[name])
                yield
    parts["end"]()
    for d in range(steps):
        each(d, parts["sent"])
        each(d, parts["drain"])
    yield


def reduce_line(spot, p_ref, out_ref, scratch):
    passed, total_ref, zs, zr = scratch
    z, b, c, lines = spot.z, spot.b, spot.c, spot.lines
    here = (z, b, c)

    def received(down, zz):
        piece = passed.at[down, zz]
        send(piece, piece, zs.at[0, 0], zr.at[down, zz], here).wait_recv()

    def hop(src, zz, down):
        return send(
            src.at[zz], passed.at[down, zz], zs.at[down, zz], zr.at[down, zz], (z + 1 - 2 * down, b, c)
        )

    def step(zz, way):
        down = 1 if way > 0 else 0
        first_one = (z == lines - 1) if down else (z == 0)

        @pl.when(jnp.logical_not(first_one))
        def _():
            received(down, zz)
            add_into(total_ref.at[zz], p_ref.at[zz], passed.at[down, zz])
            hop(total_ref, zz, down).start()

        @pl.when(first_one)
        def _():
            hop(p_ref, zz, down).start()

    for d in range(lines - 1, 0, -1):
        spot.each(d, step)
        yield

    @pl.when(z > 0)
    def _():
        received(0, z)

    @pl.when(z < lines - 1)
    def _():
        received(1, z)

    @pl.when(z == 0)
    def _():
        add_into(out_ref, p_ref.at[z], passed.at[1, z])

    @pl.when(z == lines - 1)
    def _():
        add_into(out_ref, p_ref.at[z], passed.at[0, z])

    @pl.when((z > 0) & (z < lines - 1))
    def _():
        add_into(out_ref, p_ref.at[z], passed.at[0, z], passed.at[1, z])

    for d in range(1, lines):
        spot.each(d, lambda zz, way: hop(total_ref, zz, 1 if way > 0 else 0).wait_send())
    yield


def dot_tn(left, right):
    return lax.dot_general(left, right, (((0,), (0,)), ((), ())), preferred_element_type=F32)


def products_scratch(count, width, ff):
    return [
        pltpu.VMEM((3, count, ff), BF16),
        pltpu.VMEM((2, count, 256), BF16),
        pltpu.VMEM((2, 2, 256, ff), BF16),
        pltpu.VMEM((2, ff, 256), BF16),
        DMA((3,)),
        DMA((2,)),
        DMA((2, 2)),
        DMA((2,)),
    ]


def products(ins, outs, scratch):
    x_ref, dy_ref, a_ref, dg_ref, du_ref = ins
    gate_out, up_out, down_out = outs
    near, tile, wide, tall, n_sem, t_sem, w_sem, d_sem = scratch
    half = x_ref.shape[1] // 256

    def columns(n):
        return pl.ds((n % half) * 256, 256)

    def load(n):
        src = x_ref if n < half else dy_ref
        return pltpu.make_async_copy(src.at[:, columns(n)], tile.at[n % 2], t_sem.at[n % 2])

    def store(n):
        q = n % 2
        if n < half:
            return [
                pltpu.make_async_copy(wide.at[q, 0], gate_out.at[columns(n)], w_sem.at[q, 0]),
                pltpu.make_async_copy(wide.at[q, 1], up_out.at[columns(n)], w_sem.at[q, 1]),
            ]
        return [pltpu.make_async_copy(tall.at[q], down_out.at[:, columns(n)], d_sem.at[q])]

    near_loads = [
        pltpu.make_async_copy(src, near.at[i], n_sem.at[i])
        for i, src in enumerate((a_ref, dg_ref, du_ref))
    ]
    for copy in near_loads:
        copy.start()
    load(0).start()
    yield
    for copy in near_loads:
        copy.wait()
    for n in range(2 * half):
        load(n).wait()
        if n + 1 < 2 * half:
            load(n + 1).start()
        if n % half >= 2:
            for copy in store(n - 2):
                copy.wait()
        q = n % 2
        if n < half:
            wide[q, 0] = dot_tn(tile[q], near[1]).astype(BF16)
            wide[q, 1] = dot_tn(tile[q], near[2]).astype(BF16)
        else:
            tall[q] = dot_tn(near[0], tile[q]).astype(BF16)
        for copy in store(n):
            copy.start()
        if n % 3 == 2:
            yield
    for n in (half - 2, half - 1, 2 * half - 2, 2 * half - 1):
        for copy in store(n):
            copy.wait()
    yield


def run_steps(makers):
    live = list(makers)
    while live:
        for g in list(live):
            try:
                next(g)
            except StopIteration:
                live.remove(g)

def backward_scratch(lines, rows, width):
    return [
        *gather_sems("line", lines),
        pltpu.VMEM((Q_COLS, width), BF16),
        pltpu.VMEM((lines, rows, width), BF16),
        pltpu.VMEM((lines * rows, Q_COLS), BF16),
        pltpu.VMEM((GROUPS * rows, HEAD_DIM), BF16),
        pltpu.VMEM((GROUPS * rows, HEAD_DIM), BF16),
        DMA((2,)),
    ]


def backward(spot, ins, outs, scratch):
    (own_ref, wo_ref, q_ref, k_ref, v_ref, lse_ref, mask_ref, cos_ref, sin_ref, proj_ref, gain_ref) = ins
    rows_ref, out_ref, gain_out = outs
    wo, near, mixed, query, upstream, sem = scratch[-6:]
    lines, rows = near.shape[:2]
    score_scale = HEAD_DIM ** (-0.5)
    bring = pltpu.make_async_copy(wo_ref, wo, sem.at[0])
    bring.start()
    gain_out[...] = jnp.zeros_like(gain_out)
    yield from gather(spot, "line", own_ref, rows_ref, scratch[:-6])
    load = pltpu.make_async_copy(rows_ref, near, sem.at[1])
    load.start()
    bring.wait()
    load.wait()
    for j in range(Q_COLS // 256):
        part = pl.ds(j * 256, 256)
        full = dot_nt(near[...].reshape(lines * rows, near.shape[2]), wo[part, :])
        mixed[:, part] = full.astype(BF16)
        if j % 2:
            yield

    def norm_part(i, grad, columns, which):
        turned = grad * cos_ref[i] + pltpu.roll(grad, HEAD_DIM // 2, axis=1) * sin_ref[i]
        x = proj_ref[i, :, columns]
        scale = rms_scale(x)
        normed = x * scale
        at = pl.ds(which, 1)
        gain_out[at, :] = gain_out[at, :] + jnp.sum(turned * normed, axis=0, keepdims=True)
        up = turned * gain_ref[at, :]
        out_ref[i, :, columns] = norm_back(up, normed, scale).astype(BF16)

    for i in range(lines):
        keys, values = k_ref[i], v_ref[i]
        for h in range(GROUPS):
            at, columns = pl.ds(h * rows, rows), pl.ds(h * HEAD_DIM, HEAD_DIM)
            query[at, :] = q_ref[i, :, columns]
            upstream[at, :] = mixed[pl.ds(i * rows, rows), columns]
        scores = dot_nt(query[...], keys) * score_scale
        allowed = jnp.concatenate([mask_ref[i]] * GROUPS, axis=0) > 0.5
        probs = jnp.where(allowed, jnp.exp(scores - lse_ref[i]), 0.0)
        grad_probs = dot_nt(upstream[...], values)
        mean = jnp.sum(probs * grad_probs, axis=1, keepdims=True)
        grad_scores = (probs * (grad_probs - mean)).astype(BF16)
        grad_query = jnp.dot(grad_scores, keys, preferred_element_type=F32) * score_scale
        grad_keys = dot_tn(grad_scores, query[...]) * score_scale
        grad_values = dot_tn(probs.astype(BF16), upstream[...])
        yield
        for h in range(GROUPS):
            part = grad_query[h * rows : (h + 1) * rows]
            norm_part(i, part, pl.ds(h * HEAD_DIM, HEAD_DIM), 0)
        norm_part(i, grad_keys, pl.ds(Q_COLS, HEAD_DIM), 1)
        out_ref[i, :, pl.ds(Q_COLS + HEAD_DIM, HEAD_DIM)] = grad_values.astype(BF16)
        yield


def exchange(name, cid, jobs):
    lines = lax.axis_size("line")
    cells = lax.axis_size("plane") * lax.axis_size("core")
    if cells != 8 or lines != 4:
        return [exchange_by_xla(kind, mode, x, lines, cells) for kind, mode, x in jobs]
    far, near = pl.BlockSpec(memory_space=pl.ANY), pl.BlockSpec(memory_space=pltpu.VMEM)
    args, in_specs, out_shapes, out_specs, scratch, counts = [], [], [], [], [], []
    for kind, mode, x in jobs:
        if kind == "products":
            width, ff = x[0].shape[1], x[2].shape[1]
            args += x
            in_specs += [far] * 5
            out_shapes += [jax.ShapeDtypeStruct((width, ff), BF16)] * 2
            out_shapes.append(jax.ShapeDtypeStruct((ff, width), BF16))
            out_specs += [far] * 3
            own = products_scratch(x[0].shape[0], width, ff)
            counts.append((5, 3, len(own)))
            scratch += own
            continue
        if kind == "backward":
            rows, width = x[0].shape
            args += x
            in_specs += [far] * 2 + [near] * 9
            out_shapes.append(jax.ShapeDtypeStruct((lines, rows, width), BF16))
            out_shapes.append(jax.ShapeDtypeStruct((lines, rows, x[9].shape[2]), BF16))
            out_shapes.append(jax.ShapeDtypeStruct((8, HEAD_DIM), F32))
            out_specs += [far, near, near]
            own = backward_scratch(lines, rows, width)
            counts.append((11, 3, len(own)))
            scratch += own
            continue
        rows, cols = x.shape[-2:]
        spec = near if kind == "reduce" else far
        args.append(x)
        in_specs.append(spec)
        if kind == "gather":
            lead = {"line": (lines,), "plane": (4, 2)}.get(mode, (lines, 4, 2))
            out_shapes.append(jax.ShapeDtypeStruct((*lead, rows, cols), x.dtype))
            own = gather_sems(mode, lines)
        else:
            if mode == "swap":
                out_shapes.append(jax.ShapeDtypeStruct((lines, rows, cols), x.dtype))
            else:
                out_shapes.append(jax.ShapeDtypeStruct((rows, cols), F32))
            own = reduce_scratch(mode, lines, rows, cols, x.dtype)
        out_specs.append(spec)
        scratch += own
        counts.append((1, 1, len(own)))
    kinds = [(kind, mode) for kind, mode, _ in jobs]

    def body(*refs):
        spot = Spot(lines)
        spot.greet()
        ins, outs, rest = 0, len(args), len(args) + len(out_shapes)
        makers = []
        for (kind, mode), (n_in, n_out, n_rest) in zip(kinds, counts):
            i, o, w = refs[ins : ins + n_in], refs[outs : outs + n_out], refs[rest : rest + n_rest]
            ins, outs, rest = ins + n_in, outs + n_out, rest + n_rest
            if kind == "products":
                makers.append(products(i, o, w))
            elif kind == "backward":
                makers.append(backward(spot, i, o, w))
            elif kind == "gather":
                makers.append(gather(spot, mode, i[0], o[0], w))
            elif mode == "line":
                makers.append(reduce_line(spot, i[0], o[0], w))
            else:
                makers.append(reduce(spot, mode, i[0], o[0], w))
        run_steps(makers)

    outs = pl.pallas_call(
        body,
        out_shape=tuple(out_shapes),
        in_specs=in_specs,
        out_specs=tuple(out_specs),
        scratch_shapes=scratch,
        compiler_params=pltpu.CompilerParams(
            collective_id=cid, has_side_effects=True, vmem_limit_bytes=67_000_000
        ),
        name=name,
    )(*args)
    results, at = [], 0
    for _, n_out, _ in counts:
        results.append(outs[at] if n_out == 1 else outs[at : at + n_out])
        at += n_out
    return results


def exchange_by_xla(kind, mode, x, lines, cells):
    if kind == "products":
        hidden, grad_slots, acts, grad_gate, grad_up = x
        return dot(hidden.T, grad_gate), dot(hidden.T, grad_up), dot(acts.T, grad_slots)
    rows, cols = x.shape[-2:]
    if kind == "gather":
        if mode == "swap":
            x = lax.all_to_all(x, LINE, split_axis=0, concat_axis=0, tiled=True)
            return lax.all_gather(x, PLANE, axis=1)
        return lax.all_gather(x, {"line": LINE, "plane": PLANE, "all": ALL}[mode])
    if mode == "swap":
        x = x.reshape(lines, cells, rows, cols).transpose(1, 0, 2, 3)
        x = lax.psum_scatter(x, PLANE, scatter_dimension=0, tiled=True)
        x = x.reshape(lines, rows, cols)
        return lax.all_to_all(x, LINE, split_axis=0, concat_axis=0, tiled=True)
    x = x.reshape(-1, cols)
    axes = {"line": LINE, "plane": PLANE, "all": ALL}[mode]
    return lax.psum_scatter(x, axes, scatter_dimension=0, tiled=True).astype(F32)


def padded(flat, unit):
    size = -(-flat.shape[0] // unit) * unit
    return jnp.pad(flat, (0, size - flat.shape[0])).reshape(-1, 128)


def pick_order(z, i):
    far = z // 2
    near = z * (1 - far) + (3 - z) * far
    place = (near + i) % 2 if i < 2 else i
    return place * (1 - far) + (3 - place) * far


def dot_nt(left, right):
    return lax.dot_general(left, right, (((1,), (1,)), ((), ())), preferred_element_type=F32)


def experts_body(capacity, *refs):
    lines = 4
    (h_ref, tall, own_w_ref, sel_ref, spread_ref, gate_ref, up_ref, down_ref) = refs[:8]
    (hall, py, dw_all, w_ref, sum_ref, x_out, dy_out, a_out, dg_out, du_out) = refs[8:18]
    rest = list(refs[18:])
    h_sems, w_sems, dw_sems = rest[:7], rest[7:14], rest[14:21]
    sum_scratch = rest[21:29]
    (wg, wu, wd, hb, tb, xs, zs, dys, acts, dgs, dus, rs, ys) = rest[29:42]
    (stage, stage_y, slot_w, acc, dw_ref, w_sem, l_sem, o_sem, p_sem) = rest[42:]
    spot = Spot(lines)
    z, b, c, xn, yn, dg_spot = spot.z, spot.b, spot.c, spot.xn, spot.yn, spot.dg
    me = (z * 4 + b) * 2 + c
    pair = 2 * capacity
    spot.greet()
    steps_h = gather_parts(spot, h_ref, hall, h_sems, even=True)
    steps_w = gather_parts(spot, own_w_ref, w_ref, w_sems)
    steps_dw = gather_parts(spot, dw_ref, dw_all, dw_sems, direct=True)
    both = (steps_w, steps_h)
    columns = (b, xn, yn, dg_spot)
    turn = [0]

    def term(zz, k, cc):
        return stage.at[turn[0] % 2, k, cc]

    steps_r = reduce_parts(spot, "all", term, sum_ref, sum_scratch)

    def sums(name, i, k=1):
        turn[0] = i
        steps_r[name](pick_order(z, i), k)

    def comm_dw(name, d):
        spot.each(d, steps_dw[name])

    loads = [
        pltpu.make_async_copy(gate_ref, wg, w_sem.at[0]),
        pltpu.make_async_copy(up_ref, wu, w_sem.at[1]),
        pltpu.make_async_copy(down_ref, wd, w_sem.at[2]),
    ]

    def comm(*names):
        for s in both:
            for name in names:
                part, d = name.split()
                spot.each(int(d), s[part])

    def load(n):
        i, k = n // 4, n % 4
        zz, bb = pick_order(z, i), columns[k]
        return [
            pltpu.make_async_copy(hall.at[zz, bb], hb.at[n % 3], l_sem.at[0, n % 3]),
            pltpu.make_async_copy(tall.at[zz, bb], tb.at[n % 3], l_sem.at[1, n % 3]),
        ]

    def fetch(n):
        i, k = n // 4, n % 4
        zz = pick_order(z, i)
        for s in both:
            s["shared"](zz, k)
        for copy in load(n):
            copy.start()

    def pick(n):
        i, k = n // 4, n % 4
        zz, bb = pick_order(z, i), columns[k]
        at = pl.ds(pl.multiple_of(bb * pair, 16), pair)
        which = zz * 4 + bb
        for copy in load(n):
            copy.wait()
        rows = hb.shape[2]
        width = hb.shape[3]
        mine = jnp.concatenate(
            [w_ref[zz, bb, 0, pl.ds(me, 1), :], w_ref[zz, bb, 1, pl.ds(me, 1), :]], axis=1
        )
        select = sel_ref[which]
        per_slot = jnp.sum(select.astype(F32) * mine, axis=1, keepdims=True)
        slot_w[i % 2, at, :] = jnp.broadcast_to(per_slot, (pair, 128))

        @pl.loop(0, width // 512)
        def _(j):
            part = pl.ds(pl.multiple_of(j * 512, 512), 512)
            h = hb[n % 3, :, :, part].reshape(2 * rows, 512)
            t = tb[n % 3, :, :, part].reshape(2 * rows, 512)
            xs[i % 2, at, part] = jnp.dot(select, h, preferred_element_type=F32).astype(BF16)
            t = jnp.dot(select, t, preferred_element_type=F32)
            zs[i % 2, at, part] = t.astype(BF16)
            dys[i % 2, at, part] = (per_slot * t).astype(BF16)

    def keep(i):
        zz = pick_order(z, i)
        q = i % 2
        return [
            pltpu.make_async_copy(xs.at[q], x_out.at[zz], o_sem.at[q, 0]),
            pltpu.make_async_copy(dys.at[q], dy_out.at[zz], o_sem.at[q, 1]),
            pltpu.make_async_copy(acts.at[q], a_out.at[zz], o_sem.at[q, 2]),
            pltpu.make_async_copy(dgs.at[q], dg_out.at[zz], o_sem.at[q, 3]),
            pltpu.make_async_copy(dus.at[q], du_out.at[zz], o_sem.at[q, 4]),
        ]

    def inner(i):
        q = i % 2

        @pl.loop(0, wg.shape[1] // 256)
        def _(j):
            part = pl.ds(pl.multiple_of(j * 256, 256), 256)
            g = jnp.dot(xs[q], wg[:, part], preferred_element_type=F32)
            u = jnp.dot(xs[q], wu[:, part], preferred_element_type=F32)
            da = dot_nt(dys[q], wd[part, :])
            sig = jax.nn.sigmoid(g)
            silu = g * sig
            acts[q, :, part] = (silu * u).astype(BF16)
            dgs[q, :, part] = (da * u * sig * (1.0 + g * (1.0 - sig))).astype(BF16)
            dus[q, :, part] = (da * silu).astype(BF16)

        for copy in keep(i):
            copy.start()

    def outer(i):
        q = i % 2
        acc[...] = jnp.zeros_like(acc)

        @pl.loop(0, wg.shape[0] // 256)
        def _(j):
            part = pl.ds(pl.multiple_of(j * 256, 256), 256)
            r = dot_nt(dgs[q], wg[part, :]) + dot_nt(dus[q], wu[part, :])
            rs[:, part] = r.astype(BF16)
            y = jnp.dot(acts[q], wd[:, part], preferred_element_type=F32)
            y = y.astype(BF16).astype(F32)
            met = y * zs[q, :, part].astype(F32)
            acc[...] += met[:, :128] + met[:, 128:]
            ys[:, part] = (slot_w[q, :, 0:1] * y).astype(BF16)

    def put(zz, bb, m):
        return pltpu.make_async_copy(stage_y.at[m % 2], py.at[zz, bb], p_sem.at[m % 2])

    def place(i, k, m):
        zz, bb = pick_order(z, i), columns[k]
        at = pl.ds(pl.multiple_of(bb * pair, 16), pair)
        which = zz * 4 + bb
        if m >= 2:
            put(zz, bb, m).wait()
        dw_slot = jnp.sum(acc[at, :], axis=1, keepdims=True)
        dw_ref[pl.ds(which, 1), :] = jnp.sum(
            sel_ref[which].astype(F32) * dw_slot, axis=0, keepdims=True
        )
        spread = spread_ref[which]
        rows = stage.shape[3]

        @pl.loop(0, rs.shape[1] // 512)
        def _(j):
            part = pl.ds(pl.multiple_of(j * 512, 512), 512)
            full = jnp.dot(spread, rs[at, part], preferred_element_type=F32)
            stage[i % 2, k, :, :, part] = full.astype(BF16).reshape(2, rows, 512)
            full = jnp.dot(spread, ys[at, part], preferred_element_type=F32)
            stage_y[m % 2, :, :, part] = full.astype(BF16).reshape(2, rows, 512)

        put(zz, bb, m).start()

    def places(i):
        order = (3, 1, 2, 0)
        for n, k in enumerate(order):
            place(i, k, 4 * i + n)
            if n >= 1:
                sums("start one", i, order[n - 1])
            if n >= 2:
                sums("first one", i, order[n - 2])
        sums("start one", i, 0)
        sums("first one", i, 2)

    def kept(i):
        for copy in keep(i):
            copy.wait()

    for s in both:
        s["start"]()
    for copy in loads:
        copy.start()
    for s in both:
        s["end"]()
    fetch(0)
    comm("line 1", "plane 0")
    fetch(1)
    fetch(2)
    pick(0)
    pick(1)
    comm("cross 0")
    fetch(3)
    pick(2)
    comm("line 2")
    fetch(4)
    pick(3)
    for copy in loads:
        copy.wait()
    inner(0)
    comm("plane 1")
    fetch(5)
    fetch(6)
    pick(4)
    outer(0)
    pick(5)
    pick(6)
    comm("line 3", "cross 1")
    fetch(7)
    places(0)
    pick(7)
    inner(1)
    kept(0)
    comm("plane 2")
    fetch(8)
    fetch(9)
    fetch(10)
    pick(8)
    pick(9)
    pick(10)
    sums("second", 0)
    outer(1)
    comm("cross 2")
    fetch(11)
    places(1)
    sums("third", 0)
    comm("plane 3")
    fetch(12)
    fetch(13)
    pick(11)
    inner(2)
    kept(1)
    sums("second", 1)
    fetch(14)
    pick(12)
    pick(13)
    pick(14)
    outer(2)
    comm("cross 3")
    fetch(15)
    sums("sent", 0)
    places(2)
    sums("third", 1)
    pick(15)
    inner(3)
    sums("second", 2)
    outer(3)
    sums("sent", 1)
    places(3)
    steps_dw["start"]()
    sums("third", 2)
    for d in (1, 2, 3):
        comm_dw("line", d)
    sums("second", 3)
    for d in range(4):
        comm_dw("plane", d)
    sums("third", 3)
    for d in range(4):
        comm_dw("cross", d)
    steps_r["end"]()
    for m in (0, 1):
        put(z, b, m).wait()
    for i in (2, 3):
        kept(i)
        sums("sent", i)
    for d in range(lines):
        comm(f"drain {d}")
        comm_dw("drain", d)
        spot.each(d, steps_r["drain"])
        for k in range(4):
            spot.each(d, lambda zz, way, k=k: steps_dw["shared"](zz, k))
    steps_dw["end"]()


def experts_call(hidden_two, cotangent_all, own_weights, routes_all, gate, up, down, capacity):
    lines, experts = 4, 32
    rows, width = hidden_two.shape
    ff = gate.shape[1]
    pair = 2 * capacity
    group = 4 * pair
    me = (lax.axis_index("line") * 4 + lax.axis_index("plane")) * 2 + lax.axis_index("core")
    mine = jnp.any(routes_all == me, axis=1).reshape(experts, rows)
    rank = jnp.cumsum(mine.astype(jnp.int32), axis=1) - 1
    slot = rank + (jnp.arange(experts, dtype=jnp.int32) % 2 * capacity)[:, None]
    slot = jnp.where(mine, slot, -1).reshape(experts // 2, 2 * rows)
    places = jnp.arange(pair, dtype=jnp.int32)
    select = (slot[:, None, :] == places[None, :, None]).astype(BF16)
    spread = (slot[:, :, None] == places[None, None, :]).astype(BF16)
    anywhere = pl.BlockSpec(memory_space=pl.ANY)
    near = pl.BlockSpec(memory_space=pltpu.VMEM)
    all_rows = jax.ShapeDtypeStruct((lines, 4, 2, rows, width), BF16)
    wide = jax.ShapeDtypeStruct((lines, group, width), BF16)
    thin = jax.ShapeDtypeStruct((lines, group, ff), BF16)
    return pl.pallas_call(
        functools.partial(experts_body, capacity),
        out_shape=(
            all_rows,
            all_rows,
            jax.ShapeDtypeStruct((lines, 4, 2, experts // 2, 2 * rows), F32),
            jax.ShapeDtypeStruct((lines, 4, 2, experts, rows), F32),
            jax.ShapeDtypeStruct((rows, width), F32),
            wide,
            wide,
            thin,
            thin,
            thin,
        ),
        in_specs=[anywhere, anywhere, near, near, near, anywhere, anywhere, anywhere],
        out_specs=(*[anywhere] * 3, near, near, *[anywhere] * 5),
        scratch_shapes=[
            *gather_sems("all", lines),
            *gather_sems("all", lines),
            *gather_sems("all", lines),
            *reduce_scratch("all", lines, rows, width),
            pltpu.VMEM((width, ff), BF16),
            pltpu.VMEM((width, ff), BF16),
            pltpu.VMEM((ff, width), BF16),
            pltpu.VMEM((3, 2, rows, width), BF16),
            pltpu.VMEM((3, 2, rows, width), BF16),
            pltpu.VMEM((2, group, width), BF16),
            pltpu.VMEM((2, group, width), BF16),
            pltpu.VMEM((2, group, width), BF16),
            pltpu.VMEM((2, group, ff), BF16),
            pltpu.VMEM((2, group, ff), BF16),
            pltpu.VMEM((2, group, ff), BF16),
            pltpu.VMEM((group, width), BF16),
            pltpu.VMEM((group, width), BF16),
            pltpu.VMEM((2, 4, 2, rows, width), BF16),
            pltpu.VMEM((2, 2, rows, width), BF16),
            pltpu.VMEM((2, group, 128), F32),
            pltpu.VMEM((group, 128), F32),
            pltpu.VMEM((experts // 2, 2 * rows), F32),
            DMA((3,)),
            DMA((2, 3)),
            DMA((2, 5)),
            DMA((2,)),
        ],
        compiler_params=pltpu.CompilerParams(
            collective_id=2, has_side_effects=True, vmem_limit_bytes=67_000_000
        ),
        name="experts",
    )(hidden_two, cotangent_all, own_weights, select, spread, gate, up, down)


def experts_by_xla(
    hidden_two, cotangent, own_weights, routes_all, gate, up, down, capacity, me, experts
):
    rows = hidden_two.shape[0]
    hidden_all = lax.all_gather(hidden_two, ALL, axis=0, tiled=True)
    gathered = lax.all_gather(own_weights, ALL)
    expert_ids = jnp.arange(experts, dtype=jnp.int32)
    weights_all = gathered.transpose(0, 2, 1).reshape(experts * rows, experts)
    mine = jnp.any(routes_all == me, axis=1).reshape(experts, rows)
    weight_mine = jnp.sum(jnp.where(expert_ids == me, weights_all, 0.0), axis=1).reshape(
        experts, rows
    )
    rank = jnp.cumsum(mine.astype(jnp.int32), axis=1) - 1
    slots = jnp.arange(capacity, dtype=jnp.int32)
    select = (rank[:, None, :] == slots[None, :, None]) & mine[:, None, :]
    select_low = select.astype(BF16)
    slot_weight = jnp.sum(jnp.where(select, weight_mine[:, None, :], 0.0), axis=2).reshape(-1, 1)

    def pick(values):
        return jnp.einsum(
            "sjt,std->sjd",
            select_low,
            values.reshape(experts, rows, D),
            preferred_element_type=F32,
        ).reshape(experts * capacity, D)

    def place(values):
        return (
            jnp.einsum(
                "sjt,sjd->std",
                select_low,
                values.reshape(experts, capacity, D),
                preferred_element_type=F32,
            )
            .astype(BF16)
            .reshape(experts * rows, D)
        )

    expert_rows = pick(hidden_all).astype(BF16)
    own_width = D // experts
    own_columns = lax.dynamic_slice_in_dim(hidden_all, me * own_width, own_width, axis=1)
    expert_rows, own_columns, cotangent = lax.optimization_barrier(
        (expert_rows, own_columns, cotangent)
    )
    cotangent_all = lax.all_gather(cotangent, ALL, axis=0, tiled=True)
    grad_rows_out = pick(cotangent_all)
    grad_slots = (slot_weight * grad_rows_out).astype(BF16)
    gate_act = dot(expert_rows, gate)
    up_act = dot(expert_rows, up)
    gate_sig = jax.nn.sigmoid(gate_act)
    gate_silu = gate_act * gate_sig
    expert_hidden = (gate_silu * up_act).astype(BF16)
    grad_expert_hidden = dot(grad_slots, down.T)
    grad_gate_act = (
        grad_expert_hidden * up_act * gate_sig * (1.0 + gate_act * (1.0 - gate_sig))
    ).astype(BF16)
    grad_up_act = (grad_expert_hidden * gate_silu).astype(BF16)
    grad_rows_in = (dot(grad_gate_act, gate.T) + dot(grad_up_act, up.T)).astype(BF16)
    expert_out = dot(expert_hidden, down).astype(BF16).astype(F32)
    grad_weight_slot = jnp.sum(grad_rows_out * expert_out, axis=1).reshape(experts, capacity)
    grad_weight_mine = jnp.sum(jnp.where(select, grad_weight_slot[:, :, None], 0.0), axis=1)
    out_rows = (slot_weight * expert_out).astype(BF16)

    placed = place(grad_rows_in).reshape(experts, rows, D)
    grad_weight, grad_rows_sum = exchange(
        "sum_rows", 3, [("gather", "all", grad_weight_mine), ("reduce", "all", placed)]
    )
    placed_out = place(lax.optimization_barrier((out_rows, grad_rows_sum))[0])
    return (
        own_columns,
        placed_out,
        grad_weight,
        gathered,
        grad_rows_sum,
        expert_rows,
        grad_slots,
        expert_hidden,
        grad_gate_act,
        grad_up_act,
    )


def on_device(
    tokens,
    lengths,
    routes,
    cotangent,
    query_weight,
    key_weight,
    value_weight,
    output_weight,
    router_weight,
    norm_gains,
    gate_weight,
    up_weight,
    down_weight,
):
    rows = tokens.shape[0]
    lines = lax.axis_size("line")
    cells = lax.axis_size("plane") * lax.axis_size("core")
    experts = lines * cells
    capacity = (3 * rows * TOP + 2 * experts - 1) // (2 * experts)
    score_scale = HEAD_DIM ** (-0.5)
    large = experts > 32
    own_rows = query_weight.shape[0]
    line = lax.axis_index("line")
    me = (line * lax.axis_size("plane") + lax.axis_index("plane")) * lax.axis_size(
        "core"
    ) + lax.axis_index("core")

    packed = jnp.concatenate(
        [
            query_weight.reshape(own_rows, lines, Q_COLS),
            key_weight.reshape(own_rows, lines, HEAD_DIM),
            value_weight.reshape(own_rows, lines, HEAD_DIM),
        ],
        axis=2,
    ).transpose(1, 0, 2)
    width = packed.shape[2]
    floats = padded(jnp.concatenate([router_weight.reshape(-1), norm_gains]), 32 * 128)
    whole_numbers = padded(jnp.concatenate([routes.reshape(-1), lengths.reshape(-1)]), 16 * 128)
    floats_all, numbers_all, weight_qkv, line_tokens, weight_o = exchange(
        "gather_inputs",
        0,
        [
            ("gather", "all", floats),
            ("gather", "all", whole_numbers),
            ("gather", "swap", packed),
            ("gather", "line", tokens),
            ("gather", "plane", output_weight),
        ],
    )
    weight_qkv = weight_qkv.reshape(lines * cells * own_rows, width)
    weight_o = weight_o.reshape(cells * output_weight.shape[0], D)
    floats_all = floats_all.reshape(experts, -1)
    router_size = own_rows * experts
    router = floats_all[:, :router_size].reshape(D, experts)
    gains = floats_all[:, router_size : router_size + norm_gains.shape[0]].reshape(-1).astype(F32)
    numbers_all = numbers_all.reshape(experts, -1)
    routes_all = numbers_all[:, : rows * TOP].reshape(experts * rows, TOP)
    lengths_all = numbers_all[:, rows * TOP : rows * TOP + lengths.shape[1]]
    line_lengths = lax.dynamic_slice_in_dim(
        lengths_all.reshape(lines, cells, -1), me % cells, 1, axis=1
    )[:, 0]
    gain_attn = gains[:D]
    gain_ffn = gains[D : 2 * D]
    gain_query = gains[2 * D : 2 * D + HEAD_DIM]
    gain_key = gains[2 * D + HEAD_DIM :]

    inputs = line_tokens.reshape(lines * rows, D).astype(F32)
    attn_scale = rms_scale(inputs)
    attn_normed = inputs * attn_scale
    hidden_one = (attn_normed * gain_attn).astype(BF16)
    proj = dot(hidden_one, weight_qkv)
    query_proj = proj[:, :Q_COLS].reshape(lines, rows, GROUPS, HEAD_DIM)
    key_proj = proj[:, Q_COLS : Q_COLS + HEAD_DIM].reshape(lines, rows, HEAD_DIM)
    value_proj = proj[:, Q_COLS + HEAD_DIM :].astype(BF16).reshape(lines, rows, HEAD_DIM)
    query_scale = rms_scale(query_proj)
    query_normed = query_proj * query_scale
    key_scale = rms_scale(key_proj)
    key_normed = key_proj * key_scale
    segment, positions = jax.vmap(lambda row: sequence_layout(row, rows))(line_lengths)
    cosine, sine_table = rope_tables(positions, HEAD_DIM)
    query_rot = rotate(
        query_normed * gain_query, cosine[:, :, None], sine_table[:, :, None]
    ).astype(BF16)
    key_rot = rotate(key_normed * gain_key, cosine, sine_table).astype(BF16)
    allowed = (segment[:, :, None] == segment[:, None, :]) & (
        positions[:, None, :] <= positions[:, :, None]
    )
    mixed_heads, log_total = attend(query_rot, key_rot, value_proj, allowed, score_scale)
    mixed_low = mixed_heads.reshape(lines * rows, Q_COLS).astype(BF16)
    projected = dot(mixed_low, weight_o).astype(BF16).reshape(lines, rows, D)
    jobs = [("reduce", "line", projected)]
    if not large:
        jobs.insert(0, ("gather", "all", cotangent))
    *cotangent_all, projected = exchange("sum_residual", 1, jobs)
    cotangent_all = None if large else cotangent_all[0]
    own_inputs = tokens.astype(F32)
    residual = own_inputs + projected
    ffn_scale = rms_scale(residual)
    ffn_normed = residual * ffn_scale
    hidden_two = (ffn_normed * gain_ffn).astype(BF16)

    expert_ids = jnp.arange(experts, dtype=jnp.int32)
    named = jnp.any(routes[:, :, None] == expert_ids, axis=1).T
    logits = lax.dot_general(
        router, hidden_two, (((0,), (1,)), ((), ())), preferred_element_type=F32
    )
    masked = jnp.where(named, logits, masked_score)
    exponent = jnp.where(named, jnp.exp(masked - jnp.max(masked, axis=0, keepdims=True)), 0.0)
    own_weights = exponent / jnp.sum(exponent, axis=0, keepdims=True)
    weights = (gate_weight[0], up_weight[0], down_weight[0])
    if large:
        done = experts_by_xla(
            hidden_two, cotangent, own_weights, routes_all, *weights, capacity, me, experts
        )
    else:
        done = experts_call(
            hidden_two, cotangent_all, own_weights, routes_all, *weights, capacity
        )
    hidden_all, placed_out, grad_weight, weights_all, grad_rows_sum = done[:5]
    weights_all = weights_all.reshape(experts, experts, rows).transpose(1, 0, 2)
    weights_all = weights_all.reshape(experts, experts * rows)
    kept = [v.reshape(-1, v.shape[-1]) for v in done[5:]]
    if large:
        own_columns = hidden_all
    else:
        hidden_all = hidden_all.reshape(experts * rows, D)
        own_columns = lax.dynamic_slice_in_dim(hidden_all, me * own_rows, own_rows, axis=1)
    grad_weight = grad_weight.reshape(experts, experts * rows)

    grad_logits = weights_all * (
        grad_weight - jnp.sum(weights_all * grad_weight, axis=0, keepdims=True)
    )
    grad_logits = grad_logits.astype(BF16)
    router_grad = lax.dot_general(
        own_columns, grad_logits, (((0,), (1,)), ((), ())), preferred_element_type=F32
    )
    own_grad_logits = lax.dynamic_slice_in_dim(grad_logits, me * rows, rows, axis=1).T

    grad_out = cotangent.astype(F32)
    grad_hidden_two = dot(own_grad_logits, router.T) + grad_rows_sum.astype(F32)
    grad_gain_ffn = jnp.sum(grad_hidden_two * ffn_normed, axis=0)
    grad_residual = grad_out + norm_back(grad_hidden_two * gain_ffn, ffn_normed, ffn_scale)
    grad_low = grad_residual.astype(BF16)
    jobs = [
        ("reduce", "all", placed_out.reshape(lines, -1, 2, rows, D)),
        ("products", "", kept),
    ]
    if large:
        jobs.insert(0, ("gather", "line", grad_low))
    else:
        turn_back = [jnp.concatenate([v, w], axis=-1) for v, w in ((cosine, cosine), (sine_table, -sine_table))]
        given = (
            grad_low,
            weight_o,
            query_rot.reshape(lines, rows, Q_COLS),
            key_rot,
            value_proj,
            log_total.reshape(lines, GROUPS * rows, 1),
            allowed.astype(F32),
            *turn_back,
            proj.reshape(lines, rows, width),
            jnp.pad(gains[2 * D :].reshape(2, HEAD_DIM), ((0, 6), (0, 0))),
        )
        jobs.insert(0, ("backward", "", given))
    came, out_sum, (grad_gate, grad_up, grad_down) = exchange("gather_grad", 4, jobs)
    block_out = (residual + out_sum).astype(BF16)
    grad_attn = (came if large else came[0]).reshape(lines * rows, D)
    output_part = dot(mixed_low.T, grad_attn).astype(BF16)
    if large:
        grad_mixed = dot(grad_attn, weight_o.T).astype(BF16).reshape(lines, rows, GROUPS, HEAD_DIM)
        grad_query_rot, grad_key_rot, grad_value_rot = attend_back(
            query_rot, key_rot, value_proj, allowed, score_scale, log_total, grad_mixed
        )
        grad_value_proj = grad_value_rot.astype(BF16)
        grad_query_gained = rotate(grad_query_rot, cosine[:, :, None], -sine_table[:, :, None])
        grad_gain_query = jnp.sum(grad_query_gained * query_normed, axis=(0, 1, 2))
        grad_query_proj = norm_back(grad_query_gained * gain_query, query_normed, query_scale).astype(
            BF16
        )
        grad_key_gained = rotate(grad_key_rot, cosine, -sine_table)
        grad_gain_key = jnp.sum(grad_key_gained * key_normed, axis=(0, 1))
        grad_key_proj = norm_back(grad_key_gained * gain_key, key_normed, key_scale).astype(BF16)
        grad_proj = jnp.concatenate(
            [
                grad_query_proj.reshape(lines * rows, Q_COLS),
                grad_key_proj.reshape(lines * rows, HEAD_DIM),
                grad_value_proj.reshape(lines * rows, HEAD_DIM),
            ],
            axis=1,
        )
    else:
        grad_proj = came[1].reshape(lines * rows, width)
        grad_gain_query, grad_gain_key = came[2][0], came[2][1]
    hidden_one_part = dot(grad_proj, weight_qkv.T)
    grad_gain_attn = jnp.sum(hidden_one_part * attn_normed, axis=0)
    qkv_part = dot(hidden_one.T, grad_proj).astype(BF16)
    gains_local = jnp.concatenate([grad_gain_attn, grad_gain_ffn, grad_gain_query, grad_gain_key])
    gains_all, grad_hidden_one, qkv_part, output_grad = exchange(
        "sum_gradients",
        5,
        [
            ("gather", "all", padded(gains_local, 16 * 128)),
            ("reduce", "line", hidden_one_part.astype(BF16).reshape(lines, rows, D)),
            ("reduce", "swap", qkv_part.reshape(lines, -1, 2, own_rows, width)),
            ("reduce", "plane", output_part.reshape(-1, 2, output_weight.shape[0], D)),
        ],
    )
    own_scale = rms_scale(own_inputs)
    own_normed = own_inputs * own_scale
    input_grad = grad_residual + norm_back(grad_hidden_one * gain_attn, own_normed, own_scale)
    qkv_part = qkv_part.transpose(1, 0, 2).astype(F32)
    query_grad = qkv_part[:, :, :Q_COLS].reshape(own_rows, lines * Q_COLS)
    key_grad = qkv_part[:, :, Q_COLS : Q_COLS + HEAD_DIM].reshape(own_rows, lines * HEAD_DIM)
    value_grad = qkv_part[:, :, Q_COLS + HEAD_DIM :].reshape(own_rows, lines * HEAD_DIM)
    share = norm_gains.shape[0]
    gains_all = gains_all.reshape(experts, -1)
    gains_all = lax.dynamic_slice_in_dim(gains_all, me * share, share, axis=1)
    gains_grad = jnp.sum(gains_all, axis=0)
    return (
        block_out,
        input_grad,
        query_grad,
        key_grad,
        value_grad,
        output_grad,
        router_grad,
        gains_grad,
        grad_gate[None].astype(F32),
        grad_up[None].astype(F32),
        grad_down[None].astype(F32),
    )


def solution(mesh):
    chips = mesh.shape["expert"]
    cores = mesh.shape["shard"]
    inner = Mesh(
        mesh.devices.reshape(KV_HEADS, chips // KV_HEADS, cores), ("line", "plane", "core")
    )
    return jax.shard_map(
        on_device,
        mesh=inner,
        in_specs=(
            P(ALL, None),
            P(ALL, None),
            P(ALL, None),
            P(ALL, None),
            P(ALL, None),
            P(ALL, None),
            P(ALL, None),
            P(ALL, None),
            P(ALL, None),
            P(ALL),
            P(ALL, None, None),
            P(ALL, None, None),
            P(ALL, None, None),
        ),
        out_specs=(
            P(ALL, None),
            P(ALL, None),
            P(ALL, None),
            P(ALL, None),
            P(ALL, None),
            P(ALL, None),
            P(ALL, None),
            P(ALL),
            P(ALL, None, None),
            P(ALL, None, None),
            P(ALL, None, None),
        ),
        check_vma=False,
    )
```
